32 devices in a mesh: gx: 2 (over y), gy: 4 (over x, core), gz: 4 (over z).
Axes of the slice: x: 2, y: 2, z: 4, core: 2. Of those that a mesh axis runs over, the one named last changes fastest.
Arguments:
- pressure: float32 [24, 64, 512], P('gx', 'gy', 'gz'), may hold values from -8 to 8
- wind: float32 [3, 24, 64, 512], P(None, 'gx', 'gy', 'gz'), may hold values from -6 to 6
Outputs:
- result: float32 [24, 64, 512], P('gx', 'gy', 'gz')
The draws below stay inside these ranges and needn't reach their ends.
All inputs are finite; a program needn't handle non-finite values.
Results may differ from the reference program's by a relative error of at most 0.00019.
Values sent between devices are 32-bit elements; how exact they have to be, the bound alone decides.
No kernel may reach another device: no remote copies, remote signals or barrier semaphores. Data moves between devices by JAX's collectives and lax.ppermute only.
A program may use at most 64 MiB of HBM per device.

```python
import jax
import jax.numpy as jnp

SWEEPS = 2
COARSE_SWEEPS = 4
CYCLES = 1
NX = 24
NY = 64
NZ = 512


def draw_pressure(key, part):
    noise = jax.random.normal(key, (NX, NY, NZ), jnp.float32)
    return jnp.clip(noise, -8.0, 8.0)


def level_of(own_key, dims, split, low, high):
    factor_of = 1.0
    for dim, blocks in split:
        draws = jax.random.uniform(jax.random.fold_in(jax.random.fold_in(own_key, 6), dim), (blocks,), jnp.float32, low / len(split), high / len(split))
        factor_of = factor_of * jnp.repeat(jnp.exp(draws), dims[dim] // blocks).reshape((-1,) + (1,) * (len(dims) - 1 - dim))
    return factor_of


def normal_values(key, shape, deviation, limit, shards=(), held_as=jnp.bfloat16):
    array = jax.random.normal(key, shape, jnp.float32) * deviation
    if len(shards) > 0:
        array = level_of(key, shape, shards, -0.22, 0.18) * array
    return jnp.clip(array, min=-limit, max=limit).astype(held_as)


def setup_inputs(seed: int = 0) -> dict:
    keys = jax.random.split(jax.random.key(seed), 3)
    pressure = draw_pressure(jax.random.fold_in(keys[2], 71), 0)
    wind = normal_values(keys[1], (3, NX, NY, NZ), 1.0, 6.0, ((1, 2), (2, 4), (3, 4)), jnp.float32)
    return {"pressure": pressure, "wind": wind}


OMEGA = 0.8
VISCOSITY = 1.0
REACTION = 1.0


def six_sum(padded):
    return (padded[..., 2:, 1:-1, 1:-1] + padded[..., :-2, 1:-1, 1:-1]
            + padded[..., 1:-1, 2:, 1:-1] + padded[..., 1:-1, :-2, 1:-1]
            + padded[..., 1:-1, 1:-1, 2:] + padded[..., 1:-1, 1:-1, :-2])


def central_parts(padded):
    return ((padded[..., 2:, 1:-1, 1:-1] - padded[..., :-2, 1:-1, 1:-1]) * 0.5,
            (padded[..., 1:-1, 2:, 1:-1] - padded[..., 1:-1, :-2, 1:-1]) * 0.5,
            (padded[..., 1:-1, 1:-1, 2:] - padded[..., 1:-1, 1:-1, :-2]) * 0.5)


def pad_space(values):
    return jnp.pad(values, [(0, 0)] * (values.ndim - 3) + [(1, 1), (1, 1), (1, 1)])


def laplace(values, padded, weight_scale):
    return weight_scale * (6.0 * values - six_sum(padded))


def sweep(source, values, padded, weight_scale):
    return values + (OMEGA / (6.0 * weight_scale)) * (source - laplace(values, padded, weight_scale))


def start_sweep(source, weight_scale):
    return (OMEGA / (6.0 * weight_scale)) * source


def smooth(source, values, weight_scale, sweep_count):
    for sweep_number in range(sweep_count):
        if values is None:
            values = start_sweep(source, weight_scale)
        else:
            values = sweep(source, values, pad_space(values), weight_scale)
    return values


def restrict(values):
    extent_x, extent_y, extent_z = values.shape
    blocks = values.reshape(extent_x // 2, 2, extent_y // 2, 2, extent_z // 2, 2)
    return 0.125 * jnp.sum(blocks, axis=(1, 3, 5))


def prolong(values):
    extent_x, extent_y, extent_z = values.shape
    spread = jnp.broadcast_to(values[:, None, :, None, :, None], (extent_x, 2, extent_y, 2, extent_z, 2))
    return spread.reshape(2 * extent_x, 2 * extent_y, 2 * extent_z)


def vcycle(source, values, depth_index):
    weight_scale = 0.25 ** depth_index
    if depth_index == 2:
        return smooth(source, None, weight_scale, COARSE_SWEEPS)
    values = smooth(source, values, weight_scale, SWEEPS)
    residual = source - laplace(values, pad_space(values), weight_scale)
    correction = vcycle(restrict(residual), None, depth_index + 1)
    values = values + prolong(correction)
    return smooth(source, values, weight_scale, SWEEPS)


def solve(source):
    values = None
    for cycle_number in range(CYCLES):
        values = vcycle(source, values, 0)
    return values


def momentum(padded_velocity, wind):
    centre = padded_velocity[:, 1:-1, 1:-1, 1:-1]
    diffusion = 6.0 * centre - six_sum(padded_velocity)
    slopes = central_parts(padded_velocity)
    convection = wind[0:1] * slopes[0] + wind[1:2] * slopes[1] + wind[2:3] * slopes[2]
    return REACTION * centre + VISCOSITY * diffusion + convection


def reference(pressure, wind):
    first = solve(pressure)
    velocity = jnp.stack(central_parts(pad_space(first)))
    flux = momentum(pad_space(velocity), wind)
    slopes = central_parts(pad_space(flux))
    product = -(slopes[0][0] + slopes[1][1] + slopes[2][2])
    return solve(product)
```

```python
import functools

import jax
import jax.numpy as jnp
from jax import lax
from jax.experimental import pallas as pl
from jax.experimental.pallas import tpu as pltpu
from jax.sharding import PartitionSpec as P

OMEGA = 0.8
W = OMEGA / 6.0
C0, C1, C2 = W, 4.0 * W, 16.0 * W
SIDE = 8
PLANE = ("gx", "gy")


def up(v, axis):
    return pltpu.roll(v, v.shape[axis] - 1, axis)


def down(v, axis):
    return pltpu.roll(v, 1, axis)


def mix(s, i):
    c = s[i]
    near = (s[i - 1] + s[i + 1]) + (up(c, 0) + down(c, 0)) + (up(c, 1) + down(c, 1))
    return (1.0 - OMEGA) * c + W * near


def each(n, step):
    lax.fori_loop(0, n, lambda i, _: step(i), None, unroll=2 if n % 2 == 0 else 1)


def iota(shape, axis):
    return lax.broadcasted_iota(jnp.int32, shape, axis)


def pair_matrix(rows, columns, value):
    hit = (iota((rows, columns), 0) >> 1) == iota((rows, columns), 1)
    return jnp.where(hit, value, 0.0).astype(jnp.float32)


def spread_matrix(rows, columns):
    hit = (iota((rows, columns), 1) >> 1) == iota((rows, columns), 0)
    return jnp.where(hit, 1.0, 0.0).astype(jnp.float32)


def dot(a, b):
    return jnp.dot(a, b, precision=lax.Precision.HIGHEST, preferred_element_type=jnp.float32)


def window_mask(shape, y_first, y_count, z_first, z_count):
    y = iota(shape, 0) + y_first
    z = iota(shape, 1) + z_first
    good = (y >= 0) & (y < y_count) & (z >= 0) & (z < z_count)
    return jnp.where(good, 1.0, 0.0).astype(jnp.float32)


class Sizes:
    def __init__(self, gx, gy, gz, bx, by, bz):
        self.gx, self.gy, self.gz = gx, gy, gz
        self.bx, self.by, self.bz = bx, by, bz
        self.rows, self.lanes = by + 2 * SIDE, 2 * bz
        self.one = gx == 2
        self.c1_n = bx // 2 + (1 if self.one else 2)
        self.c2_n = bx // 2 + (2 if self.one else 4)
        self.yf_n = bx + (3 if self.one else 6)
        self.nx1, self.ny1 = gx * bx // 2, gy * by // 2
        self.rows1 = self.ny1 + SIDE
        self.rows1p = -(-self.rows1 // 16) * 16
        self.l1 = bz
        self.c1_rows = by // 2 + 4
        self.c2_rows = by // 2 + 8
        self.edge = 5
        self.edge_sets = 1 if self.one else 2
        self.pack1 = self.c1_n * self.c1_rows + self.edge_sets * self.edge * 2 * by
        self.pack2 = self.c2_n * self.c2_rows + self.yf_n * 8

    def c1_first(self, i):
        return -i if self.one else -1

    def c2_first(self, i):
        return -2 * i if self.one else -2

    def yf_first(self, i):
        return -3 * i if self.one else -3


def slab_kernel(k, p_ref, w_ref, right_ref, left_ref):
    bx, bz = k.bx, k.bz
    half, part = bz // 2, bz // 4
    lane = iota((k.by, bz), 1)
    for x in range(bx):
        p = pltpu.roll(p_ref[x], half, 1)
        a, b = w_ref[0, x], w_ref[1, x]
        right_ref[x] = jnp.where(lane < half, p, jnp.where(lane < half + part, pltpu.roll(a, bz - part, 1), b))
        left_ref[x] = jnp.where(lane >= half, p, jnp.where(lane < part, a, pltpu.roll(b, part, 1)))
    for q in range(-(-bx // 4)):
        r_all, l_all = jnp.zeros((k.by, bz), jnp.float32), jnp.zeros((k.by, bz), jnp.float32)
        for r in range(min(4, bx - 4 * q)):
            c = w_ref[2, 4 * q + r]
            here = (lane >= part * r) & (lane < part * (r + 1))
            r_all = jnp.where(here, pltpu.roll(c, (part * r + part) % bz, 1), r_all)
            l_all = jnp.where(here, pltpu.roll(c, part * r, 1) if r else c, l_all)
        right_ref[bx + q] = r_all
        left_ref[bx + q] = l_all


def lane_roll(v, shift):
    shift = shift % v.shape[1]
    return pltpu.roll(v, shift, 1) if shift else v


def pressure_window(k, p, low, high):
    half = k.bz // 2
    lane = iota(p.shape, 1)
    p = pltpu.roll(p, half, 1)
    return jnp.concatenate([jnp.where(lane < half, low, p), jnp.where(lane < half, p, high)], axis=1)


def wind_window(k, w, low, low_at, high, high_at):
    half, part = k.bz // 2, k.bz // 4
    lane = iota(w.shape, 1)
    w = pltpu.roll(w, half, 1)
    first = jnp.where(lane >= half, w, jnp.where(lane >= part, lane_roll(low, part - low_at), 0.0))
    second = jnp.where(lane < half, w, jnp.where(lane < half + part, lane_roll(high, half - high_at), 0.0))
    return jnp.concatenate([first, second], axis=1)


def place():
    return lax.axis_index("gx"), lax.axis_index("gy"), lax.axis_index("gz")


def fine_mask(k, iy, iz):
    return window_mask((k.rows, k.lanes), iy * k.by - SIDE, k.gy * k.by, iz * k.bz - k.bz // 2, k.gz * k.bz)


def x_inside(k, ix, plane):
    place_x = ix * k.bx + plane
    return jnp.where((place_x >= 0) & (place_x < k.gx * k.bx), 1.0, 0.0).astype(jnp.float32)


def restrict_planes(src, first, n, half_ref, out, value):
    rows, lanes = src.shape[1], src.shape[2]
    a = pair_matrix(lanes, half_ref.shape[2], value)

    def step(j):
        s = src[first + 2 * j] + src[first + 2 * j + 1]
        half_ref[j] = dot(s + up(s, 0), a)

    for j in range(n):
        step(j)
    for j in range(n):
        out[j] = half_ref[j, pl.ds(0, rows // 2, stride=2), :]


def zero(ref):
    ref[...] = jnp.zeros(ref.shape, ref.dtype)


def first_kernel(k, p_ref, low_ref, high_ref, win_ref, send_a, send_b, pack_ref, b, m, half_ref, c1):
    ix, iy, iz = place()
    bx, by = k.bx, k.by
    pad = 3
    zero(b)
    zero(m)
    for x in range(bx):
        w = pressure_window(k, p_ref[x], low_ref[x], high_ref[x])
        win_ref[x] = w
        b[x + pad, SIDE:SIDE + by, :] = w
    tail = lax.rem(iy, 2) == 0
    for x in range(bx):
        head_rows, tail_rows = win_ref[x, :8, :], win_ref[x, by - 8:, :]
        send_a[x] = jnp.where(tail, tail_rows, head_rows)
        send_b[x] = jnp.where(tail, head_rows, tail_rows)
    mask = fine_mask(k, iy, iz)

    def step1(i):
        m[i + pad - 1] = mix(b, i + pad - 1) * (mask * x_inside(k, ix, i - 1))

    each(bx + 2, step1)

    def step2(i):
        b[i + pad - 2] = mix(m, i + pad - 2)

    each(bx + 4, step2)
    restrict_planes(b, pad - 2, bx // 2 + 2, half_ref, c1, 0.125)
    start = (k.c1_first(ix) + 1) if k.one else 0
    for j in range(k.c1_n):
        pack_ref[j * k.c1_rows:(j + 1) * k.c1_rows, :] = c1[start + j, 2:2 + k.c1_rows, :]
    at = k.c1_n * k.c1_rows
    starts = [(1 - ix) * (bx - k.edge)] if k.one else [0, bx - k.edge]
    for first in starts:
        for j in range(k.edge):
            for t in range(2):
                pack_ref[at:at + by, :] = win_ref[first + j, :, t * k.bz:(t + 1) * k.bz]
                at += by


def coarse(k, iz, b1, m1, e1, half_ref, b2, u2, v2):
    n1, n2 = k.nx1, k.nx1 // 2
    rows1, rows2, l1 = k.rows1, k.rows1p // 2, k.l1
    y0 = -(SIDE // 2)
    mask1 = window_mask((rows1, l1), y0, k.ny1, iz * (k.bz // 2) - k.bz // 4, k.gz * (k.bz // 2))
    lane2 = iota((rows2, l1), 1)
    mask2 = window_mask((rows2, l1), y0 // 2, k.ny1 // 2, iz * (k.bz // 4) - k.bz // 8, k.gz * (k.bz // 4))
    mask2 = jnp.where(lane2 < l1 // 2, mask2, 0.0)
    zero(m1)
    zero(e1)
    zero(u2)
    zero(v2)
    for i in range(n1):
        b1[i + 2] = b1[i + 2] * mask1

    def pre(i):
        c = mix(b1, i + 2) * mask1
        m1[i + 2] = c
        e1[i + 2] = C1 * (b1[i + 2] + c)

    each(n1, pre)
    a = pair_matrix(l1, l1, 0.125)
    for j in range(n2):
        s = mix(m1, 2 * j + 2) + mix(m1, 2 * j + 3)
        half_ref[j, :rows1, :] = dot(s + up(s, 0), a)
        if k.rows1p > rows1:
            half_ref[j, rows1:, :] = jnp.zeros((k.rows1p - rows1, l1), jnp.float32)
    for j in range(n2):
        s = half_ref[j, pl.ds(0, rows2, stride=2), :] * (mask2 * C2)
        b2[j] = s
        u2[j + 1] = s
    src, dst = u2, v2
    for _ in range(3):
        for j in range(n2):
            dst[j + 1] = (mix(src, j + 1) + b2[j]) * mask2
        src, dst = dst, src
    spread = spread_matrix(l1, l1)
    for j in range(n2):
        e = dot(src[j + 1], spread)
        half_ref[j, pl.ds(0, rows2, stride=2), :] = e
        half_ref[j, pl.ds(1, rows2, stride=2), :] = e
    for j in range(n2):
        e = half_ref[j, :rows1, :]
        e1[2 * j + 2] += e
        e1[2 * j + 3] += e
    for src, dst in ((e1, m1), (m1, e1)):

        def post(i):
            dst[i + 2] = (mix(src, i + 2) + C1 * b1[i + 2]) * mask1

        each(n1, post)


def prolonged(k, e1, ix, iy, first, n, half_ref, put):
    by = k.by
    for j in range(n):
        e = e1[ix * (k.bx // 2) + (first + j + 2), pl.ds(pl.multiple_of(iy * (by // 2), 8), k.rows // 2), :]
        half_ref[j, pl.ds(0, k.rows // 2, stride=2), :] = e
        half_ref[j, pl.ds(1, k.rows // 2, stride=2), :] = e
    spread = spread_matrix(k.l1, k.lanes)
    for j in range(n):
        put(j, dot(half_ref[j], spread))


def overlap_add(k, g_ref, b1, n, rows, y_skip, first_of):
    zero(b1)
    for i in range(k.gx):
        for j in range(k.gy):
            at_y = j * (k.by // 2) + y_skip
            for q in range(n):
                x = i * (k.bx // 2) + first_of(i) + q
                if 0 <= x < k.nx1:
                    part = g_ref[i * k.gy + j, q * rows:(q + 1) * rows, :]
                    b1[x + 2, at_y:at_y + rows, :] += part


def own_lanes(k, v):
    half = k.bz // 2
    first, second = v[:, :k.bz], v[:, k.bz:]
    lane = iota(first.shape, 1)
    return jnp.where(lane < half, pltpu.roll(first, half, 1), pltpu.roll(second, half, 1))


def middle_kernel(k, g_ref, win_ref, got_a, got_b, w_ref, low_ref, high_ref, pack_ref, xa_ref, xb_ref, own_ref,
                  b1, m1, e1, half1, b2, u2, v2, b, m, v, vel, flux, half_ref, c2):
    ix, iy, iz = place()
    bx, by = k.bx, k.by
    overlap_add(k, g_ref, b1, k.c1_n, k.c1_rows, 2, k.c1_first)
    coarse(k, iz, b1, m1, e1, half1, b2, u2, v2)
    pad = 5
    mask = fine_mask(k, iy, iz)
    even = lax.rem(iy, 2) == 0
    for x in range(bx):
        b[x + pad, :SIDE, :] = jnp.where(even, got_b[x], got_a[x])
        b[x + pad, SIDE:SIDE + by, :] = win_ref[x]
        b[x + pad, SIDE + by:, :] = jnp.where(even, got_a[x], got_b[x])
    base = k.c1_n * k.c1_rows
    span = k.edge * 2 * by
    y_low, y_high = jnp.maximum(iy - 1, 0), jnp.minimum(iy + 1, k.gy - 1)
    for side in range(2):
        if k.one:
            who, shift = 1 - ix, 0
        else:
            who = jnp.maximum(ix - 1, 0) if side == 0 else jnp.minimum(ix + 1, k.gx - 1)
            shift = span if side == 0 else 0
        for j in range(k.edge):
            at = pad - k.edge + j if side == 0 else pad + bx + j
            for t in range(2):
                row = base + shift + (2 * j + t) * by
                lanes = slice(t * k.bz, (t + 1) * k.bz)
                b[at, :SIDE, lanes] = g_ref[who * k.gy + y_low, row + by - 8:row + by, :]
                b[at, SIDE:SIDE + by, lanes] = g_ref[who * k.gy + iy, row:row + by, :]
                b[at, SIDE + by:, lanes] = g_ref[who * k.gy + y_high, row:row + 8, :]

    def clean(i):
        b[i] = b[i] * (mask * x_inside(k, ix, i - pad))

    each(bx + 2 * pad, clean)

    def put(j, e):
        for t in range(2):
            v[pad - 4 + 2 * j + t] = e

    prolonged(k, e1, ix, iy, -2, bx // 2 + 4, half_ref, put)

    def pre(i):
        at = i + pad - 4
        here = mask * x_inside(k, ix, i - 4)
        v[at] = (v[at] + C0 * (b[at] + mix(b, at))) * here

    each(bx + 8, pre)

    def post1(i):
        at = i + pad - 3
        m[at] = (mix(v, at) + C0 * b[at]) * (mask * x_inside(k, ix, i - 3))

    each(bx + 6, post1)

    def post2(i):
        at = i + pad - 2
        v[at] = (mix(m, at) + C0 * b[at]) * (mask * x_inside(k, ix, i - 2))

    each(bx + 4, post2)

    def speed(i):
        at = i + pad - 1
        here = 0.5 * (mask * x_inside(k, ix, i - 1))
        c = v[at]
        vel[0, i] = (v[at + 1] - v[at - 1]) * here
        vel[1, i] = (up(c, 0) - down(c, 0)) * here
        vel[2, i] = (up(c, 1) - down(c, 1)) * here

    each(bx + 2, speed)
    own_mask = mask[SIDE:SIDE + by, :]
    zero(flux)
    half, part = k.bz // 2, k.bz // 4
    for x in range(bx):
        low, high = low_ref[x], high_ref[x]
        w0 = 0.5 * wind_window(k, w_ref[0, x], low, half, high, 0)
        w1 = 0.5 * wind_window(k, w_ref[1, x], low, half + part, high, part)
        q, r = x // 4, x % 4
        w2 = 0.5 * wind_window(k, w_ref[2, x], low_ref[bx + q], part * r, high_ref[bx + q], part * r)
        for d in range(3):
            c = vel[d, x + 1, SIDE:SIDE + by, :]
            xp, xm = vel[d, x + 2, SIDE:SIDE + by, :], vel[d, x, SIDE:SIDE + by, :]
            yp, ym = vel[d, x + 1, SIDE + 1:SIDE + by + 1, :], vel[d, x + 1, SIDE - 1:SIDE + by - 1, :]
            zp, zm = up(c, 1), down(c, 1)
            near = (xp + xm) + (yp + ym) + (zp + zm)
            total = 7.0 * c - near + w0 * (xp - xm) + w1 * (yp - ym) + w2 * (zp - zm)
            flux[d, x + 2, SIDE:SIDE + by, :] = total * own_mask
    zero(b)
    zero(m)

    def spread_flux(i):
        at = i + pad - 1
        f1, f2 = flux[1, i + 1], flux[2, i + 1]
        total = (flux[0, i + 2] - flux[0, i]) + (up(f1, 0) - down(f1, 0)) + (up(f2, 1) - down(f2, 1))
        b[at] = total * (-0.5 * (mask * x_inside(k, ix, i - 1)))

    each(bx + 2, spread_flux)
    zero(v)

    def power1(i):
        at = i + pad - 2
        c = mix(b, at) * (mask * x_inside(k, ix, i - 2))
        m[at] = c
        b[at] = b[at] + c

    def power1_pure(i):
        at = i + pad - 2
        m[at] = mix(b, at) * (mask * x_inside(k, ix, i - 2))

    each(bx + 4, power1_pure)

    def power2(i):
        at = i + pad - 3
        v[at] = mix(m, at) * (mask * x_inside(k, ix, i - 3))

    each(bx + 6, power2)

    def power3(i):
        at = i + pad - 4
        b[at] = C0 * ((b[at] + m[at]) + (v[at] + mix(v, at))) * (mask * x_inside(k, ix, i - 4))

    each(bx + 8, power3)
    restrict_planes(v, pad - 4, bx // 2 + 4, half_ref, c2, 0.125)
    start = (k.c2_first(ix) + 2) if k.one else 0
    for j in range(k.c2_n):
        pack_ref[j * k.c2_rows:(j + 1) * k.c2_rows, :] = c2[start + j]
    row8 = iota((8, k.bz), 0)
    at = k.c2_n * k.c2_rows
    start = (k.yf_first(ix) if k.one else -3) + pad
    for j in range(k.yf_n):
        c = own_lanes(k, jnp.where(iota((8, k.lanes), 0) < 4, b[start + j, SIDE + by:, :], b[start + j, :SIDE, :]))
        pack_ref[at:at + 8, :] = c
        at += 8
    upper = lax.rem(ix, 2) == 0
    first_a = pad + jnp.where(upper, bx, -4)
    first_b = pad + jnp.where(upper, -4, bx)
    for j in range(4):
        xa_ref[j] = own_lanes(k, b[first_a + j, SIDE:SIDE + by, :])
        if xb_ref is not None:
            xb_ref[j] = own_lanes(k, b[first_b + j, SIDE:SIDE + by, :])
    for x in range(bx):
        own_ref[x] = own_lanes(k, b[x + pad, SIDE:SIDE + by, :])


def last_kernel(k, g_ref, own_ref, xa_ref, xb_ref, out_ref, b1, m1, e1, half1, b2, u2, v2, v, m, half_ref):
    ix, iy, iz = place()
    bx, by = k.bx, k.by
    overlap_add(k, g_ref, b1, k.c2_n, k.c2_rows, 0, k.c2_first)
    coarse(k, iz, b1, m1, e1, half1, b2, u2, v2)
    pad = 2
    mask = fine_mask(k, iy, iz)

    def put(j, e):
        for t in range(2):
            plane = -2 + 2 * j + t
            v[pad + plane] = e * (mask * x_inside(k, ix, plane))

    prolonged(k, e1, ix, iy, -1, bx // 2 + 2, half_ref, put)

    def post1(i):
        at = i + pad - 1
        m[at] = mix(v, at) * (mask * x_inside(k, ix, i - 1))

    each(bx + 2, post1)
    base = k.c2_n * k.c2_rows
    low_ok = jnp.where(iy > 0, 1.0, 0.0).astype(jnp.float32)
    high_ok = jnp.where(iy < k.gy - 1, 1.0, 0.0).astype(jnp.float32)
    y_low, y_high = jnp.maximum(iy - 1, 0), jnp.minimum(iy + 1, k.gy - 1)
    row8 = iota((8, k.bz), 0)
    low_keep = jnp.where(row8 < 4, low_ok, 0.0)
    high_keep = jnp.where(row8 >= 4, high_ok, 0.0)
    for x in range(bx):
        out_ref[x] = own_lanes(k, mix(m, x + pad)[SIDE:SIDE + by, :]) + own_ref[x]

    def frame(who, first, x_from, x_to, ok):
        for x in range(x_from, x_to):
            row = base + (x - first) * 8
            if not isinstance(row, int):
                row = pl.multiple_of(row, 8)
            lo = g_ref[who * k.gy + y_low, pl.ds(row, 8), :] * ok
            hi = g_ref[who * k.gy + y_high, pl.ds(row, 8), :] * ok
            out_ref[x, :8, :] += lo * low_keep
            out_ref[x, by - 8:, :] += hi * high_keep

    one = jnp.float32(1.0)
    frame(ix, k.yf_first(ix), 0, bx, one)
    upper = lax.rem(ix, 2) == 0
    if k.one:
        for j in range(3):
            x = jnp.where(ix == 0, bx - 3 + j, j)
            row = pl.multiple_of(base + jnp.where(ix == 0, j, bx + j) * 8, 8)
            lo = g_ref[(1 - ix) * k.gy + y_low, pl.ds(row, 8), :]
            hi = g_ref[(1 - ix) * k.gy + y_high, pl.ds(row, 8), :]
            out_ref[x, :8, :] += lo * low_keep
            out_ref[x, by - 8:, :] += hi * high_keep
    else:
        frame(jnp.maximum(ix - 1, 0), -3 - bx, 0, 3, jnp.where(ix > 0, 1.0, 0.0).astype(jnp.float32))
        frame(jnp.minimum(ix + 1, k.gx - 1), bx - 3, bx - 3, bx, jnp.where(ix < k.gx - 1, 1.0, 0.0).astype(jnp.float32))
    for j in range(4):
        out_ref[jnp.where(upper, bx - 4, 0) + j] += xa_ref[j]
        if xb_ref is not None:
            out_ref[jnp.where(upper, 0, bx - 4) + j] += xb_ref[j]


def call(kernel, outs, scratch, args, flops):
    f32 = lambda s: jax.ShapeDtypeStruct(s, jnp.float32)
    return pl.pallas_call(
        kernel,
        out_shape=[f32(s) for s in outs],
        scratch_shapes=[pltpu.VMEM(s, jnp.float32) for s in scratch],
        compiler_params=pltpu.CompilerParams(vmem_limit_bytes=40 * 1024 * 1024),
        cost_estimate=pl.CostEstimate(flops=flops, bytes_accessed=1 << 20, transcendentals=0),
    )(*args)


def pairs(n):
    first = [(i, i ^ 1) for i in range(n) if (i ^ 1) < n]
    second = [(i + s, i + 1 - s) for i in range(1, n - 1, 2) for s in (0, 1)]
    return first, second


def chain(n, step):
    return [(i, i + step) for i in range(n) if 0 <= i + step < n]


def coarse_scratch(k):
    n1, n2, rows2 = k.nx1, k.nx1 // 2, k.rows1p // 2
    big = (n1 + 4, k.rows1, k.l1)
    return [big, big, big, (n2, k.rows1p, k.l1), (n2, rows2, k.l1), (n2 + 2, rows2, k.l1), (n2 + 2, rows2, k.l1)]


def body(k, pressure, wind):
    bx, by, bz = k.bx, k.by, k.bz
    slab = (bx + -(-bx // 4), by, bz)
    right, left = call(functools.partial(slab_kernel, k), [slab, slab], [], (pressure, wind), 1 << 20)
    low = lax.ppermute(right, "gz", chain(k.gz, 1))
    high = lax.ppermute(left, "gz", chain(k.gz, -1))
    fine = lambda n: (n, k.rows, k.lanes)
    window, send_a, send_b, pack = call(
        functools.partial(first_kernel, k),
        [(bx, by, k.lanes), (bx, 8, k.lanes), (bx, 8, k.lanes), (k.pack1, bz)],
        [fine(bx + 6), fine(bx + 6), (bx // 2 + 2, k.rows, k.l1), (bx // 2 + 2, k.rows // 2, k.l1)],
        (pressure, low, high), 1 << 22)
    ya, yb = pairs(k.gy)
    got_a = lax.ppermute(send_a, "gy", ya)
    got_b = lax.ppermute(send_b, "gy", yb)
    gathered = lax.all_gather(pack, PLANE)
    xa, xb = pairs(k.gx)
    x_outs = [(4, by, bz)] * (2 if xb else 1)
    n_in = 7

    def middle(*refs):
        ins, rest = refs[:n_in], refs[n_in:]
        pack_ref, rest = rest[0], rest[1:]
        xa_ref, rest = rest[0], rest[1:]
        xb_ref = None
        if xb:
            xb_ref, rest = rest[0], rest[1:]
        middle_kernel(k, *ins, pack_ref, xa_ref, xb_ref, *rest)

    big = fine(bx + 10)
    outs = call(
        middle, [(k.pack2, bz)] + x_outs + [(bx, by, bz)],
        coarse_scratch(k) + [big, big, big, (3,) + fine(bx + 2), (3,) + fine(bx + 4),
                             (bx // 2 + 4, k.rows, k.l1), (bx // 2 + 4, k.rows // 2, k.l1)],
        (gathered, window, got_a, got_b, wind, low, high), 1 << 24)
    pack, frames, own = outs[0], outs[1:-1], outs[-1]
    got = [lax.ppermute(f, "gx", perm) for f, perm in zip(frames, (xa, xb))]
    gathered = lax.all_gather(pack, PLANE)

    def last(*refs):
        g_ref, own_ref, xa_ref, rest = refs[0], refs[1], refs[2], refs[3:]
        xb_ref = None
        if xb:
            xb_ref, rest = rest[0], rest[1:]
        last_kernel(k, g_ref, own_ref, xa_ref, xb_ref, *rest)

    (result,) = call(
        last, [(bx, by, bz)],
        coarse_scratch(k) + [fine(bx + 4), fine(bx + 4), (bx // 2 + 2, k.rows, k.l1)],
        (gathered, own, *got), 1 << 23)
    return result


def solution(mesh):
    gx, gy, gz = (mesh.shape[a] for a in ("gx", "gy", "gz"))

    def run(pressure, wind):
        return body(Sizes(gx, gy, gz, *pressure.shape), pressure, wind)

    in_specs = (P("gx", "gy", "gz"), P(None, "gx", "gy", "gz"))
    return jax.shard_map(run, mesh=mesh, in_specs=in_specs, out_specs=P("gx", "gy", "gz"), check_vma=False)
```

```python
import functools

import jax
import jax.numpy as jnp
from jax import lax
from jax.experimental import pallas as pl
from jax.experimental.pallas import tpu as pltpu
from jax.sharding import PartitionSpec as P

OMEGA = 0.8
W = OMEGA / 6.0
C0, C1, C2 = W, 4.0 * W, 16.0 * W
SIDE = 8
PLANE = ("gx", "gy")


def up(v, axis):
    return pltpu.roll(v, v.shape[axis] - 1, axis)


def down(v, axis):
    return pltpu.roll(v, 1, axis)


def mix(s, i):
    c = s[i]
    near = (s[i - 1] + s[i + 1]) + (up(c, 0) + down(c, 0)) + (up(c, 1) + down(c, 1))
    return (1.0 - OMEGA) * c + W * near


def each(n, step):
    lax.fori_loop(0, n, lambda i, _: step(i), None, unroll=True)


def iota(shape, axis):
    return lax.broadcasted_iota(jnp.int32, shape, axis)


def pair_matrix(rows, columns, value):
    hit = (iota((rows, columns), 0) >> 1) == iota((rows, columns), 1)
    return jnp.where(hit, value, 0.0).astype(jnp.float32)


def spread_matrix(rows, columns):
    hit = (iota((rows, columns), 1) >> 1) == iota((rows, columns), 0)
    return jnp.where(hit, 1.0, 0.0).astype(jnp.float32)


def dot(a, b):
    return jnp.dot(a, b, precision=lax.Precision.HIGHEST, preferred_element_type=jnp.float32)


def window_mask(shape, y_first, y_count, z_first, z_count):
    y = iota(shape, 0) + y_first
    z = iota(shape, 1) + z_first
    good = (y >= 0) & (y < y_count) & (z >= 0) & (z < z_count)
    return jnp.where(good, 1.0, 0.0).astype(jnp.float32)


class Sizes:
    def __init__(self, gx, gy, gz, bx, by, bz):
        self.gx, self.gy, self.gz = gx, gy, gz
        self.bx, self.by, self.bz = bx, by, bz
        self.rows, self.lanes = by + 2 * SIDE, 2 * bz
        self.one = gx == 2
        self.c1_n = bx // 2 + (1 if self.one else 2)
        self.c2_n = bx // 2 + (2 if self.one else 4)
        self.yf_n = bx + (3 if self.one else 6)
        self.nx1, self.ny1 = gx * bx // 2, gy * by // 2
        self.rows1 = self.ny1 + SIDE
        self.rows1p = -(-self.rows1 // 16) * 16
        self.l1 = bz
        self.c1_rows = by // 2 + 4
        self.c2_rows = by // 2 + 8
        self.edge = 5
        self.edge_sets = 1 if self.one else 2
        self.pack1 = self.c1_n * self.c1_rows + self.edge_sets * self.edge * 2 * by
        self.pack2 = self.c2_n * self.c2_rows + self.yf_n * 8

    def c1_first(self, i):
        return -i if self.one else -1

    def c2_first(self, i):
        return -2 * i if self.one else -2

    def yf_first(self, i):
        return -3 * i if self.one else -3


def slab_kernel(k, p_ref, w_ref, right_ref, left_ref):
    bx, bz = k.bx, k.bz
    half, part = bz // 2, bz // 4
    lane = iota((k.by, bz), 1)
    for x in range(bx):
        p = pltpu.roll(p_ref[x], half, 1)
        a, b = w_ref[0, x], w_ref[1, x]
        right_ref[x] = jnp.where(lane < half, p, jnp.where(lane < half + part, pltpu.roll(a, bz - part, 1), b))
        left_ref[x] = jnp.where(lane >= half, p, jnp.where(lane < part, a, pltpu.roll(b, part, 1)))
    for q in range(-(-bx // 4)):
        r_all, l_all = jnp.zeros((k.by, bz), jnp.float32), jnp.zeros((k.by, bz), jnp.float32)
        for r in range(min(4, bx - 4 * q)):
            c = w_ref[2, 4 * q + r]
            here = (lane >= part * r) & (lane < part * (r + 1))
            r_all = jnp.where(here, pltpu.roll(c, (part * r + part) % bz, 1), r_all)
            l_all = jnp.where(here, pltpu.roll(c, part * r, 1) if r else c, l_all)
        right_ref[bx + q] = r_all
        left_ref[bx + q] = l_all


def lane_roll(v, shift):
    shift = shift % v.shape[1]
    return pltpu.roll(v, shift, 1) if shift else v


def pressure_window(k, p, low, high):
    half = k.bz // 2
    lane = iota(p.shape, 1)
    p = pltpu.roll(p, half, 1)
    return jnp.concatenate([jnp.where(lane < half, low, p), jnp.where(lane < half, p, high)], axis=1)


def wind_window(k, w, low, low_at, high, high_at):
    half, part = k.bz // 2, k.bz // 4
    lane = iota(w.shape, 1)
    w = pltpu.roll(w, half, 1)
    first = jnp.where(lane >= half, w, jnp.where(lane >= part, lane_roll(low, part - low_at), 0.0))
    second = jnp.where(lane < half, w, jnp.where(lane < half + part, lane_roll(high, half - high_at), 0.0))
    return jnp.concatenate([first, second], axis=1)


def place():
    return lax.axis_index("gx"), lax.axis_index("gy"), lax.axis_index("gz")


def fine_mask(k, iy, iz):
    return window_mask((k.rows, k.lanes), iy * k.by - SIDE, k.gy * k.by, iz * k.bz - k.bz // 2, k.gz * k.bz)


def x_inside(k, ix, plane):
    place_x = ix * k.bx + plane
    return jnp.where((place_x >= 0) & (place_x < k.gx * k.bx), 1.0, 0.0).astype(jnp.float32)


def restrict_planes(src, first, n, half_ref, out, value):
    rows, lanes = src.shape[1], src.shape[2]
    a = pair_matrix(lanes, half_ref.shape[2], value)

    def step(j):
        s = src[first + 2 * j] + src[first + 2 * j + 1]
        half_ref[j] = dot(s + up(s, 0), a)

    for j in range(n):
        step(j)
    for j in range(n):
        out[j] = half_ref[j, pl.ds(0, rows // 2, stride=2), :]


def zero(ref):
    ref[...] = jnp.zeros(ref.shape, ref.dtype)


def first_kernel(k, p_ref, low_ref, high_ref, win_ref, send_a, send_b, pack_ref, b, m, half_ref, c1):
    ix, iy, iz = place()
    bx, by = k.bx, k.by
    pad = 3
    zero(b)
    zero(m)
    for x in range(bx):
        w = pressure_window(k, p_ref[x], low_ref[x], high_ref[x])
        win_ref[x] = w
        b[x + pad, SIDE:SIDE + by, :] = w
    tail = lax.rem(iy, 2) == 0
    for x in range(bx):
        head_rows, tail_rows = win_ref[x, :8, :], win_ref[x, by - 8:, :]
        send_a[x] = jnp.where(tail, tail_rows, head_rows)
        send_b[x] = jnp.where(tail, head_rows, tail_rows)
    mask = fine_mask(k, iy, iz)

    def step1(i):
        m[i + pad - 1] = mix(b, i + pad - 1) * (mask * x_inside(k, ix, i - 1))

    each(bx + 2, step1)

    def step2(i):
        b[i + pad - 2] = mix(m, i + pad - 2)

    each(bx + 4, step2)
    restrict_planes(b, pad - 2, bx // 2 + 2, half_ref, c1, 0.125)
    start = (k.c1_first(ix) + 1) if k.one else 0
    for j in range(k.c1_n):
        pack_ref[j * k.c1_rows:(j + 1) * k.c1_rows, :] = c1[start + j, 2:2 + k.c1_rows, :]
    at = k.c1_n * k.c1_rows
    starts = [(1 - ix) * (bx - k.edge)] if k.one else [0, bx - k.edge]
    for first in starts:
        for j in range(k.edge):
            for t in range(2):
                pack_ref[at:at + by, :] = win_ref[first + j, :, t * k.bz:(t + 1) * k.bz]
                at += by


def coarse(k, iz, b1, m1, e1, half_ref, b2, u2, v2):
    n1, n2 = k.nx1, k.nx1 // 2
    rows1, rows2, l1 = k.rows1, k.rows1p // 2, k.l1
    y0 = -(SIDE // 2)
    mask1 = window_mask((rows1, l1), y0, k.ny1, iz * (k.bz // 2) - k.bz // 4, k.gz * (k.bz // 2))
    lane2 = iota((rows2, l1), 1)
    mask2 = window_mask((rows2, l1), y0 // 2, k.ny1 // 2, iz * (k.bz // 4) - k.bz // 8, k.gz * (k.bz // 4))
    mask2 = jnp.where(lane2 < l1 // 2, mask2, 0.0)
    zero(m1)
    zero(e1)
    zero(u2)
    zero(v2)
    for i in range(n1):
        b1[i + 2] = b1[i + 2] * mask1

    def pre(i):
        c = mix(b1, i + 2) * mask1
        m1[i + 2] = c
        e1[i + 2] = C1 * (b1[i + 2] + c)

    each(n1, pre)
    a = pair_matrix(l1, l1, 0.125)
    for j in range(n2):
        s = mix(m1, 2 * j + 2) + mix(m1, 2 * j + 3)
        half_ref[j, :rows1, :] = dot(s + up(s, 0), a)
        if k.rows1p > rows1:
            half_ref[j, rows1:, :] = jnp.zeros((k.rows1p - rows1, l1), jnp.float32)
    for j in range(n2):
        s = half_ref[j, pl.ds(0, rows2, stride=2), :] * (mask2 * C2)
        b2[j] = s
        u2[j + 1] = s
    src, dst = u2, v2
    for _ in range(3):
        for j in range(n2):
            dst[j + 1] = (mix(src, j + 1) + b2[j]) * mask2
        src, dst = dst, src
    spread = spread_matrix(l1, l1)
    for j in range(n2):
        e = dot(src[j + 1], spread)
        half_ref[j, pl.ds(0, rows2, stride=2), :] = e
        half_ref[j, pl.ds(1, rows2, stride=2), :] = e
    for j in range(n2):
        e = half_ref[j, :rows1, :]
        e1[2 * j + 2] += e
        e1[2 * j + 3] += e
    for src, dst in ((e1, m1), (m1, e1)):

        def post(i):
            dst[i + 2] = (mix(src, i + 2) + C1 * b1[i + 2]) * mask1

        each(n1, post)


def prolonged(k, e1, ix, iy, first, n, half_ref, put):
    by = k.by
    for j in range(n):
        e = e1[ix * (k.bx // 2) + (first + j + 2), pl.ds(pl.multiple_of(iy * (by // 2), 8), k.rows // 2), :]
        half_ref[j, pl.ds(0, k.rows // 2, stride=2), :] = e
        half_ref[j, pl.ds(1, k.rows // 2, stride=2), :] = e
    spread = spread_matrix(k.l1, k.lanes)
    for j in range(n):
        put(j, dot(half_ref[j], spread))


def overlap_add(k, g_ref, b1, n, rows, y_skip, first_of):
    zero(b1)
    for i in range(k.gx):
        for j in range(k.gy):
            at_y = j * (k.by // 2) + y_skip
            for q in range(n):
                x = i * (k.bx // 2) + first_of(i) + q
                if 0 <= x < k.nx1:
                    part = g_ref[i * k.gy + j, q * rows:(q + 1) * rows, :]
                    b1[x + 2, at_y:at_y + rows, :] += part


def own_lanes(k, v):
    half = k.bz // 2
    first, second = v[:, :k.bz], v[:, k.bz:]
    lane = iota(first.shape, 1)
    return jnp.where(lane < half, pltpu.roll(first, half, 1), pltpu.roll(second, half, 1))


def middle_kernel(k, g_ref, win_ref, got_a, got_b, w_ref, low_ref, high_ref, pack_ref, xa_ref, xb_ref, own_ref,
                  b1, m1, e1, half1, b2, u2, v2, b, m, v, vel, flux, half_ref, c2):
    ix, iy, iz = place()
    bx, by = k.bx, k.by
    overlap_add(k, g_ref, b1, k.c1_n, k.c1_rows, 2, k.c1_first)
    coarse(k, iz, b1, m1, e1, half1, b2, u2, v2)
    pad = 5
    mask = fine_mask(k, iy, iz)
    even = lax.rem(iy, 2) == 0
    for x in range(bx):
        b[x + pad, :SIDE, :] = jnp.where(even, got_b[x], got_a[x])
        b[x + pad, SIDE:SIDE + by, :] = win_ref[x]
        b[x + pad, SIDE + by:, :] = jnp.where(even, got_a[x], got_b[x])
    base = k.c1_n * k.c1_rows
    span = k.edge * 2 * by
    y_low, y_high = jnp.maximum(iy - 1, 0), jnp.minimum(iy + 1, k.gy - 1)
    for side in range(2):
        if k.one:
            who, shift = 1 - ix, 0
        else:
            who = jnp.maximum(ix - 1, 0) if side == 0 else jnp.minimum(ix + 1, k.gx - 1)
            shift = span if side == 0 else 0
        for j in range(k.edge):
            at = pad - k.edge + j if side == 0 else pad + bx + j
            for t in range(2):
                row = base + shift + (2 * j + t) * by
                lanes = slice(t * k.bz, (t + 1) * k.bz)
                b[at, :SIDE, lanes] = g_ref[who * k.gy + y_low, row + by - 8:row + by, :]
                b[at, SIDE:SIDE + by, lanes] = g_ref[who * k.gy + iy, row:row + by, :]
                b[at, SIDE + by:, lanes] = g_ref[who * k.gy + y_high, row:row + 8, :]

    def clean(i):
        b[i] = b[i] * (mask * x_inside(k, ix, i - pad))

    each(bx + 2 * pad, clean)

    def put(j, e):
        for t in range(2):
            v[pad - 4 + 2 * j + t] = e

    prolonged(k, e1, ix, iy, -2, bx // 2 + 4, half_ref, put)

    def pre(i):
        at = i + pad - 4
        here = mask * x_inside(k, ix, i - 4)
        v[at] = (v[at] + C0 * (b[at] + mix(b, at))) * here

    each(bx + 8, pre)

    def post1(i):
        at = i + pad - 3
        m[at] = (mix(v, at) + C0 * b[at]) * (mask * x_inside(k, ix, i - 3))

    each(bx + 6, post1)

    def post2(i):
        at = i + pad - 2
        v[at] = (mix(m, at) + C0 * b[at]) * (mask * x_inside(k, ix, i - 2))

    each(bx + 4, post2)

    def speed(i):
        at = i + pad - 1
        here = 0.5 * (mask * x_inside(k, ix, i - 1))
        c = v[at]
        vel[0, i] = (v[at + 1] - v[at - 1]) * here
        vel[1, i] = (up(c, 0) - down(c, 0)) * here
        vel[2, i] = (up(c, 1) - down(c, 1)) * here

    each(bx + 2, speed)
    own_mask = mask[SIDE:SIDE + by, :]
    zero(flux)
    half, part = k.bz // 2, k.bz // 4
    for x in range(bx):
        low, high = low_ref[x], high_ref[x]
        w0 = 0.5 * wind_window(k, w_ref[0, x], low, half, high, 0)
        w1 = 0.5 * wind_window(k, w_ref[1, x], low, half + part, high, part)
        q, r = x // 4, x % 4
        w2 = 0.5 * wind_window(k, w_ref[2, x], low_ref[bx + q], part * r, high_ref[bx + q], part * r)
        for d in range(3):
            c = vel[d, x + 1, SIDE:SIDE + by, :]
            xp, xm = vel[d, x + 2, SIDE:SIDE + by, :], vel[d, x, SIDE:SIDE + by, :]
            yp, ym = vel[d, x + 1, SIDE + 1:SIDE + by + 1, :], vel[d, x + 1, SIDE - 1:SIDE + by - 1, :]
            zp, zm = up(c, 1), down(c, 1)
            near = (xp + xm) + (yp + ym) + (zp + zm)
            total = 7.0 * c - near + w0 * (xp - xm) + w1 * (yp - ym) + w2 * (zp - zm)
            flux[d, x + 2, SIDE:SIDE + by, :] = total * own_mask
    zero(b)
    zero(m)

    def spread_flux(i):
        at = i + pad - 1
        f1, f2 = flux[1, i + 1], flux[2, i + 1]
        total = (flux[0, i + 2] - flux[0, i]) + (up(f1, 0) - down(f1, 0)) + (up(f2, 1) - down(f2, 1))
        b[at] = total * (-0.5 * (mask * x_inside(k, ix, i - 1)))

    each(bx + 2, spread_flux)
    zero(v)

    def power1(i):
        at = i + pad - 2
        c = mix(b, at) * (mask * x_inside(k, ix, i - 2))
        m[at] = c
        b[at] = b[at] + c

    def power1_pure(i):
        at = i + pad - 2
        m[at] = mix(b, at) * (mask * x_inside(k, ix, i - 2))

    each(bx + 4, power1_pure)

    def power2(i):
        at = i + pad - 3
        v[at] = mix(m, at) * (mask * x_inside(k, ix, i - 3))

    each(bx + 6, power2)

    def power3(i):
        at = i + pad - 4
        b[at] = C0 * ((b[at] + m[at]) + (v[at] + mix(v, at))) * (mask * x_inside(k, ix, i - 4))

    each(bx + 8, power3)
    restrict_planes(v, pad - 4, bx // 2 + 4, half_ref, c2, 0.125)
    start = (k.c2_first(ix) + 2) if k.one else 0
    for j in range(k.c2_n):
        pack_ref[j * k.c2_rows:(j + 1) * k.c2_rows, :] = c2[start + j]
    row8 = iota((8, k.bz), 0)
    at = k.c2_n * k.c2_rows
    start = (k.yf_first(ix) if k.one else -3) + pad
    for j in range(k.yf_n):
        c = own_lanes(k, jnp.where(iota((8, k.lanes), 0) < 4, b[start + j, SIDE + by:, :], b[start + j, :SIDE, :]))
        pack_ref[at:at + 8, :] = c
        at += 8
    upper = lax.rem(ix, 2) == 0
    first_a = pad + jnp.where(upper, bx, -4)
    first_b = pad + jnp.where(upper, -4, bx)
    for j in range(4):
        xa_ref[j] = own_lanes(k, b[first_a + j, SIDE:SIDE + by, :])
        if xb_ref is not None:
            xb_ref[j] = own_lanes(k, b[first_b + j, SIDE:SIDE + by, :])
    for x in range(bx):
        own_ref[x] = own_lanes(k, b[x + pad, SIDE:SIDE + by, :])


def last_kernel(k, g_ref, own_ref, xa_ref, xb_ref, out_ref, b1, m1, e1, half1, b2, u2, v2, v, m, half_ref):
    ix, iy, iz = place()
    bx, by = k.bx, k.by
    overlap_add(k, g_ref, b1, k.c2_n, k.c2_rows, 0, k.c2_first)
    coarse(k, iz, b1, m1, e1, half1, b2, u2, v2)
    pad = 2
    mask = fine_mask(k, iy, iz)

    def put(j, e):
        for t in range(2):
            plane = -2 + 2 * j + t
            v[pad + plane] = e * (mask * x_inside(k, ix, plane))

    prolonged(k, e1, ix, iy, -1, bx // 2 + 2, half_ref, put)

    def post1(i):
        at = i + pad - 1
        m[at] = mix(v, at) * (mask * x_inside(k, ix, i - 1))

    each(bx + 2, post1)
    base = k.c2_n * k.c2_rows
    low_ok = jnp.where(iy > 0, 1.0, 0.0).astype(jnp.float32)
    high_ok = jnp.where(iy < k.gy - 1, 1.0, 0.0).astype(jnp.float32)
    y_low, y_high = jnp.maximum(iy - 1, 0), jnp.minimum(iy + 1, k.gy - 1)
    row8 = iota((8, k.bz), 0)
    low_keep = jnp.where(row8 < 4, low_ok, 0.0)
    high_keep = jnp.where(row8 >= 4, high_ok, 0.0)
    for x in range(bx):
        out_ref[x] = own_lanes(k, mix(m, x + pad)[SIDE:SIDE + by, :]) + own_ref[x]

    def frame(who, first, x_from, x_to, ok):
        for x in range(x_from, x_to):
            row = base + (x - first) * 8
            if not isinstance(row, int):
                row = pl.multiple_of(row, 8)
            lo = g_ref[who * k.gy + y_low, pl.ds(row, 8), :] * ok
            hi = g_ref[who * k.gy + y_high, pl.ds(row, 8), :] * ok
            out_ref[x, :8, :] += lo * low_keep
            out_ref[x, by - 8:, :] += hi * high_keep

    one = jnp.float32(1.0)
    frame(ix, k.yf_first(ix), 0, bx, one)
    upper = lax.rem(ix, 2) == 0
    if k.one:
        for j in range(3):
            x = jnp.where(ix == 0, bx - 3 + j, j)
            row = pl.multiple_of(base + jnp.where(ix == 0, j, bx + j) * 8, 8)
            lo = g_ref[(1 - ix) * k.gy + y_low, pl.ds(row, 8), :]
            hi = g_ref[(1 - ix) * k.gy + y_high, pl.ds(row, 8), :]
            out_ref[x, :8, :] += lo * low_keep
            out_ref[x, by - 8:, :] += hi * high_keep
    else:
        frame(jnp.maximum(ix - 1, 0), -3 - bx, 0, 3, jnp.where(ix > 0, 1.0, 0.0).astype(jnp.float32))
        frame(jnp.minimum(ix + 1, k.gx - 1), bx - 3, bx - 3, bx, jnp.where(ix < k.gx - 1, 1.0, 0.0).astype(jnp.float32))
    for j in range(4):
        out_ref[jnp.where(upper, bx - 4, 0) + j] += xa_ref[j]
        if xb_ref is not None:
            out_ref[jnp.where(upper, 0, bx - 4) + j] += xb_ref[j]


def call(kernel, outs, scratch, args, flops):
    f32 = lambda s: jax.ShapeDtypeStruct(s, jnp.float32)
    return pl.pallas_call(
        kernel,
        out_shape=[f32(s) for s in outs],
        scratch_shapes=[pltpu.VMEM(s, jnp.float32) for s in scratch],
        compiler_params=pltpu.CompilerParams(vmem_limit_bytes=40 * 1024 * 1024),
        cost_estimate=pl.CostEstimate(flops=flops, bytes_accessed=1 << 20, transcendentals=0),
    )(*args)


def pairs(n):
    first = [(i, i ^ 1) for i in range(n) if (i ^ 1) < n]
    second = [(i + s, i + 1 - s) for i in range(1, n - 1, 2) for s in (0, 1)]
    return first, second


def chain(n, step):
    return [(i, i + step) for i in range(n) if 0 <= i + step < n]


def coarse_scratch(k):
    n1, n2, rows2 = k.nx1, k.nx1 // 2, k.rows1p // 2
    big = (n1 + 4, k.rows1, k.l1)
    return [big, big, big, (n2, k.rows1p, k.l1), (n2, rows2, k.l1), (n2 + 2, rows2, k.l1), (n2 + 2, rows2, k.l1)]


def body(k, pressure, wind):
    bx, by, bz = k.bx, k.by, k.bz
    slab = (bx + -(-bx // 4), by, bz)
    right, left = call(functools.partial(slab_kernel, k), [slab, slab], [], (pressure, wind), 1 << 20)
    low = lax.ppermute(right, "gz", chain(k.gz, 1))
    high = lax.ppermute(left, "gz", chain(k.gz, -1))
    fine = lambda n: (n, k.rows, k.lanes)
    window, send_a, send_b, pack = call(
        functools.partial(first_kernel, k),
        [(bx, by, k.lanes), (bx, 8, k.lanes), (bx, 8, k.lanes), (k.pack1, bz)],
        [fine(bx + 6), fine(bx + 6), (bx // 2 + 2, k.rows, k.l1), (bx // 2 + 2, k.rows // 2, k.l1)],
        (pressure, low, high), 1 << 22)
    ya, yb = pairs(k.gy)
    got_a = lax.ppermute(send_a, "gy", ya)
    got_b = lax.ppermute(send_b, "gy", yb)
    gathered = lax.all_gather(pack, PLANE)
    xa, xb = pairs(k.gx)
    x_outs = [(4, by, bz)] * (2 if xb else 1)
    n_in = 7

    def middle(*refs):
        ins, rest = refs[:n_in], refs[n_in:]
        pack_ref, rest = rest[0], rest[1:]
        xa_ref, rest = rest[0], rest[1:]
        xb_ref = None
        if xb:
            xb_ref, rest = rest[0], rest[1:]
        middle_kernel(k, *ins, pack_ref, xa_ref, xb_ref, *rest)

    big = fine(bx + 10)
    outs = call(
        middle, [(k.pack2, bz)] + x_outs + [(bx, by, bz)],
        coarse_scratch(k) + [big, big, big, (3,) + fine(bx + 2), (3,) + fine(bx + 4),
                             (bx // 2 + 4, k.rows, k.l1), (bx // 2 + 4, k.rows // 2, k.l1)],
        (gathered, window, got_a, got_b, wind, low, high), 1 << 24)
    pack, frames, own = outs[0], outs[1:-1], outs[-1]
    got = [lax.ppermute(f, "gx", perm) for f, perm in zip(frames, (xa, xb))]
    gathered = lax.all_gather(pack, PLANE)

    def last(*refs):
        g_ref, own_ref, xa_ref, rest = refs[0], refs[1], refs[2], refs[3:]
        xb_ref = None
        if xb:
            xb_ref, rest = rest[0], rest[1:]
        last_kernel(k, g_ref, own_ref, xa_ref, xb_ref, *rest)

    (result,) = call(
        last, [(bx, by, bz)],
        coarse_scratch(k) + [fine(bx + 4), fine(bx + 4), (bx // 2 + 2, k.rows, k.l1)],
        (gathered, own, *got), 1 << 23)
    return result


def solution(mesh):
    gx, gy, gz = (mesh.shape[a] for a in ("gx", "gy", "gz"))

    def run(pressure, wind):
        return body(Sizes(gx, gy, gz, *pressure.shape), pressure, wind)

    in_specs = (P("gx", "gy", "gz"), P(None, "gx", "gy", "gz"))
    return jax.shard_map(run, mesh=mesh, in_specs=in_specs, out_specs=P("gx", "gy", "gz"), check_vma=False)
```

```python
import functools

import jax
import jax.numpy as jnp
from jax import lax
from jax.experimental import pallas as pl
from jax.experimental.pallas import tpu as pltpu
from jax.sharding import PartitionSpec as P

OMEGA = 0.8
W = OMEGA / 6.0
C0, C1, C2 = W, 4.0 * W, 16.0 * W
SIDE = 8
PLANE = ("gx", "gy")


def up(v, axis):
    return pltpu.roll(v, v.shape[axis] - 1, axis)


def down(v, axis):
    return pltpu.roll(v, 1, axis)


def mix(s, i):
    c = s[i]
    near = (s[i - 1] + s[i + 1]) + (up(c, 0) + down(c, 0)) + (up(c, 1) + down(c, 1))
    return (1.0 - OMEGA) * c + W * near


def each(n, step):
    lax.fori_loop(0, n, lambda i, _: step(i), None, unroll=True)


def iota(shape, axis):
    return lax.broadcasted_iota(jnp.int32, shape, axis)


def pair_matrix(rows, columns, value):
    hit = (iota((rows, columns), 0) >> 1) == iota((rows, columns), 1)
    return jnp.where(hit, value, 0.0).astype(jnp.float32)


def spread_matrix(rows, columns):
    hit = (iota((rows, columns), 1) >> 1) == iota((rows, columns), 0)
    return jnp.where(hit, 1.0, 0.0).astype(jnp.float32)


def dot(a, b):
    return jnp.dot(a, b, precision=lax.Precision.HIGHEST, preferred_element_type=jnp.float32)


def window_mask(shape, y_first, y_count, z_first, z_count):
    y = iota(shape, 0) + y_first
    z = iota(shape, 1) + z_first
    good = (y >= 0) & (y < y_count) & (z >= 0) & (z < z_count)
    return jnp.where(good, 1.0, 0.0).astype(jnp.float32)


class Sizes:
    def __init__(self, gx, gy, gz, bx, by, bz):
        self.gx, self.gy, self.gz = gx, gy, gz
        self.bx, self.by, self.bz = bx, by, bz
        self.rows, self.lanes = by + 2 * SIDE, 2 * bz
        self.one = gx == 2
        self.c1_n = bx // 2 + (1 if self.one else 2)
        self.c2_n = bx // 2 + (2 if self.one else 4)
        self.yf_n = bx + (3 if self.one else 6)
        self.nx1, self.ny1 = gx * bx // 2, gy * by // 2
        self.rows1 = self.ny1 + SIDE
        self.rows1p = -(-self.rows1 // 16) * 16
        self.l1 = bz
        self.c1_rows = by // 2 + 4
        self.c2_rows = by // 2 + 8
        self.edge = 5
        self.edge_sets = 1 if self.one else 2
        self.pack1 = self.c1_n * self.c1_rows + self.edge_sets * self.edge * 2 * by
        self.pack2 = self.c2_n * self.c2_rows + self.yf_n * 8

    def c1_first(self, i):
        return -i if self.one else -1

    def c2_first(self, i):
        return -2 * i if self.one else -2

    def yf_first(self, i):
        return -3 * i if self.one else -3


def slab_kernel(k, p_ref, w_ref, right_ref, left_ref):
    bx, bz = k.bx, k.bz
    half, part = bz // 2, bz // 4
    lane = iota((k.by, bz), 1)
    for x in range(bx):
        p = pltpu.roll(p_ref[x], half, 1)
        a, b = w_ref[0, x], w_ref[1, x]
        right_ref[x] = jnp.where(lane < half, p, jnp.where(lane < half + part, pltpu.roll(a, bz - part, 1), b))
        left_ref[x] = jnp.where(lane >= half, p, jnp.where(lane < part, a, pltpu.roll(b, part, 1)))
    for q in range(-(-bx // 4)):
        r_all, l_all = jnp.zeros((k.by, bz), jnp.float32), jnp.zeros((k.by, bz), jnp.float32)
        for r in range(min(4, bx - 4 * q)):
            c = w_ref[2, 4 * q + r]
            here = (lane >= part * r) & (lane < part * (r + 1))
            r_all = jnp.where(here, pltpu.roll(c, (part * r + part) % bz, 1), r_all)
            l_all = jnp.where(here, pltpu.roll(c, part * r, 1) if r else c, l_all)
        right_ref[bx + q] = r_all
        left_ref[bx + q] = l_all


def lane_roll(v, shift):
    shift = shift % v.shape[1]
    return pltpu.roll(v, shift, 1) if shift else v


def pressure_window(k, p, low, high):
    half = k.bz // 2
    lane = iota(p.shape, 1)
    p = pltpu.roll(p, half, 1)
    return jnp.concatenate([jnp.where(lane < half, low, p), jnp.where(lane < half, p, high)], axis=1)


def wind_window(k, w, low, low_at, high, high_at):
    half, part = k.bz // 2, k.bz // 4
    lane = iota(w.shape, 1)
    w = pltpu.roll(w, half, 1)
    first = jnp.where(lane >= half, w, jnp.where(lane >= part, lane_roll(low, part - low_at), 0.0))
    second = jnp.where(lane < half, w, jnp.where(lane < half + part, lane_roll(high, half - high_at), 0.0))
    return jnp.concatenate([first, second], axis=1)


def place():
    return lax.axis_index("gx"), lax.axis_index("gy"), lax.axis_index("gz")


def fine_mask(k, iy, iz):
    return window_mask((k.rows, k.lanes), iy * k.by - SIDE, k.gy * k.by, iz * k.bz - k.bz // 2, k.gz * k.bz)


def x_inside(k, ix, plane):
    place_x = ix * k.bx + plane
    return jnp.where((place_x >= 0) & (place_x < k.gx * k.bx), 1.0, 0.0).astype(jnp.float32)


def restrict_planes(src, first, n, half_ref, out, value):
    rows, lanes = src.shape[1], src.shape[2]
    a = pair_matrix(lanes, half_ref.shape[2], value)

    def step(j):
        s = src[first + 2 * j] + src[first + 2 * j + 1]
        half_ref[j] = dot(s + up(s, 0), a)

    for j in range(n):
        step(j)
    for j in range(n):
        out[j] = half_ref[j, pl.ds(0, rows // 2, stride=2), :]


def zero(ref):
    ref[...] = jnp.zeros(ref.shape, ref.dtype)


def first_kernel(k, p_ref, low_ref, high_ref, win_ref, send_a, send_b, pack_ref, b, m, half_ref, c1):
    ix, iy, iz = place()
    bx, by = k.bx, k.by
    pad = 3
    zero(b)
    zero(m)
    for x in range(bx):
        w = pressure_window(k, p_ref[x], low_ref[x], high_ref[x])
        win_ref[x] = w
        b[x + pad, SIDE:SIDE + by, :] = w
    tail = lax.rem(iy, 2) == 0
    for x in range(bx):
        head_rows, tail_rows = win_ref[x, :8, :], win_ref[x, by - 8:, :]
        send_a[x] = jnp.where(tail, tail_rows, head_rows)
        send_b[x] = jnp.where(tail, head_rows, tail_rows)
    mask = fine_mask(k, iy, iz)

    def step1(i):
        m[i + pad - 1] = mix(b, i + pad - 1) * (mask * x_inside(k, ix, i - 1))

    each(bx + 2, step1)

    def step2(i):
        b[i + pad - 2] = mix(m, i + pad - 2)

    each(bx + 4, step2)
    restrict_planes(b, pad - 2, bx // 2 + 2, half_ref, c1, 0.125)
    start = (k.c1_first(ix) + 1) if k.one else 0
    for j in range(k.c1_n):
        pack_ref[j * k.c1_rows:(j + 1) * k.c1_rows, :] = c1[start + j, 2:2 + k.c1_rows, :]
    at = k.c1_n * k.c1_rows
    starts = [(1 - ix) * (bx - k.edge)] if k.one else [0, bx - k.edge]
    for first in starts:
        for j in range(k.edge):
            for t in range(2):
                pack_ref[at:at + by, :] = win_ref[first + j, :, t * k.bz:(t + 1) * k.bz]
                at += by


def coarse(k, iz, b1, m1, e1, half_ref, b2, u2, v2):
    n1, n2 = k.nx1, k.nx1 // 2
    rows1, rows2, l1 = k.rows1, k.rows1p // 2, k.l1
    y0 = -(SIDE // 2)
    mask1 = window_mask((rows1, l1), y0, k.ny1, iz * (k.bz // 2) - k.bz // 4, k.gz * (k.bz // 2))
    lane2 = iota((rows2, l1), 1)
    mask2 = window_mask((rows2, l1), y0 // 2, k.ny1 // 2, iz * (k.bz // 4) - k.bz // 8, k.gz * (k.bz // 4))
    mask2 = jnp.where(lane2 < l1 // 2, mask2, 0.0)
    zero(m1)
    zero(e1)
    zero(u2)
    zero(v2)
    for i in range(n1):
        b1[i + 2] = b1[i + 2] * mask1

    def pre(i):
        c = mix(b1, i + 2) * mask1
        m1[i + 2] = c
        e1[i + 2] = C1 * (b1[i + 2] + c)

    each(n1, pre)
    a = pair_matrix(l1, l1, 0.125)
    for j in range(n2):
        s = mix(m1, 2 * j + 2) + mix(m1, 2 * j + 3)
        half_ref[j, :rows1, :] = dot(s + up(s, 0), a)
        if k.rows1p > rows1:
            half_ref[j, rows1:, :] = jnp.zeros((k.rows1p - rows1, l1), jnp.float32)
    for j in range(n2):
        s = half_ref[j, pl.ds(0, rows2, stride=2), :] * (mask2 * C2)
        b2[j] = s
        u2[j + 1] = s
    src, dst = u2, v2
    for _ in range(3):
        for j in range(n2):
            dst[j + 1] = (mix(src, j + 1) + b2[j]) * mask2
        src, dst = dst, src
    spread = spread_matrix(l1, l1)
    for j in range(n2):
        e = dot(src[j + 1], spread)
        half_ref[j, pl.ds(0, rows2, stride=2), :] = e
        half_ref[j, pl.ds(1, rows2, stride=2), :] = e
    for j in range(n2):
        e = half_ref[j, :rows1, :]
        e1[2 * j + 2] += e
        e1[2 * j + 3] += e
    for src, dst in ((e1, m1), (m1, e1)):

        def post(i):
            dst[i + 2] = (mix(src, i + 2) + C1 * b1[i + 2]) * mask1

        each(n1, post)


def prolonged(k, e1, ix, iy, first, n, half_ref, put):
    by = k.by
    for j in range(n):
        e = e1[ix * (k.bx // 2) + (first + j + 2), pl.ds(pl.multiple_of(iy * (by // 2), 8), k.rows // 2), :]
        half_ref[j, pl.ds(0, k.rows // 2, stride=2), :] = e
        half_ref[j, pl.ds(1, k.rows // 2, stride=2), :] = e
    spread = spread_matrix(k.l1, k.lanes)
    for j in range(n):
        put(j, dot(half_ref[j], spread))


def overlap_add(k, g_ref, b1, n, rows, y_skip, first_of):
    zero(b1)
    for i in range(k.gx):
        for j in range(k.gy):
            at_y = j * (k.by // 2) + y_skip
            for q in range(n):
                x = i * (k.bx // 2) + first_of(i) + q
                if 0 <= x < k.nx1:
                    part = g_ref[i * k.gy + j, q * rows:(q + 1) * rows, :]
                    b1[x + 2, at_y:at_y + rows, :] += part


def own_lanes(k, v):
    half = k.bz // 2
    first, second = v[:, :k.bz], v[:, k.bz:]
    lane = iota(first.shape, 1)
    return jnp.where(lane < half, pltpu.roll(first, half, 1), pltpu.roll(second, half, 1))


def assemble_edges(k, refs, b1, b, pad):
    g_ref, win_ref, got_a, got_b, w_ref, low_ref, high_ref = refs
    ix, iy, iz = place()
    bx, by = k.bx, k.by
    overlap_add(k, g_ref, b1, k.c1_n, k.c1_rows, 2, k.c1_first)
    even = lax.rem(iy, 2) == 0
    for x in range(bx):
        b[x + pad, :SIDE, :] = jnp.where(even, got_b[x], got_a[x])
        b[x + pad, SIDE:SIDE + by, :] = win_ref[x]
        b[x + pad, SIDE + by:, :] = jnp.where(even, got_a[x], got_b[x])
    base = k.c1_n * k.c1_rows
    span = k.edge * 2 * by
    y_low, y_high = jnp.maximum(iy - 1, 0), jnp.minimum(iy + 1, k.gy - 1)
    for side in range(2):
        if k.one:
            who, shift = 1 - ix, 0
        else:
            who = jnp.maximum(ix - 1, 0) if side == 0 else jnp.minimum(ix + 1, k.gx - 1)
            shift = span if side == 0 else 0
        for j in range(k.edge):
            at = pad - k.edge + j if side == 0 else pad + bx + j
            for t in range(2):
                row = base + shift + (2 * j + t) * by
                lanes = slice(t * k.bz, (t + 1) * k.bz)
                b[at, :SIDE, lanes] = g_ref[who * k.gy + y_low, row + by - 8:row + by, :]
                b[at, SIDE:SIDE + by, lanes] = g_ref[who * k.gy + iy, row:row + by, :]
                b[at, SIDE + by:, lanes] = g_ref[who * k.gy + y_high, row:row + 8, :]
    half, part = k.bz // 2, k.bz // 4

    def winds(x):
        low, high = low_ref[x], high_ref[x]
        q, r = x // 4, x % 4
        return (wind_window(k, w_ref[0, x], low, half, high, 0),
                wind_window(k, w_ref[1, x], low, half + part, high, part),
                wind_window(k, w_ref[2, x], low_ref[bx + q], part * r, high_ref[bx + q], part * r))

    return winds


def slab_places(k):
    groups = lambda n: -(-n // 4)
    rows1 = k.ny1
    fine_n = k.bx + k.edge if k.one else k.bx + 2 * k.edge
    at_fine = groups(k.nx1) * rows1
    at_wind = at_fine + groups(fine_n) * k.rows
    return fine_n, at_fine, at_wind, at_wind + groups(3 * k.bx) * k.by


def take_slab(k, ref, base, rows, i, to):
    part = k.bz // 4
    at = base + (i // 4) * rows
    return lane_roll(ref[at:at + rows, :], to - part * (i % 4))


def assemble_plane(k, refs, b1, b, pad):
    c1_ref, win_ref, w_ref, low_ref, high_ref = refs
    ix, iy, iz = place()
    bx, by = k.bx, k.by
    half, part = k.bz // 2, k.bz // 4
    fine_n, at_fine, at_wind, _ = slab_places(k)
    zero(b1)
    top = SIDE // 2
    lane = iota((k.ny1, k.l1), 1)
    for x in range(k.nx1):
        low = take_slab(k, low_ref, 0, k.ny1, x, 1)
        high = take_slab(k, high_ref, 0, k.ny1, x, 3 * part - 1)
        low = jnp.where((lane >= 1) & (lane <= part), low, 0.0)
        high = jnp.where((lane >= 3 * part - 1) & (lane < 4 * part - 1), high, 0.0)
        b1[x + 2, top:top + k.ny1, :] = c1_ref[x] + (low + high)
    lane = iota((k.rows, k.bz), 1)
    zero(b)
    first = -k.edge * ix if k.one else -k.edge
    for j in range(fine_n):
        p = pltpu.roll(win_ref[j], half, 1)
        low = take_slab(k, low_ref, at_fine, k.rows, j, part)
        high = take_slab(k, high_ref, at_fine, k.rows, j, half)
        at = first + j + pad
        b[at, :, :k.bz] = jnp.where(lane >= half, p, jnp.where(lane >= part, low, 0.0))
        b[at, :, k.bz:] = jnp.where(lane < half, p, jnp.where(lane < half + part, high, 0.0))
    lane_w = iota((by, k.bz), 1)

    def winds(x):
        found = []
        for d in range(3):
            w = pltpu.roll(w_ref[d, x], half, 1)
            low = take_slab(k, low_ref, at_wind, by, d * bx + x, part)
            high = take_slab(k, high_ref, at_wind, by, d * bx + x, half)
            found.append(jnp.concatenate(
                [jnp.where(lane_w >= half, w, jnp.where(lane_w >= part, low, 0.0)),
                 jnp.where(lane_w < half, w, jnp.where(lane_w < half + part, high, 0.0))], axis=1))
        return found

    return winds


def plane_kernel(k, g_ref, w_ref, c1_ref, win_ref, right_ref, left_ref, p, m, q, half_ref):
    ix, iy, iz = place()
    bx, by, bz = k.bx, k.by, k.bz
    nx, ny = k.gx * bx, k.gy * by
    half, part = bz // 2, bz // 4
    pad_x = k.edge
    fine_n, at_fine, at_wind, _ = slab_places(k)
    for i in range(pad_x):
        p[i] = jnp.zeros(p.shape[1:], jnp.float32)
        p[pad_x + nx + i] = jnp.zeros(p.shape[1:], jnp.float32)
    for x in range(nx):
        p[pad_x + x, :SIDE, :] = jnp.zeros((SIDE, bz), jnp.float32)
        p[pad_x + x, SIDE + ny:, :] = jnp.zeros((SIDE, bz), jnp.float32)
        for j in range(k.gy):
            p[pad_x + x, SIDE + j * by:SIDE + (j + 1) * by, :] = g_ref[(x // bx) * k.gy + j, x % bx]
    zero(m)
    lane = iota((ny + SIDE, bz), 1)
    not_last = jnp.where(lane < bz - 1, 1.0, 0.0).astype(jnp.float32)
    not_first = jnp.where(lane > 0, 1.0, 0.0).astype(jnp.float32)
    last_ok = jnp.where(iz < k.gz - 1, W * W, 0.0).astype(jnp.float32)
    first_ok = jnp.where(iz > 0, W * W, 0.0).astype(jnp.float32)
    ends = (1.0 - not_last) * last_ok + (1.0 - not_first) * first_ok
    for x in range(nx):
        c = p[pad_x + x, SIDE:, :]
        four = (p[pad_x + x - 1, SIDE:, :] + p[pad_x + x + 1, SIDE:, :]) + (up(c, 0) + down(c, 0))
        along = up(c, 1) * not_last + down(c, 1) * not_first
        mixed = (1.0 - OMEGA) * c + W * (four + along)
        m[x + 1, :ny, :] = mixed[:ny]
        q[x] = ((1.0 - OMEGA + W) * W * c + W * mixed + (W * W) * four)[:ny]

    def twice(x):
        c = m[x + 1]
        four = (m[x] + m[x + 2]) + (up(c, 0) + down(c, 0))
        along = up(c, 1) * not_last + down(c, 1) * not_first
        return ((1.0 - OMEGA) * c + W * (four + along) + ends * p[pad_x + x, SIDE:, :])[:ny]

    row, column = iota((bz, k.l1), 0), iota((bz, k.l1), 1)
    own = jnp.where((row >> 1) + part == column, 0.125, 0.0).astype(jnp.float32)
    rim = ((row == 0) & (column == part - 1)) | ((row == bz - 1) & (column == 3 * part))
    rim = jnp.where(rim, 0.125, 0.0).astype(jnp.float32)
    for j in range(k.nx1):
        s = twice(2 * j) + twice(2 * j + 1)
        t = q[2 * j] + q[2 * j + 1]
        half_ref[j] = dot(s + up(s, 0), own) + dot(t + up(t, 0), rim)
    for j in range(k.nx1):
        c1_ref[j] = half_ref[j, pl.ds(0, k.ny1, stride=2), :]

    def pack(ref, base, rows, n, load, from_lane):
        lane = iota((rows, bz), 1)
        for group in range(-(-n // 4)):
            total = jnp.zeros((rows, bz), jnp.float32)
            for r in range(min(4, n - 4 * group)):
                moved = lane_roll(load(4 * group + r), part * r - from_lane)
                total = jnp.where((lane >= part * r) & (lane < part * (r + 1)), moved, total)
            ref[base + group * rows:base + (group + 1) * rows, :] = total

    first = ix * (bx - k.edge) + pad_x if k.one else ix * bx + pad_x - k.edge
    for j in range(fine_n):
        win_ref[j] = p[first + j, pl.ds(pl.multiple_of(iy * by, 8), k.rows), :]
    for ref, lane1, lane0 in ((right_ref, 2 * part + 1, 3 * part), (left_ref, part - 1, 0)):
        pack(ref, 0, k.ny1, k.nx1, lambda i: c1_ref[i], lane1)
        pack(ref, at_fine, k.rows, fine_n, lambda i: win_ref[i], lane0)
        pack(ref, at_wind, by, 3 * bx, lambda i: w_ref[i // bx, i % bx], lane0)


def middle_kernel(k, assemble, ins, pack_ref, xa_ref, xb_ref, own_ref,
                  b1, m1, e1, half1, b2, u2, v2, b, m, v, vel, flux, half_ref, c2):
    ix, iy, iz = place()
    bx, by = k.bx, k.by
    pad = 5
    winds = assemble(k, ins, b1, b, pad)
    coarse(k, iz, b1, m1, e1, half1, b2, u2, v2)
    mask = fine_mask(k, iy, iz)

    def clean(i):
        b[i] = b[i] * (mask * x_inside(k, ix, i - pad))

    each(bx + 2 * pad, clean)

    def put(j, e):
        for t in range(2):
            v[pad - 4 + 2 * j + t] = e

    prolonged(k, e1, ix, iy, -2, bx // 2 + 4, half_ref, put)

    def pre(i):
        at = i + pad - 4
        here = mask * x_inside(k, ix, i - 4)
        v[at] = (v[at] + C0 * (b[at] + mix(b, at))) * here

    each(bx + 8, pre)

    def post1(i):
        at = i + pad - 3
        m[at] = (mix(v, at) + C0 * b[at]) * (mask * x_inside(k, ix, i - 3))

    each(bx + 6, post1)

    def post2(i):
        at = i + pad - 2
        v[at] = (mix(m, at) + C0 * b[at]) * (mask * x_inside(k, ix, i - 2))

    each(bx + 4, post2)

    def speed(i):
        at = i + pad - 1
        here = 0.5 * (mask * x_inside(k, ix, i - 1))
        c = v[at]
        vel[0, i] = (v[at + 1] - v[at - 1]) * here
        vel[1, i] = (up(c, 0) - down(c, 0)) * here
        vel[2, i] = (up(c, 1) - down(c, 1)) * here

    each(bx + 2, speed)
    own_mask = mask[SIDE:SIDE + by, :]
    zero(flux)
    for x in range(bx):
        w0, w1, w2 = (0.5 * w for w in winds(x))
        for d in range(3):
            c = vel[d, x + 1, SIDE:SIDE + by, :]
            xp, xm = vel[d, x + 2, SIDE:SIDE + by, :], vel[d, x, SIDE:SIDE + by, :]
            yp, ym = vel[d, x + 1, SIDE + 1:SIDE + by + 1, :], vel[d, x + 1, SIDE - 1:SIDE + by - 1, :]
            zp, zm = up(c, 1), down(c, 1)
            near = (xp + xm) + (yp + ym) + (zp + zm)
            total = 7.0 * c - near + w0 * (xp - xm) + w1 * (yp - ym) + w2 * (zp - zm)
            flux[d, x + 2, SIDE:SIDE + by, :] = total * own_mask
    zero(b)
    zero(m)

    def spread_flux(i):
        at = i + pad - 1
        f1, f2 = flux[1, i + 1], flux[2, i + 1]
        total = (flux[0, i + 2] - flux[0, i]) + (up(f1, 0) - down(f1, 0)) + (up(f2, 1) - down(f2, 1))
        b[at] = total * (-0.5 * (mask * x_inside(k, ix, i - 1)))

    each(bx + 2, spread_flux)
    zero(v)

    def power1_pure(i):
        at = i + pad - 2
        m[at] = mix(b, at) * (mask * x_inside(k, ix, i - 2))

    each(bx + 4, power1_pure)

    def power2(i):
        at = i + pad - 3
        v[at] = mix(m, at) * (mask * x_inside(k, ix, i - 3))

    each(bx + 6, power2)

    def power3(i):
        at = i + pad - 4
        b[at] = C0 * ((b[at] + m[at]) + (v[at] + mix(v, at))) * (mask * x_inside(k, ix, i - 4))

    each(bx + 8, power3)
    restrict_planes(v, pad - 4, bx // 2 + 4, half_ref, c2, 0.125)
    start = (k.c2_first(ix) + 2) if k.one else 0
    for j in range(k.c2_n):
        pack_ref[j * k.c2_rows:(j + 1) * k.c2_rows, :] = c2[start + j]
    row8 = iota((8, k.bz), 0)
    at = k.c2_n * k.c2_rows
    start = (k.yf_first(ix) if k.one else -3) + pad
    for j in range(k.yf_n):
        c = own_lanes(k, jnp.where(iota((8, k.lanes), 0) < 4, b[start + j, SIDE + by:, :], b[start + j, :SIDE, :]))
        pack_ref[at:at + 8, :] = c
        at += 8
    upper = lax.rem(ix, 2) == 0
    first_a = pad + jnp.where(upper, bx, -4)
    first_b = pad + jnp.where(upper, -4, bx)
    for j in range(4):
        xa_ref[j] = own_lanes(k, b[first_a + j, SIDE:SIDE + by, :])
        if xb_ref is not None:
            xb_ref[j] = own_lanes(k, b[first_b + j, SIDE:SIDE + by, :])
    for x in range(bx):
        own_ref[x] = own_lanes(k, b[x + pad, SIDE:SIDE + by, :])


def last_kernel(k, g_ref, own_ref, xa_ref, xb_ref, out_ref, b1, m1, e1, half1, b2, u2, v2, v, m, half_ref):
    ix, iy, iz = place()
    bx, by = k.bx, k.by
    overlap_add(k, g_ref, b1, k.c2_n, k.c2_rows, 0, k.c2_first)
    coarse(k, iz, b1, m1, e1, half1, b2, u2, v2)
    pad = 2
    mask = fine_mask(k, iy, iz)

    def put(j, e):
        for t in range(2):
            plane = -2 + 2 * j + t
            v[pad + plane] = e * (mask * x_inside(k, ix, plane))

    prolonged(k, e1, ix, iy, -1, bx // 2 + 2, half_ref, put)

    def post1(i):
        at = i + pad - 1
        m[at] = mix(v, at) * (mask * x_inside(k, ix, i - 1))

    each(bx + 2, post1)
    base = k.c2_n * k.c2_rows
    low_ok = jnp.where(iy > 0, 1.0, 0.0).astype(jnp.float32)
    high_ok = jnp.where(iy < k.gy - 1, 1.0, 0.0).astype(jnp.float32)
    y_low, y_high = jnp.maximum(iy - 1, 0), jnp.minimum(iy + 1, k.gy - 1)
    row8 = iota((8, k.bz), 0)
    low_keep = jnp.where(row8 < 4, low_ok, 0.0)
    high_keep = jnp.where(row8 >= 4, high_ok, 0.0)
    for x in range(bx):
        out_ref[x] = own_lanes(k, mix(m, x + pad)[SIDE:SIDE + by, :]) + own_ref[x]

    def frame(who, first, x_from, x_to, ok):
        for x in range(x_from, x_to):
            row = base + (x - first) * 8
            if not isinstance(row, int):
                row = pl.multiple_of(row, 8)
            lo = g_ref[who * k.gy + y_low, pl.ds(row, 8), :] * ok
            hi = g_ref[who * k.gy + y_high, pl.ds(row, 8), :] * ok
            out_ref[x, :8, :] += lo * low_keep
            out_ref[x, by - 8:, :] += hi * high_keep

    one = jnp.float32(1.0)
    frame(ix, k.yf_first(ix), 0, bx, one)
    upper = lax.rem(ix, 2) == 0
    if k.one:
        for j in range(3):
            x = jnp.where(ix == 0, bx - 3 + j, j)
            row = pl.multiple_of(base + jnp.where(ix == 0, j, bx + j) * 8, 8)
            lo = g_ref[(1 - ix) * k.gy + y_low, pl.ds(row, 8), :]
            hi = g_ref[(1 - ix) * k.gy + y_high, pl.ds(row, 8), :]
            out_ref[x, :8, :] += lo * low_keep
            out_ref[x, by - 8:, :] += hi * high_keep
    else:
        frame(jnp.maximum(ix - 1, 0), -3 - bx, 0, 3, jnp.where(ix > 0, 1.0, 0.0).astype(jnp.float32))
        frame(jnp.minimum(ix + 1, k.gx - 1), bx - 3, bx - 3, bx, jnp.where(ix < k.gx - 1, 1.0, 0.0).astype(jnp.float32))
    for j in range(4):
        out_ref[jnp.where(upper, bx - 4, 0) + j] += xa_ref[j]
        if xb_ref is not None:
            out_ref[jnp.where(upper, 0, bx - 4) + j] += xb_ref[j]


def call(kernel, outs, scratch, args, flops):
    f32 = lambda s: jax.ShapeDtypeStruct(s, jnp.float32)
    return pl.pallas_call(
        kernel,
        out_shape=[f32(s) for s in outs],
        scratch_shapes=[pltpu.VMEM(s, jnp.float32) for s in scratch],
        compiler_params=pltpu.CompilerParams(vmem_limit_bytes=40 * 1024 * 1024),
        cost_estimate=pl.CostEstimate(flops=flops, bytes_accessed=1 << 20, transcendentals=0),
    )(*args)


def pairs(n):
    first = [(i, i ^ 1) for i in range(n) if (i ^ 1) < n]
    second = [(i + s, i + 1 - s) for i in range(1, n - 1, 2) for s in (0, 1)]
    return first, second


def chain(n, step):
    return [(i, i + step) for i in range(n) if 0 <= i + step < n]


def coarse_scratch(k):
    n1, n2, rows2 = k.nx1, k.nx1 // 2, k.rows1p // 2
    big = (n1 + 4, k.rows1, k.l1)
    return [big, big, big, (n2, k.rows1p, k.l1), (n2, rows2, k.l1), (n2 + 2, rows2, k.l1), (n2 + 2, rows2, k.l1)]


def edge_form(k, pressure, wind):
    bx, by, bz = k.bx, k.by, k.bz
    slab = (bx + -(-bx // 4), by, bz)
    right, left = call(functools.partial(slab_kernel, k), [slab, slab], [], (pressure, wind), 1 << 20)
    low = lax.ppermute(right, "gz", chain(k.gz, 1))
    high = lax.ppermute(left, "gz", chain(k.gz, -1))
    fine = lambda n: (n, k.rows, k.lanes)
    window, send_a, send_b, pack = call(
        functools.partial(first_kernel, k),
        [(bx, by, k.lanes), (bx, 8, k.lanes), (bx, 8, k.lanes), (k.pack1, bz)],
        [fine(bx + 6), fine(bx + 6), (bx // 2 + 2, k.rows, k.l1), (bx // 2 + 2, k.rows // 2, k.l1)],
        (pressure, low, high), 1 << 22)
    ya, yb = pairs(k.gy)
    got_a = lax.ppermute(send_a, "gy", ya)
    got_b = lax.ppermute(send_b, "gy", yb)
    gathered = lax.all_gather(pack, PLANE)
    return assemble_edges, (gathered, window, got_a, got_b, wind, low, high)


def plane_form(k, pressure, wind):
    bx, by, bz = k.bx, k.by, k.bz
    nx, ny = k.gx * bx, k.gy * by
    gathered = lax.all_gather(pressure, PLANE)
    fine_n, _, _, slab_rows = slab_places(k)
    c1, window, right, left = call(
        functools.partial(plane_kernel, k),
        [(k.nx1, k.ny1, k.l1), (fine_n, k.rows, bz), (slab_rows, bz), (slab_rows, bz)],
        [(nx + 2 * k.edge, ny + 2 * SIDE, bz), (nx + 2, ny + SIDE, bz), (nx, ny, bz), (k.nx1, ny, k.l1)],
        (gathered, wind), 1 << 22)
    low = lax.ppermute(right, "gz", chain(k.gz, 1))
    high = lax.ppermute(left, "gz", chain(k.gz, -1))
    return assemble_plane, (c1, window, wind, low, high)


def body(k, pressure, wind):
    bx, by, bz = k.bx, k.by, k.bz
    fine = lambda n: (n, k.rows, k.lanes)
    small_plane = k.gx * k.gy * bx * by * bz * 4 <= 1 << 20
    assemble, args = (plane_form if small_plane else edge_form)(k, pressure, wind)
    xa, xb = pairs(k.gx)
    x_outs = [(4, by, bz)] * (2 if xb else 1)

    def middle(*refs):
        ins, rest = refs[:len(args)], refs[len(args):]
        pack_ref, rest = rest[0], rest[1:]
        xa_ref, rest = rest[0], rest[1:]
        xb_ref = None
        if xb:
            xb_ref, rest = rest[0], rest[1:]
        middle_kernel(k, assemble, ins, pack_ref, xa_ref, xb_ref, *rest)

    big = fine(bx + 10)
    outs = call(
        middle, [(k.pack2, bz)] + x_outs + [(bx, by, bz)],
        coarse_scratch(k) + [big, big, big, (3,) + fine(bx + 2), (3,) + fine(bx + 4),
                             (bx // 2 + 4, k.rows, k.l1), (bx // 2 + 4, k.rows // 2, k.l1)],
        args, 1 << 24)
    pack, frames, own = outs[0], outs[1:-1], outs[-1]
    got = [lax.ppermute(f, "gx", perm) for f, perm in zip(frames, (xa, xb))]
    gathered = lax.all_gather(pack, PLANE)

    def last(*refs):
        g_ref, own_ref, xa_ref, rest = refs[0], refs[1], refs[2], refs[3:]
        xb_ref = None
        if xb:
            xb_ref, rest = rest[0], rest[1:]
        last_kernel(k, g_ref, own_ref, xa_ref, xb_ref, *rest)

    (result,) = call(
        last, [(bx, by, bz)],
        coarse_scratch(k) + [fine(bx + 4), fine(bx + 4), (bx // 2 + 2, k.rows, k.l1)],
        (gathered, own, *got), 1 << 23)
    return result


def solution(mesh):
    gx, gy, gz = (mesh.shape[a] for a in ("gx", "gy", "gz"))

    def run(pressure, wind):
        return body(Sizes(gx, gy, gz, *pressure.shape), pressure, wind)

    in_specs = (P("gx", "gy", "gz"), P(None, "gx", "gy", "gz"))
    return jax.shard_map(run, mesh=mesh, in_specs=in_specs, out_specs=P("gx", "gy", "gz"), check_vma=False)
```

```python
import functools

import jax
import jax.numpy as jnp
from jax import lax
from jax.experimental import pallas as pl
from jax.experimental.pallas import tpu as pltpu
from jax.sharding import PartitionSpec as P

OMEGA = 0.8
W = OMEGA / 6.0
C0, C1, C2 = W, 4.0 * W, 16.0 * W
SIDE = 8
PLANE = ("gx", "gy")


def up(v, axis):
    return pltpu.roll(v, v.shape[axis] - 1, axis)


def down(v, axis):
    return pltpu.roll(v, 1, axis)


def mix(s, i):
    c = s[i]
    near = (s[i - 1] + s[i + 1]) + (up(c, 0) + down(c, 0)) + (up(c, 1) + down(c, 1))
    return (1.0 - OMEGA) * c + W * near


def each(n, step):
    lax.fori_loop(0, n, lambda i, _: step(i), None, unroll=True)


def iota(shape, axis):
    return lax.broadcasted_iota(jnp.int32, shape, axis)


def pair_matrix(rows, columns, value):
    hit = (iota((rows, columns), 0) >> 1) == iota((rows, columns), 1)
    return jnp.where(hit, value, 0.0).astype(jnp.float32)


def spread_matrix(rows, columns):
    hit = (iota((rows, columns), 1) >> 1) == iota((rows, columns), 0)
    return jnp.where(hit, 1.0, 0.0).astype(jnp.float32)


def dot(a, b):
    return jnp.dot(a, b, precision=lax.Precision.HIGHEST, preferred_element_type=jnp.float32)


def window_mask(shape, y_first, y_count, z_first, z_count):
    y = iota(shape, 0) + y_first
    z = iota(shape, 1) + z_first
    good = (y >= 0) & (y < y_count) & (z >= 0) & (z < z_count)
    return jnp.where(good, 1.0, 0.0).astype(jnp.float32)


class Sizes:
    def __init__(self, gx, gy, gz, bx, by, bz):
        self.gx, self.gy, self.gz = gx, gy, gz
        self.bx, self.by, self.bz = bx, by, bz
        self.rows, self.lanes = by + 2 * SIDE, 2 * bz
        self.one = gx == 2
        self.c1_n = bx // 2 + (1 if self.one else 2)
        self.c2_n = bx // 2 + (2 if self.one else 4)
        self.yf_n = bx + (3 if self.one else 6)
        self.nx1, self.ny1 = gx * bx // 2, gy * by // 2
        self.rows1 = self.ny1 + SIDE
        self.rows1p = -(-self.rows1 // 16) * 16
        self.l1 = bz
        self.c1_rows = by // 2 + 4
        self.c2_rows = by // 2 + 8
        self.edge = 5
        self.edge_sets = 1 if self.one else 2
        self.pack1 = self.c1_n * self.c1_rows + self.edge_sets * self.edge * 2 * by
        self.pack2 = self.c2_n * self.c2_rows + self.yf_n * 8

    def c1_first(self, i):
        return -i if self.one else -1

    def c2_first(self, i):
        return -2 * i if self.one else -2

    def yf_first(self, i):
        return -3 * i if self.one else -3


def slab_kernel(k, p_ref, w_ref, right_ref, left_ref):
    bx, bz = k.bx, k.bz
    half, part = bz // 2, bz // 4
    lane = iota((k.by, bz), 1)
    for x in range(bx):
        p = pltpu.roll(p_ref[x], half, 1)
        a, b = w_ref[0, x], w_ref[1, x]
        right_ref[x] = jnp.where(lane < half, p, jnp.where(lane < half + part, pltpu.roll(a, bz - part, 1), b))
        left_ref[x] = jnp.where(lane >= half, p, jnp.where(lane < part, a, pltpu.roll(b, part, 1)))
    for q in range(-(-bx // 4)):
        r_all, l_all = jnp.zeros((k.by, bz), jnp.float32), jnp.zeros((k.by, bz), jnp.float32)
        for r in range(min(4, bx - 4 * q)):
            c = w_ref[2, 4 * q + r]
            here = (lane >= part * r) & (lane < part * (r + 1))
            r_all = jnp.where(here, pltpu.roll(c, (part * r + part) % bz, 1), r_all)
            l_all = jnp.where(here, pltpu.roll(c, part * r, 1) if r else c, l_all)
        right_ref[bx + q] = r_all
        left_ref[bx + q] = l_all


def lane_roll(v, shift):
    shift = shift % v.shape[1]
    return pltpu.roll(v, shift, 1) if shift else v


def pressure_window(k, p, low, high):
    half = k.bz // 2
    lane = iota(p.shape, 1)
    p = pltpu.roll(p, half, 1)
    return jnp.concatenate([jnp.where(lane < half, low, p), jnp.where(lane < half, p, high)], axis=1)


def wind_window(k, w, low, low_at, high, high_at):
    half, part = k.bz // 2, k.bz // 4
    lane = iota(w.shape, 1)
    w = pltpu.roll(w, half, 1)
    first = jnp.where(lane >= half, w, jnp.where(lane >= part, lane_roll(low, part - low_at), 0.0))
    second = jnp.where(lane < half, w, jnp.where(lane < half + part, lane_roll(high, half - high_at), 0.0))
    return jnp.concatenate([first, second], axis=1)


def place():
    return lax.axis_index("gx"), lax.axis_index("gy"), lax.axis_index("gz")


def fine_mask(k, iy, iz):
    return window_mask((k.rows, k.lanes), iy * k.by - SIDE, k.gy * k.by, iz * k.bz - k.bz // 2, k.gz * k.bz)


def x_inside(k, ix, plane):
    place_x = ix * k.bx + plane
    return jnp.where((place_x >= 0) & (place_x < k.gx * k.bx), 1.0, 0.0).astype(jnp.float32)


def restrict_planes(src, first, n, half_ref, out, value):
    rows, lanes = src.shape[1], src.shape[2]
    a = pair_matrix(lanes, half_ref.shape[2], value)

    def step(j):
        s = src[first + 2 * j] + src[first + 2 * j + 1]
        half_ref[j] = dot(s + up(s, 0), a)

    for j in range(n):
        step(j)
    for j in range(n):
        out[j] = half_ref[j, pl.ds(0, rows // 2, stride=2), :]


def zero(ref):
    ref[...] = jnp.zeros(ref.shape, ref.dtype)


def first_kernel(k, p_ref, low_ref, high_ref, win_ref, send_a, send_b, pack_ref, b, m, half_ref, c1):
    ix, iy, iz = place()
    bx, by = k.bx, k.by
    pad = 3
    zero(b)
    zero(m)
    for x in range(bx):
        w = pressure_window(k, p_ref[x], low_ref[x], high_ref[x])
        win_ref[x] = w
        b[x + pad, SIDE:SIDE + by, :] = w
    tail = lax.rem(iy, 2) == 0
    for x in range(bx):
        head_rows, tail_rows = win_ref[x, :8, :], win_ref[x, by - 8:, :]
        send_a[x] = jnp.where(tail, tail_rows, head_rows)
        send_b[x] = jnp.where(tail, head_rows, tail_rows)
    mask = fine_mask(k, iy, iz)

    def step1(i):
        m[i + pad - 1] = mix(b, i + pad - 1) * (mask * x_inside(k, ix, i - 1))

    each(bx + 2, step1)

    def step2(i):
        b[i + pad - 2] = mix(m, i + pad - 2)

    each(bx + 4, step2)
    restrict_planes(b, pad - 2, bx // 2 + 2, half_ref, c1, 0.125)
    start = (k.c1_first(ix) + 1) if k.one else 0
    for j in range(k.c1_n):
        pack_ref[j * k.c1_rows:(j + 1) * k.c1_rows, :] = c1[start + j, 2:2 + k.c1_rows, :]
    at = k.c1_n * k.c1_rows
    starts = [(1 - ix) * (bx - k.edge)] if k.one else [0, bx - k.edge]
    for first in starts:
        for j in range(k.edge):
            for t in range(2):
                pack_ref[at:at + by, :] = win_ref[first + j, :, t * k.bz:(t + 1) * k.bz]
                at += by


def coarse(k, iz, b1, m1, e1, half_ref, b2, u2, v2):
    n1, n2 = k.nx1, k.nx1 // 2
    rows1, rows2, l1 = k.rows1, k.rows1p // 2, k.l1
    y0 = -(SIDE // 2)
    mask1 = window_mask((rows1, l1), y0, k.ny1, iz * (k.bz // 2) - k.bz // 4, k.gz * (k.bz // 2))
    lane2 = iota((rows2, l1), 1)
    mask2 = window_mask((rows2, l1), y0 // 2, k.ny1 // 2, iz * (k.bz // 4) - k.bz // 8, k.gz * (k.bz // 4))
    mask2 = jnp.where(lane2 < l1 // 2, mask2, 0.0)
    zero(m1)
    zero(e1)
    zero(u2)
    zero(v2)
    for i in range(n1):
        b1[i + 2] = b1[i + 2] * mask1

    def pre(i):
        c = mix(b1, i + 2) * mask1
        m1[i + 2] = c
        e1[i + 2] = C1 * (b1[i + 2] + c)

    each(n1, pre)
    a = pair_matrix(l1, l1, 0.125)
    for j in range(n2):
        s = mix(m1, 2 * j + 2) + mix(m1, 2 * j + 3)
        half_ref[j, :rows1, :] = dot(s + up(s, 0), a)
        if k.rows1p > rows1:
            half_ref[j, rows1:, :] = jnp.zeros((k.rows1p - rows1, l1), jnp.float32)
    for j in range(n2):
        s = half_ref[j, pl.ds(0, rows2, stride=2), :] * (mask2 * C2)
        b2[j] = s
        u2[j + 1] = s
    src, dst = u2, v2
    for _ in range(3):
        for j in range(n2):
            dst[j + 1] = (mix(src, j + 1) + b2[j]) * mask2
        src, dst = dst, src
    spread = spread_matrix(l1, l1)
    for j in range(n2):
        e = dot(src[j + 1], spread)
        half_ref[j, pl.ds(0, rows2, stride=2), :] = e
        half_ref[j, pl.ds(1, rows2, stride=2), :] = e
    for j in range(n2):
        e = half_ref[j, :rows1, :]
        e1[2 * j + 2] += e
        e1[2 * j + 3] += e
    for src, dst in ((e1, m1), (m1, e1)):

        def post(i):
            dst[i + 2] = (mix(src, i + 2) + C1 * b1[i + 2]) * mask1

        each(n1, post)


def prolonged(k, e1, ix, iy, first, n, half_ref, put):
    by = k.by
    for j in range(n):
        e = e1[ix * (k.bx // 2) + (first + j + 2), pl.ds(pl.multiple_of(iy * (by // 2), 8), k.rows // 2), :]
        half_ref[j, pl.ds(0, k.rows // 2, stride=2), :] = e
        half_ref[j, pl.ds(1, k.rows // 2, stride=2), :] = e
    spread = spread_matrix(k.l1, k.lanes)
    for j in range(n):
        put(j, dot(half_ref[j], spread))


def overlap_add(k, g_ref, b1, n, rows, y_skip, first_of):
    zero(b1)
    for i in range(k.gx):
        for j in range(k.gy):
            at_y = j * (k.by // 2) + y_skip
            for q in range(n):
                x = i * (k.bx // 2) + first_of(i) + q
                if 0 <= x < k.nx1:
                    part = g_ref[i * k.gy + j, q * rows:(q + 1) * rows, :]
                    b1[x + 2, at_y:at_y + rows, :] += part


def own_lanes(k, v):
    half = k.bz // 2
    first, second = v[:, :k.bz], v[:, k.bz:]
    lane = iota(first.shape, 1)
    return jnp.where(lane < half, pltpu.roll(first, half, 1), pltpu.roll(second, half, 1))


def assemble_edges(k, refs, b1, b, pad):
    g_ref, win_ref, got_a, got_b, w_ref, low_ref, high_ref = refs
    ix, iy, iz = place()
    bx, by = k.bx, k.by
    overlap_add(k, g_ref, b1, k.c1_n, k.c1_rows, 2, k.c1_first)
    even = lax.rem(iy, 2) == 0
    for x in range(bx):
        b[x + pad, :SIDE, :] = jnp.where(even, got_b[x], got_a[x])
        b[x + pad, SIDE:SIDE + by, :] = win_ref[x]
        b[x + pad, SIDE + by:, :] = jnp.where(even, got_a[x], got_b[x])
    base = k.c1_n * k.c1_rows
    span = k.edge * 2 * by
    y_low, y_high = jnp.maximum(iy - 1, 0), jnp.minimum(iy + 1, k.gy - 1)
    for side in range(2):
        if k.one:
            who, shift = 1 - ix, 0
        else:
            who = jnp.maximum(ix - 1, 0) if side == 0 else jnp.minimum(ix + 1, k.gx - 1)
            shift = span if side == 0 else 0
        for j in range(k.edge):
            at = pad - k.edge + j if side == 0 else pad + bx + j
            for t in range(2):
                row = base + shift + (2 * j + t) * by
                lanes = slice(t * k.bz, (t + 1) * k.bz)
                b[at, :SIDE, lanes] = g_ref[who * k.gy + y_low, row + by - 8:row + by, :]
                b[at, SIDE:SIDE + by, lanes] = g_ref[who * k.gy + iy, row:row + by, :]
                b[at, SIDE + by:, lanes] = g_ref[who * k.gy + y_high, row:row + 8, :]
    half, part = k.bz // 2, k.bz // 4

    def winds(x):
        low, high = low_ref[x], high_ref[x]
        q, r = x // 4, x % 4
        return (wind_window(k, w_ref[0, x], low, half, high, 0),
                wind_window(k, w_ref[1, x], low, half + part, high, part),
                wind_window(k, w_ref[2, x], low_ref[bx + q], part * r, high_ref[bx + q], part * r))

    return winds


def middle_kernel(k, assemble, ins, pack_ref, xa_ref, xb_ref, own_ref,
                  b1, m1, e1, half1, b2, u2, v2, b, m, v, vel, flux, half_ref, c2):
    ix, iy, iz = place()
    bx, by = k.bx, k.by
    pad = 5
    winds = assemble(k, ins, b1, b, pad)
    coarse(k, iz, b1, m1, e1, half1, b2, u2, v2)
    mask = fine_mask(k, iy, iz)

    def clean(i):
        b[i] = b[i] * (mask * x_inside(k, ix, i - pad))

    each(bx + 2 * pad, clean)

    def put(j, e):
        for t in range(2):
            v[pad - 4 + 2 * j + t] = e

    prolonged(k, e1, ix, iy, -2, bx // 2 + 4, half_ref, put)

    def pre(i):
        at = i + pad - 4
        here = mask * x_inside(k, ix, i - 4)
        v[at] = (v[at] + C0 * (b[at] + mix(b, at))) * here

    each(bx + 8, pre)

    def post1(i):
        at = i + pad - 3
        m[at] = (mix(v, at) + C0 * b[at]) * (mask * x_inside(k, ix, i - 3))

    each(bx + 6, post1)

    def post2(i):
        at = i + pad - 2
        v[at] = (mix(m, at) + C0 * b[at]) * (mask * x_inside(k, ix, i - 2))

    each(bx + 4, post2)

    def speed(i):
        at = i + pad - 1
        here = 0.5 * (mask * x_inside(k, ix, i - 1))
        c = v[at]
        vel[0, i] = (v[at + 1] - v[at - 1]) * here
        vel[1, i] = (up(c, 0) - down(c, 0)) * here
        vel[2, i] = (up(c, 1) - down(c, 1)) * here

    each(bx + 2, speed)
    own_mask = mask[SIDE:SIDE + by, :]
    zero(flux)
    for x in range(bx):
        w0, w1, w2 = (0.5 * w for w in winds(x))
        for d in range(3):
            c = vel[d, x + 1, SIDE:SIDE + by, :]
            xp, xm = vel[d, x + 2, SIDE:SIDE + by, :], vel[d, x, SIDE:SIDE + by, :]
            yp, ym = vel[d, x + 1, SIDE + 1:SIDE + by + 1, :], vel[d, x + 1, SIDE - 1:SIDE + by - 1, :]
            zp, zm = up(c, 1), down(c, 1)
            near = (xp + xm) + (yp + ym) + (zp + zm)
            total = 7.0 * c - near + w0 * (xp - xm) + w1 * (yp - ym) + w2 * (zp - zm)
            flux[d, x + 2, SIDE:SIDE + by, :] = total * own_mask
    zero(b)
    zero(m)

    def spread_flux(i):
        at = i + pad - 1
        f1, f2 = flux[1, i + 1], flux[2, i + 1]
        total = (flux[0, i + 2] - flux[0, i]) + (up(f1, 0) - down(f1, 0)) + (up(f2, 1) - down(f2, 1))
        b[at] = total * (-0.5 * (mask * x_inside(k, ix, i - 1)))

    each(bx + 2, spread_flux)
    zero(v)

    def power1_pure(i):
        at = i + pad - 2
        m[at] = mix(b, at) * (mask * x_inside(k, ix, i - 2))

    each(bx + 4, power1_pure)

    def power2(i):
        at = i + pad - 3
        v[at] = mix(m, at) * (mask * x_inside(k, ix, i - 3))

    each(bx + 6, power2)

    def power3(i):
        at = i + pad - 4
        b[at] = C0 * ((b[at] + m[at]) + (v[at] + mix(v, at))) * (mask * x_inside(k, ix, i - 4))

    each(bx + 8, power3)
    restrict_planes(v, pad - 4, bx // 2 + 4, half_ref, c2, 0.125)
    start = (k.c2_first(ix) + 2) if k.one else 0
    for j in range(k.c2_n):
        pack_ref[j * k.c2_rows:(j + 1) * k.c2_rows, :] = c2[start + j]
    row8 = iota((8, k.bz), 0)
    at = k.c2_n * k.c2_rows
    start = (k.yf_first(ix) if k.one else -3) + pad
    for j in range(k.yf_n):
        c = own_lanes(k, jnp.where(iota((8, k.lanes), 0) < 4, b[start + j, SIDE + by:, :], b[start + j, :SIDE, :]))
        pack_ref[at:at + 8, :] = c
        at += 8
    upper = lax.rem(ix, 2) == 0
    first_a = pad + jnp.where(upper, bx, -4)
    first_b = pad + jnp.where(upper, -4, bx)
    for j in range(4):
        xa_ref[j] = own_lanes(k, b[first_a + j, SIDE:SIDE + by, :])
        if xb_ref is not None:
            xb_ref[j] = own_lanes(k, b[first_b + j, SIDE:SIDE + by, :])
    for x in range(bx):
        own_ref[x] = own_lanes(k, b[x + pad, SIDE:SIDE + by, :])


def last_kernel(k, g_ref, own_ref, xa_ref, xb_ref, out_ref, b1, m1, e1, half1, b2, u2, v2, v, m, half_ref):
    ix, iy, iz = place()
    bx, by = k.bx, k.by
    overlap_add(k, g_ref, b1, k.c2_n, k.c2_rows, 0, k.c2_first)
    coarse(k, iz, b1, m1, e1, half1, b2, u2, v2)
    pad = 2
    mask = fine_mask(k, iy, iz)

    def put(j, e):
        for t in range(2):
            plane = -2 + 2 * j + t
            v[pad + plane] = e * (mask * x_inside(k, ix, plane))

    prolonged(k, e1, ix, iy, -1, bx // 2 + 2, half_ref, put)

    def post1(i):
        at = i + pad - 1
        m[at] = mix(v, at) * (mask * x_inside(k, ix, i - 1))

    each(bx + 2, post1)
    base = k.c2_n * k.c2_rows
    low_ok = jnp.where(iy > 0, 1.0, 0.0).astype(jnp.float32)
    high_ok = jnp.where(iy < k.gy - 1, 1.0, 0.0).astype(jnp.float32)
    y_low, y_high = jnp.maximum(iy - 1, 0), jnp.minimum(iy + 1, k.gy - 1)
    row8 = iota((8, k.bz), 0)
    low_keep = jnp.where(row8 < 4, low_ok, 0.0)
    high_keep = jnp.where(row8 >= 4, high_ok, 0.0)
    for x in range(bx):
        out_ref[x] = own_lanes(k, mix(m, x + pad)[SIDE:SIDE + by, :]) + own_ref[x]

    def frame(who, first, x_from, x_to, ok):
        for x in range(x_from, x_to):
            row = base + (x - first) * 8
            if not isinstance(row, int):
                row = pl.multiple_of(row, 8)
            lo = g_ref[who * k.gy + y_low, pl.ds(row, 8), :] * ok
            hi = g_ref[who * k.gy + y_high, pl.ds(row, 8), :] * ok
            out_ref[x, :8, :] += lo * low_keep
            out_ref[x, by - 8:, :] += hi * high_keep

    one = jnp.float32(1.0)
    frame(ix, k.yf_first(ix), 0, bx, one)
    upper = lax.rem(ix, 2) == 0
    if k.one:
        for j in range(3):
            x = jnp.where(ix == 0, bx - 3 + j, j)
            row = pl.multiple_of(base + jnp.where(ix == 0, j, bx + j) * 8, 8)
            lo = g_ref[(1 - ix) * k.gy + y_low, pl.ds(row, 8), :]
            hi = g_ref[(1 - ix) * k.gy + y_high, pl.ds(row, 8), :]
            out_ref[x, :8, :] += lo * low_keep
            out_ref[x, by - 8:, :] += hi * high_keep
    else:
        frame(jnp.maximum(ix - 1, 0), -3 - bx, 0, 3, jnp.where(ix > 0, 1.0, 0.0).astype(jnp.float32))
        frame(jnp.minimum(ix + 1, k.gx - 1), bx - 3, bx - 3, bx, jnp.where(ix < k.gx - 1, 1.0, 0.0).astype(jnp.float32))
    for j in range(4):
        out_ref[jnp.where(upper, bx - 4, 0) + j] += xa_ref[j]
        if xb_ref is not None:
            out_ref[jnp.where(upper, 0, bx - 4) + j] += xb_ref[j]


def call(kernel, outs, scratch, args, flops):
    f32 = lambda s: jax.ShapeDtypeStruct(s, jnp.float32)
    return pl.pallas_call(
        kernel,
        out_shape=[f32(s) for s in outs],
        scratch_shapes=[pltpu.VMEM(s, jnp.float32) for s in scratch],
        compiler_params=pltpu.CompilerParams(vmem_limit_bytes=40 * 1024 * 1024),
        cost_estimate=pl.CostEstimate(flops=flops, bytes_accessed=1 << 20, transcendentals=0),
    )(*args)


def pairs(n):
    first = [(i, i ^ 1) for i in range(n) if (i ^ 1) < n]
    second = [(i + s, i + 1 - s) for i in range(1, n - 1, 2) for s in (0, 1)]
    return first, second


def chain(n, step):
    return [(i, i + step) for i in range(n) if 0 <= i + step < n]


def coarse_scratch(k):
    n1, n2, rows2 = k.nx1, k.nx1 // 2, k.rows1p // 2
    big = (n1 + 4, k.rows1, k.l1)
    return [big, big, big, (n2, k.rows1p, k.l1), (n2, rows2, k.l1), (n2 + 2, rows2, k.l1), (n2 + 2, rows2, k.l1)]


def edge_form(k, pressure, wind):
    bx, by, bz = k.bx, k.by, k.bz
    slab = (bx + -(-bx // 4), by, bz)
    right, left = call(functools.partial(slab_kernel, k), [slab, slab], [], (pressure, wind), 1 << 20)
    low = lax.ppermute(right, "gz", chain(k.gz, 1))
    high = lax.ppermute(left, "gz", chain(k.gz, -1))
    fine = lambda n: (n, k.rows, k.lanes)
    window, send_a, send_b, pack = call(
        functools.partial(first_kernel, k),
        [(bx, by, k.lanes), (bx, 8, k.lanes), (bx, 8, k.lanes), (k.pack1, bz)],
        [fine(bx + 6), fine(bx + 6), (bx // 2 + 2, k.rows, k.l1), (bx // 2 + 2, k.rows // 2, k.l1)],
        (pressure, low, high), 1 << 22)
    ya, yb = pairs(k.gy)
    got_a = lax.ppermute(send_a, "gy", ya)
    got_b = lax.ppermute(send_b, "gy", yb)
    gathered = lax.all_gather(pack, PLANE)
    return assemble_edges, (gathered, window, got_a, got_b, wind, low, high)


def general(k, pressure, wind):
    bx, by, bz = k.bx, k.by, k.bz
    fine = lambda n: (n, k.rows, k.lanes)
    assemble, args = edge_form(k, pressure, wind)
    xa, xb = pairs(k.gx)
    x_outs = [(4, by, bz)] * (2 if xb else 1)

    def middle(*refs):
        ins, rest = refs[:len(args)], refs[len(args):]
        pack_ref, rest = rest[0], rest[1:]
        xa_ref, rest = rest[0], rest[1:]
        xb_ref = None
        if xb:
            xb_ref, rest = rest[0], rest[1:]
        middle_kernel(k, assemble, ins, pack_ref, xa_ref, xb_ref, *rest)

    big = fine(bx + 10)
    outs = call(
        middle, [(k.pack2, bz)] + x_outs + [(bx, by, bz)],
        coarse_scratch(k) + [big, big, big, (3,) + fine(bx + 2), (3,) + fine(bx + 4),
                             (bx // 2 + 4, k.rows, k.l1), (bx // 2 + 4, k.rows // 2, k.l1)],
        args, 1 << 24)
    pack, frames, own = outs[0], outs[1:-1], outs[-1]
    got = [lax.ppermute(f, "gx", perm) for f, perm in zip(frames, (xa, xb))]
    gathered = lax.all_gather(pack, PLANE)

    def last(*refs):
        g_ref, own_ref, xa_ref, rest = refs[0], refs[1], refs[2], refs[3:]
        xb_ref = None
        if xb:
            xb_ref, rest = rest[0], rest[1:]
        last_kernel(k, g_ref, own_ref, xa_ref, xb_ref, *rest)

    (result,) = call(
        last, [(bx, by, bz)],
        coarse_scratch(k) + [fine(bx + 4), fine(bx + 4), (bx // 2 + 2, k.rows, k.l1)],
        (gathered, own, *got), 1 << 23)
    return result

FR = 5
CR = 2


class Mirror:
    def __init__(self, gx, gy, gz, bx, by, bz):
        self.gx, self.gy, self.gz, self.bx, self.by, self.bz = gx, gy, gz, bx, by, bz
        self.rows = by + 2 * FR
        self.core = by + 8
        self.nx, self.ny = gx * bx, gy * by
        self.nx1, self.ny1 = self.nx // 2, self.ny // 2
        self.rows1 = self.ny1 + 8
        self.part = bz // 4
        groups = lambda n: -(-n // 4)
        self.fine_n = bx + 5
        self.at_fine = groups(self.nx1) * self.ny1
        self.at_wind = self.at_fine + groups(self.fine_n) * self.rows
        self.slab_rows = self.at_wind + groups(3 * bx) * by
        self.c2_n, self.c2_rows = bx // 2 + 2, by // 2 + 4
        self.yf_n, self.yf_at = bx + 3, (bx // 2 + 2) * (by // 2 + 4)
        self.pack = self.yf_at + 8 * self.yf_n


def exact_dot(x, a):
    high = x.astype(jnp.bfloat16)
    low = (x - high.astype(jnp.float32)).astype(jnp.bfloat16)
    return (jnp.dot(high, a, preferred_element_type=jnp.float32)
            + jnp.dot(low, a, preferred_element_type=jnp.float32))


def matrix(hit, value):
    return jnp.where(hit, value, 0.0).astype(jnp.float32).astype(jnp.bfloat16)


def flag(good):
    return jnp.where(good, 1.0, 0.0).astype(jnp.float32)


def beside(c0, c1):
    n = c0.shape[1]
    lane = iota(c0.shape, 1)
    last, first = lane == n - 1, lane == 0
    u0, u1, d0, d1 = up(c0, 1), up(c1, 1), down(c0, 1), down(c1, 1)
    return ((jnp.where(last, u1, u0), jnp.where(last, u0, u1)),
            (jnp.where(first, d1, d0), jnp.where(first, d0, d1)))


def mix_halves(s, i, halves=2):
    n = s.shape[2] - 2
    c = [s[i + 1, h, 1:1 + n, :] for h in range(2)]
    plus, minus = beside(*c)
    out = []
    for h in range(halves):
        near = (s[i, h, 1:1 + n, :] + s[i + 2, h, 1:1 + n, :]) + (s[i + 1, h, 2:2 + n, :] + s[i + 1, h, :n, :])
        out.append((1.0 - OMEGA) * c[h] + W * (near + (plus[h] + minus[h])))
    return out


def halves_mask(k, iy, iz):
    y = iota((k.core, k.bz), 0) + (iy * k.by - 4)
    lane = iota((k.core, k.bz), 1)
    y_good = (y >= 0) & (y < k.ny)
    edge = flag(y_good)
    side = jnp.where(lane < k.bz // 2, jnp.where(iz < k.gz - 1, 1.0, 0.0), jnp.where(iz > 0, 1.0, 0.0))
    return edge, edge * side.astype(jnp.float32)


def zero_rim(s):
    s[0] = jnp.zeros(s.shape[1:], jnp.float32)
    n = s.shape[2]
    for i in range(1, s.shape[0]):
        for h in range(2):
            s[i, h, 0:1, :] = jnp.zeros((1, s.shape[3]), jnp.float32)
            s[i, h, n - 1:n, :] = jnp.zeros((1, s.shape[3]), jnp.float32)


def mix1(k, s, i, n, at):
    c = s[i + 1, at:at + n, :]
    near = (s[i, at:at + n, :] + s[i + 2, at:at + n, :]) + (s[i + 1, at + 1:at + n + 1, :] + s[i + 1, at - 1:at + n - 1, :])
    return (1.0 - OMEGA) * c + W * (near + (up(c, 1) + down(c, 1)))


def coarse_plane(k, iz, b1, m1, e1, half_ref, b2, u2, v2):
    n1, n2, ny, l1 = k.nx1, k.nx1 // 2, k.ny1, k.bz
    ny2 = ny // 2
    lane = iota((ny, l1), 1)
    low_ok, high_ok = flag(iz > 0), flag(iz < k.gz - 1)
    mask1 = jnp.where(lane < l1 // 2, 1.0, jnp.where(lane < 3 * l1 // 4, high_ok, low_ok))
    lane2 = iota((ny2, l1), 1)
    own2 = l1 // 8
    mask2 = jnp.where(lane2 < own2, low_ok, jnp.where(lane2 < 3 * own2, 1.0, jnp.where(lane2 < 4 * own2, high_ok, 0.0)))
    for s in (m1, e1):
        for i in (0, n1 + 1):
            s[i] = jnp.zeros(s.shape[1:], jnp.float32)
    for s in (b1, m1, e1):
        for i in range(n1):
            s[i + 1, :CR, :] = jnp.zeros((CR, l1), jnp.float32)
            s[i + 1, CR + ny:, :] = jnp.zeros((k.rows1 - CR - ny, l1), jnp.float32)
    zero(u2)
    zero(v2)
    for i in range(n1):
        b1[i + 1, CR:CR + ny, :] = b1[i + 1, CR:CR + ny, :] * mask1
    for i in range(n1):
        c = mix1(k, b1, i, ny, CR) * mask1
        m1[i + 1, CR:CR + ny, :] = c
        e1[i + 1, CR:CR + ny, :] = C1 * (b1[i + 1, CR:CR + ny, :] + c)
    row, column = iota((l1, l1), 0), iota((l1, l1), 1)
    linear = lambda x: (jnp.where(x < 3 * l1 // 4, x, x - l1) >> 1) + own2
    for j in range(n2):
        half_ref[j] = mix1(k, m1, 2 * j, ny, CR) + mix1(k, m1, 2 * j + 1, ny, CR)
    pairs_sum = [half_ref[j, pl.ds(0, ny2, stride=2), :] + half_ref[j, pl.ds(1, ny2, stride=2), :] for j in range(n2)]
    r2 = exact_dot(jnp.concatenate(pairs_sum, axis=0), matrix(linear(row) == column, 0.125))
    for j in range(n2):
        c = r2[j * ny2:(j + 1) * ny2] * (mask2 * C2)
        b2[j] = c
        u2[j + 1, 1:1 + ny2, :] = c
    src, dst = u2, v2
    for _ in range(3):
        for j in range(n2):
            dst[j + 1, 1:1 + ny2, :] = (mix1(k, src, j, ny2, 1) + b2[j]) * mask2
        src, dst = dst, src
    stack = jnp.concatenate([src[j + 1, 1:1 + ny2, :] for j in range(n2)], axis=0)
    spread = exact_dot(stack, matrix(row == linear(column), 1.0))
    for j in range(n2):
        e = spread[j * ny2:(j + 1) * ny2]
        half_ref[j, pl.ds(0, ny2, stride=2), :] = e
        half_ref[j, pl.ds(1, ny2, stride=2), :] = e
    for j in range(n2):
        e = half_ref[j]
        for t in range(2):
            e1[2 * j + t + 1, CR:CR + ny, :] = e1[2 * j + t + 1, CR:CR + ny, :] + e
    for src, dst in ((e1, m1), (m1, e1)):
        for i in range(n1):
            dst[i + 1, CR:CR + ny, :] = (mix1(k, src, i, ny, CR) + C1 * b1[i + 1, CR:CR + ny, :]) * mask1


def from_end(ix, i, count):
    return jnp.where(ix == 0, i, count - 1 - i)


def prolong_halves(k, ix, iy, e1, n, v):
    half, rows = k.bz // 2, k.core // 2
    first = pl.multiple_of(iy * (k.by // 2), 8)
    stack = jnp.concatenate([e1[from_end(ix, j, k.nx1) + 1, pl.ds(first, 16), :] for j in range(n)], axis=0)
    row, column = iota((k.bz, 2 * k.bz), 0), iota((k.bz, 2 * k.bz), 1)
    spread = exact_dot(stack, matrix(row == (column >> 1), 1.0))
    for j in range(n):
        for h in range(2):
            e = spread[16 * j:16 * j + rows, h * k.bz:(h + 1) * k.bz]
            for t in range(2):
                v[2 * j + t + 1, h, pl.ds(1, rows, stride=2), :] = e
                v[2 * j + t + 1, h, pl.ds(2, rows, stride=2), :] = e


def take_slab(k, ref, base, rows, i, to):
    at = base + (i // 4) * rows
    return lane_roll(ref[at:at + rows, :], to - k.part * (i % 4))


def plane_kernel(k, g_ref, w_ref, c1_ref, win_ref, right_ref, left_ref, p, m, q, half_ref):
    ix, iy, iz = place()
    bx, by, bz, nx, ny, part = k.bx, k.by, k.bz, k.nx, k.ny, k.part
    p[0] = jnp.zeros(p.shape[1:], jnp.float32)
    p[nx + 1] = jnp.zeros(p.shape[1:], jnp.float32)
    m[0] = jnp.zeros(m.shape[1:], jnp.float32)
    m[nx + 1] = jnp.zeros(m.shape[1:], jnp.float32)
    for x in range(nx):
        p[x + 1, :FR, :] = jnp.zeros((FR, bz), jnp.float32)
        p[x + 1, FR + ny:, :] = jnp.zeros((p.shape[1] - FR - ny, bz), jnp.float32)
        m[x + 1, 0:1, :] = jnp.zeros((1, bz), jnp.float32)
        m[x + 1, ny + 1:, :] = jnp.zeros((m.shape[1] - ny - 1, bz), jnp.float32)
        for j in range(k.gy):
            p[x + 1, FR + j * by:FR + (j + 1) * by, :] = g_ref[(x // bx) * k.gy + j, x % bx]
    lane = iota((ny, bz), 1)
    first, last = lane == 0, lane == bz - 1
    ends = jnp.where(first, flag(iz > 0), jnp.where(last, flag(iz < k.gz - 1), 0.0)) * (W * W)

    def parts(s, x, at):
        c = s[x + 1, at:at + ny, :]
        four = (s[x, at:at + ny, :] + s[x + 2, at:at + ny, :]) + (s[x + 1, at + 1:at + ny + 1, :] + s[x + 1, at - 1:at + ny - 1, :])
        along = jnp.where(last, 0.0, up(c, 1)) + jnp.where(first, 0.0, down(c, 1))
        return c, four, (1.0 - OMEGA) * c + W * (four + along)

    for x in range(nx):
        c, four, mixed = parts(p, x, FR)
        m[x + 1, 1:1 + ny, :] = mixed
        q[x] = (1.0 - OMEGA + W) * c + (mixed + W * four)
    row, column = iota((bz, bz), 0), iota((bz, bz), 1)
    own = matrix((row >> 1) == column, 0.125)
    rim = ((row == 0) & (column == bz - 1)) | ((row == bz - 1) & (column == bz // 2))
    rim = matrix(rim, 0.125)
    half_rows = ny // 2
    for j in range(k.nx1):
        s = None
        for x in (2 * j, 2 * j + 1):
            r = parts(m, x, 1)[2] + ends * p[x + 1, FR:FR + ny, :]
            s = r if s is None else s + r
        half_ref[j] = s
        t = (q[2 * j, pl.ds(0, half_rows, stride=2), :] + q[2 * j, pl.ds(1, half_rows, stride=2), :]
             + q[2 * j + 1, pl.ds(0, half_rows, stride=2), :] + q[2 * j + 1, pl.ds(1, half_rows, stride=2), :])
        s = half_ref[j, pl.ds(0, half_rows, stride=2), :] + half_ref[j, pl.ds(1, half_rows, stride=2), :]
        c1_ref[j] = exact_dot(s, own) + exact_dot(W * t, rim)

    def pack(ref, base, rows, n, load, from_lane):
        lane = iota((rows, bz), 1)
        for group in range(-(-n // 4)):
            total = jnp.zeros((rows, bz), jnp.float32)
            for r in range(min(4, n - 4 * group)):
                moved = lane_roll(load(4 * group + r), part * r - from_lane)
                total = jnp.where((lane >= part * r) & (lane < part * (r + 1)), moved, total)
            ref[base + group * rows:base + (group + 1) * rows, :] = total

    for i in range(k.fine_n):
        win_ref[i] = p[from_end(ix, i, nx) + 1, pl.ds(pl.multiple_of(iy * by, 8), k.rows), :]
    for ref, lane1, lane0 in ((right_ref, part + 1, 3 * part), (left_ref, bz - 1, 0)):
        pack(ref, 0, k.ny1, k.nx1, lambda i: c1_ref[i], lane1)
        pack(ref, k.at_fine, k.rows, k.fine_n, lambda i: win_ref[i], lane0)
        pack(ref, k.at_wind, by, 3 * bx, lambda i: w_ref[i // bx, from_end(ix, i % bx, bx)], lane0)


def solve_kernel(k, c1_ref, win_ref, w_ref, low_ref, high_ref, pack_ref, x_ref, own_ref,
                 b1, m1, e1, half1, b2, u2, v2, b, m, v, vel, flux, half_ref):
    ix, iy, iz = place()
    bx, by, bz, part, n = k.bx, k.by, k.bz, k.part, k.core
    lane = iota((k.ny1, bz), 1)
    for s in (b1,):
        for i in (0, k.nx1 + 1):
            s[i] = jnp.zeros(s.shape[1:], jnp.float32)
    for x in range(k.nx1):
        low = take_slab(k, low_ref, 0, k.ny1, x, 3 * part + 1)
        high = take_slab(k, high_ref, 0, k.ny1, x, 2 * part - 1)
        low = jnp.where((lane >= 3 * part + 1) | (lane == 0), low, 0.0)
        high = jnp.where((lane >= 2 * part - 1) & (lane < 3 * part - 1), high, 0.0)
        b1[x + 1, CR:CR + k.ny1, :] = c1_ref[x] + (low + high)
    coarse_plane(k, iz, b1, m1, e1, half1, b2, u2, v2)
    mask = halves_mask(k, iy, iz)
    for s in (b, m, v):
        zero_rim(s)

    def outer(low, high, lane):
        return jnp.where(lane >= 3 * part, low, jnp.where(lane < part, high, 0.0))

    lane = iota((k.rows, bz), 1)
    for i in range(k.fine_n):
        b[i + 1, 0] = win_ref[i]
        b[i + 1, 1] = outer(take_slab(k, low_ref, k.at_fine, k.rows, i, 3 * part),
                            take_slab(k, high_ref, k.at_fine, k.rows, i, 0), lane)
    prolong_halves(k, ix, iy, e1, bx // 2 + 2, v)
    for i in range(bx + 4):
        mb = mix_halves(b, i)
        for h in range(2):
            v[i + 1, h, 1:1 + n, :] = (v[i + 1, h, 1:1 + n, :] + C0 * (b[i + 1, h, 1:1 + n, :] + mb[h])) * mask[h]
    for src, dst, count in ((v, m, bx + 3), (m, v, bx + 2)):
        for i in range(count):
            c = mix_halves(src, i)
            for h in range(2):
                dst[i + 1, h, 1:1 + n, :] = (c[h] + C0 * b[i + 1, h, 1:1 + n, :]) * mask[h]
    half_mask = [0.5 * c for c in mask]
    for d in range(3):
        vel[d, 0] = jnp.zeros(vel.shape[2:], jnp.float32)
    for i in range(bx + 1):
        plus, minus = beside(v[i + 1, 0, 1:1 + n, :], v[i + 1, 1, 1:1 + n, :])
        for h in range(2):
            vel[0, i + 1, h] = (v[i + 2, h, 1:1 + n, :] - v[i, h, 1:1 + n, :]) * half_mask[h]
            vel[1, i + 1, h] = (v[i + 1, h, 2:2 + n, :] - v[i + 1, h, :n, :]) * half_mask[h]
            vel[2, i + 1, h] = (plus[h] - minus[h]) * half_mask[h]
    own_at = 4
    zero(flux)
    sign = jnp.where(ix == 0, 0.5, -0.5).astype(jnp.float32)
    lane = iota((by, bz), 1)
    for x in range(bx):
        winds = []
        for d in range(3):
            low = take_slab(k, low_ref, k.at_wind, by, d * bx + x, 3 * part)
            high = take_slab(k, high_ref, k.at_wind, by, d * bx + x, 0)
            scale = sign if d == 0 else 0.5
            winds.append((scale * w_ref[d, from_end(ix, x, bx)], scale * outer(low, high, lane)))
        for d in range(3):
            at = lambda i, h, r: vel[d, i + 1, h, own_at + r:own_at + r + by, :]
            c = [at(x, h, 0) for h in range(2)]
            plus, minus = beside(*c)
            for h in range(2):
                xp, xm, yp, ym, zp, zm = at(x + 1, h, 0), at(x - 1, h, 0), at(x, h, 1), at(x, h, -1), plus[h], minus[h]
                near = (xp + xm) + (yp + ym) + (zp + zm)
                total = 7.0 * c[h] - near + winds[0][h] * (xp - xm) + winds[1][h] * (yp - ym) + winds[2][h] * (zp - zm)
                if h == 1:
                    total = total * mask[1][own_at:own_at + by]
                flux[d, x + 1, h, own_at + 1:own_at + 1 + by, :] = total
    minus_mask = [-0.5 * c for c in mask]
    for s, first in ((b, bx + 2), (m, bx + 3), (v, bx + 4)):
        for i in range(first, bx + 6):
            s[i] = jnp.zeros(s.shape[1:], jnp.float32)
    for i in range(bx + 1):
        plus, minus = beside(flux[2, i + 1, 0, 1:1 + n, :], flux[2, i + 1, 1, 1:1 + n, :])
        for h in range(2):
            total = (flux[0, i + 2, h, 1:1 + n, :] - flux[0, i, h, 1:1 + n, :]
                     + (flux[1, i + 1, h, 2:2 + n, :] - flux[1, i + 1, h, :n, :]) + (plus[h] - minus[h]))
            b[i + 1, h, 1:1 + n, :] = total * minus_mask[h]
    zero_rows = jnp.zeros((1, bz), jnp.float32)
    for i in range(bx + 1):
        for h in range(2):
            b[i + 1, h, 0:1, :] = zero_rows
            b[i + 1, h, n + 1:n + 2, :] = zero_rows
    for src, dst, count in ((b, m, bx + 2), (m, v, bx + 3)):
        for i in range(count):
            c = mix_halves(src, i)
            for h in range(2):
                dst[i + 1, h, 1:1 + n, :] = c[h] * mask[h]
    half_rows = n // 2
    for j in range(k.c2_n):
        for h in range(2):
            take = lambda i, r: v[i + 1, h, pl.ds(r, half_rows, stride=2), :]
            half_ref[h, j, :half_rows, :] = (take(2 * j, 1) + take(2 * j, 2)) + (take(2 * j + 1, 1) + take(2 * j + 1, 2))
            half_ref[h, j, half_rows:, :] = jnp.zeros((16 - half_rows, bz), jnp.float32)
    row, column = iota((bz, bz), 0), iota((bz, bz), 1)
    c2 = (exact_dot(half_ref[0].reshape(k.c2_n * 16, bz), matrix((row >> 1) == column, 0.125))
          + exact_dot(half_ref[1].reshape(k.c2_n * 16, bz), matrix((row >> 1) + bz // 2 == column, 0.125)))
    for j in range(k.c2_n):
        pack_ref[j * k.c2_rows:(j + 1) * k.c2_rows, :] = c2[16 * j:16 * j + k.c2_rows]
    for i in range(bx + 4):
        c = mix_halves(v, i, 1)[0]
        at = lambda s: s[i + 1, 0, 1:1 + n, :]
        c = C0 * ((at(b) + at(m)) + (at(v) + c)) * mask[0]
        if i < bx:
            own_ref[i] = c[4:4 + by]
        else:
            x_ref[i - bx] = c[4:4 + by]
        if i < k.yf_n:
            row = k.yf_at + 8 * i
            pack_ref[row:row + 4, :] = c[4 + by:8 + by]
            pack_ref[row + 4:row + 8, :] = c[:4]


def close_kernel(k, g_ref, own_ref, x_ref, out_ref, b1, m1, e1, half1, b2, u2, v2, v, m):
    ix, iy, iz = place()
    bx, by, bz, n = k.bx, k.by, k.bz, k.core
    zero(b1)
    for i in range(2):
        for j in range(k.gy):
            at = j * (by // 2)
            for q in range(k.c2_n):
                x = q if i == 0 else k.nx1 - 1 - q
                part = g_ref[i * k.gy + j, q * k.c2_rows:(q + 1) * k.c2_rows, :]
                b1[x + 1, at:at + k.c2_rows, :] += part
    coarse_plane(k, iz, b1, m1, e1, half1, b2, u2, v2)
    mask = halves_mask(k, iy, iz)
    for s in (v, m):
        zero_rim(s)
    prolong_halves(k, ix, iy, e1, bx // 2 + 1, v)
    for i in range(bx + 2):
        for h in range(2):
            v[i + 1, h, 1:1 + n, :] = v[i + 1, h, 1:1 + n, :] * mask[h]
    for i in range(bx + 1):
        c = mix_halves(v, i)
        for h in range(2):
            m[i + 1, h, 1:1 + n, :] = c[h] * mask[h]
    low_ok, high_ok = flag(iy > 0), flag(iy < k.gy - 1)
    y_low, y_high = jnp.maximum(iy - 1, 0), jnp.minimum(iy + 1, k.gy - 1)
    for i in range(bx):
        c = mix_halves(m, i, 1)[0][4:4 + by] + own_ref[i]
        if i >= bx - 4:
            c = c + x_ref[bx - 1 - i]
        at = from_end(ix, i, bx)
        out_ref[at] = c
        low, high = 0.0, 0.0
        for who, plane in ((ix, i), (1 - ix, 2 * bx - 1 - i)):
            if plane < k.yf_n:
                row = k.yf_at + 8 * plane
                low = low + g_ref[who * k.gy + y_low, row:row + 4, :]
                high = high + g_ref[who * k.gy + y_high, row + 4:row + 8, :]
        out_ref[at, :4, :] += low * low_ok
        out_ref[at, by - 4:, :] += high * high_ok


def mirrored(k, pressure, wind):
    bx, by, bz = k.bx, k.by, k.bz
    n1, n2 = k.nx1, k.nx1 // 2
    fine = lambda n: (n + 2, 2, k.rows, bz)
    level1 = [(n1 + 2, k.rows1, bz)] * 3
    level2 = [(n2, k.ny1, bz), (n2, k.ny1 // 2, bz)] + [(n2 + 2, k.ny1 // 2 + 2, bz)] * 2
    gathered = lax.all_gather(pressure, PLANE)
    c1, window, right, left = call(
        functools.partial(plane_kernel, k),
        [(n1, k.ny1, bz), (k.fine_n, k.rows, bz), (k.slab_rows, bz), (k.slab_rows, bz)],
        [(k.nx + 2, -(-(k.ny + 2 * FR) // 8) * 8, bz), (k.nx + 2, k.ny + 2, bz), (k.nx, k.ny, bz), (n1, k.ny, bz)],
        (gathered, wind), 1 << 22)
    low = lax.ppermute(right, "gz", chain(k.gz, 1))
    high = lax.ppermute(left, "gz", chain(k.gz, -1))
    pack, frame, own = call(
        functools.partial(solve_kernel, k),
        [(k.pack, bz), (4, by, bz), (bx, by, bz)],
        level1 + level2 + [fine(bx + 5)] * 3 + [(3, bx + 3, 2, k.core, bz), (3,) + fine(bx + 1), (2, k.c2_n, 16, bz)],
        (c1, window, wind, low, high), 1 << 24)
    frame = lax.ppermute(frame, "gx", pairs(k.gx)[0])
    gathered = lax.all_gather(pack, PLANE)
    (result,) = call(
        functools.partial(close_kernel, k), [(bx, by, bz)],
        level1 + level2 + [fine(bx + 2)] * 2,
        (gathered, own, frame), 1 << 23)
    return result


def solution(mesh):
    gx, gy, gz = (mesh.shape[a] for a in ("gx", "gy", "gz"))

    def run(pressure, wind):
        form, sizes = (mirrored, Mirror) if gx == 2 else (general, Sizes)
        return form(sizes(gx, gy, gz, *pressure.shape), pressure, wind)

    in_specs = (P("gx", "gy", "gz"), P(None, "gx", "gy", "gz"))
    return jax.shard_map(run, mesh=mesh, in_specs=in_specs, out_specs=P("gx", "gy", "gz"), check_vma=False)
```

```python
import functools

import jax
import jax.numpy as jnp
from jax import lax
from jax.experimental import pallas as pl
from jax.experimental.pallas import tpu as pltpu
from jax.sharding import PartitionSpec as P

OMEGA = 0.8
W = OMEGA / 6.0
C0, C1, C2 = W, 4.0 * W, 16.0 * W
SIDE = 8
PLANE = ("gx", "gy")


def up(v, axis):
    return pltpu.roll(v, v.shape[axis] - 1, axis)


def down(v, axis):
    return pltpu.roll(v, 1, axis)


def mix(s, i):
    c = s[i]
    near = (s[i - 1] + s[i + 1]) + (up(c, 0) + down(c, 0)) + (up(c, 1) + down(c, 1))
    return (1.0 - OMEGA) * c + W * near


def each(n, step):
    lax.fori_loop(0, n, lambda i, _: step(i), None, unroll=True)


def iota(shape, axis):
    return lax.broadcasted_iota(jnp.int32, shape, axis)


def pair_matrix(rows, columns, value):
    hit = (iota((rows, columns), 0) >> 1) == iota((rows, columns), 1)
    return jnp.where(hit, value, 0.0).astype(jnp.float32)


def spread_matrix(rows, columns):
    hit = (iota((rows, columns), 1) >> 1) == iota((rows, columns), 0)
    return jnp.where(hit, 1.0, 0.0).astype(jnp.float32)


def dot(a, b):
    return jnp.dot(a, b, precision=lax.Precision.HIGHEST, preferred_element_type=jnp.float32)


def window_mask(shape, y_first, y_count, z_first, z_count):
    y = iota(shape, 0) + y_first
    z = iota(shape, 1) + z_first
    good = (y >= 0) & (y < y_count) & (z >= 0) & (z < z_count)
    return jnp.where(good, 1.0, 0.0).astype(jnp.float32)


class Sizes:
    def __init__(self, gx, gy, gz, bx, by, bz):
        self.gx, self.gy, self.gz = gx, gy, gz
        self.bx, self.by, self.bz = bx, by, bz
        self.rows, self.lanes = by + 2 * SIDE, 2 * bz
        self.one = gx == 2
        self.c1_n = bx // 2 + (1 if self.one else 2)
        self.c2_n = bx // 2 + (2 if self.one else 4)
        self.yf_n = bx + (3 if self.one else 6)
        self.nx1, self.ny1 = gx * bx // 2, gy * by // 2
        self.rows1 = self.ny1 + SIDE
        self.rows1p = -(-self.rows1 // 16) * 16
        self.l1 = bz
        self.c1_rows = by // 2 + 4
        self.c2_rows = by // 2 + 8
        self.edge = 5
        self.edge_sets = 1 if self.one else 2
        self.pack1 = self.c1_n * self.c1_rows + self.edge_sets * self.edge * 2 * by
        self.pack2 = self.c2_n * self.c2_rows + self.yf_n * 8

    def c1_first(self, i):
        return -i if self.one else -1

    def c2_first(self, i):
        return -2 * i if self.one else -2

    def yf_first(self, i):
        return -3 * i if self.one else -3


def slab_kernel(k, p_ref, w_ref, right_ref, left_ref):
    bx, bz = k.bx, k.bz
    half, part = bz // 2, bz // 4
    lane = iota((k.by, bz), 1)
    for x in range(bx):
        p = pltpu.roll(p_ref[x], half, 1)
        a, b = w_ref[0, x], w_ref[1, x]
        right_ref[x] = jnp.where(lane < half, p, jnp.where(lane < half + part, pltpu.roll(a, bz - part, 1), b))
        left_ref[x] = jnp.where(lane >= half, p, jnp.where(lane < part, a, pltpu.roll(b, part, 1)))
    for q in range(-(-bx // 4)):
        r_all, l_all = jnp.zeros((k.by, bz), jnp.float32), jnp.zeros((k.by, bz), jnp.float32)
        for r in range(min(4, bx - 4 * q)):
            c = w_ref[2, 4 * q + r]
            here = (lane >= part * r) & (lane < part * (r + 1))
            r_all = jnp.where(here, pltpu.roll(c, (part * r + part) % bz, 1), r_all)
            l_all = jnp.where(here, pltpu.roll(c, part * r, 1) if r else c, l_all)
        right_ref[bx + q] = r_all
        left_ref[bx + q] = l_all


def lane_roll(v, shift):
    shift = shift % v.shape[1]
    return pltpu.roll(v, shift, 1) if shift else v


def pressure_window(k, p, low, high):
    half = k.bz // 2
    lane = iota(p.shape, 1)
    p = pltpu.roll(p, half, 1)
    return jnp.concatenate([jnp.where(lane < half, low, p), jnp.where(lane < half, p, high)], axis=1)


def wind_window(k, w, low, low_at, high, high_at):
    half, part = k.bz // 2, k.bz // 4
    lane = iota(w.shape, 1)
    w = pltpu.roll(w, half, 1)
    first = jnp.where(lane >= half, w, jnp.where(lane >= part, lane_roll(low, part - low_at), 0.0))
    second = jnp.where(lane < half, w, jnp.where(lane < half + part, lane_roll(high, half - high_at), 0.0))
    return jnp.concatenate([first, second], axis=1)


def place():
    return lax.axis_index("gx"), lax.axis_index("gy"), lax.axis_index("gz")


def fine_mask(k, iy, iz):
    return window_mask((k.rows, k.lanes), iy * k.by - SIDE, k.gy * k.by, iz * k.bz - k.bz // 2, k.gz * k.bz)


def x_inside(k, ix, plane):
    place_x = ix * k.bx + plane
    return jnp.where((place_x >= 0) & (place_x < k.gx * k.bx), 1.0, 0.0).astype(jnp.float32)


def restrict_planes(src, first, n, half_ref, out, value):
    rows, lanes = src.shape[1], src.shape[2]
    a = pair_matrix(lanes, half_ref.shape[2], value)

    def step(j):
        s = src[first + 2 * j] + src[first + 2 * j + 1]
        half_ref[j] = dot(s + up(s, 0), a)

    for j in range(n):
        step(j)
    for j in range(n):
        out[j] = half_ref[j, pl.ds(0, rows // 2, stride=2), :]


def zero(ref):
    ref[...] = jnp.zeros(ref.shape, ref.dtype)


def first_kernel(k, p_ref, low_ref, high_ref, win_ref, send_a, send_b, pack_ref, b, m, half_ref, c1):
    ix, iy, iz = place()
    bx, by = k.bx, k.by
    pad = 3
    zero(b)
    zero(m)
    for x in range(bx):
        w = pressure_window(k, p_ref[x], low_ref[x], high_ref[x])
        win_ref[x] = w
        b[x + pad, SIDE:SIDE + by, :] = w
    tail = lax.rem(iy, 2) == 0
    for x in range(bx):
        head_rows, tail_rows = win_ref[x, :8, :], win_ref[x, by - 8:, :]
        send_a[x] = jnp.where(tail, tail_rows, head_rows)
        send_b[x] = jnp.where(tail, head_rows, tail_rows)
    mask = fine_mask(k, iy, iz)

    def step1(i):
        m[i + pad - 1] = mix(b, i + pad - 1) * (mask * x_inside(k, ix, i - 1))

    each(bx + 2, step1)

    def step2(i):
        b[i + pad - 2] = mix(m, i + pad - 2)

    each(bx + 4, step2)
    restrict_planes(b, pad - 2, bx // 2 + 2, half_ref, c1, 0.125)
    start = (k.c1_first(ix) + 1) if k.one else 0
    for j in range(k.c1_n):
        pack_ref[j * k.c1_rows:(j + 1) * k.c1_rows, :] = c1[start + j, 2:2 + k.c1_rows, :]
    at = k.c1_n * k.c1_rows
    starts = [(1 - ix) * (bx - k.edge)] if k.one else [0, bx - k.edge]
    for first in starts:
        for j in range(k.edge):
            for t in range(2):
                pack_ref[at:at + by, :] = win_ref[first + j, :, t * k.bz:(t + 1) * k.bz]
                at += by


def coarse(k, iz, b1, m1, e1, half_ref, b2, u2, v2):
    n1, n2 = k.nx1, k.nx1 // 2
    rows1, rows2, l1 = k.rows1, k.rows1p // 2, k.l1
    y0 = -(SIDE // 2)
    mask1 = window_mask((rows1, l1), y0, k.ny1, iz * (k.bz // 2) - k.bz // 4, k.gz * (k.bz // 2))
    lane2 = iota((rows2, l1), 1)
    mask2 = window_mask((rows2, l1), y0 // 2, k.ny1 // 2, iz * (k.bz // 4) - k.bz // 8, k.gz * (k.bz // 4))
    mask2 = jnp.where(lane2 < l1 // 2, mask2, 0.0)
    zero(m1)
    zero(e1)
    zero(u2)
    zero(v2)
    for i in range(n1):
        b1[i + 2] = b1[i + 2] * mask1

    def pre(i):
        c = mix(b1, i + 2) * mask1
        m1[i + 2] = c
        e1[i + 2] = C1 * (b1[i + 2] + c)

    each(n1, pre)
    a = pair_matrix(l1, l1, 0.125)
    for j in range(n2):
        s = mix(m1, 2 * j + 2) + mix(m1, 2 * j + 3)
        half_ref[j, :rows1, :] = dot(s + up(s, 0), a)
        if k.rows1p > rows1:
            half_ref[j, rows1:, :] = jnp.zeros((k.rows1p - rows1, l1), jnp.float32)
    for j in range(n2):
        s = half_ref[j, pl.ds(0, rows2, stride=2), :] * (mask2 * C2)
        b2[j] = s
        u2[j + 1] = s
    src, dst = u2, v2
    for _ in range(3):
        for j in range(n2):
            dst[j + 1] = (mix(src, j + 1) + b2[j]) * mask2
        src, dst = dst, src
    spread = spread_matrix(l1, l1)
    for j in range(n2):
        e = dot(src[j + 1], spread)
        half_ref[j, pl.ds(0, rows2, stride=2), :] = e
        half_ref[j, pl.ds(1, rows2, stride=2), :] = e
    for j in range(n2):
        e = half_ref[j, :rows1, :]
        e1[2 * j + 2] += e
        e1[2 * j + 3] += e
    for src, dst in ((e1, m1), (m1, e1)):

        def post(i):
            dst[i + 2] = (mix(src, i + 2) + C1 * b1[i + 2]) * mask1

        each(n1, post)


def prolonged(k, e1, ix, iy, first, n, half_ref, put):
    by = k.by
    for j in range(n):
        e = e1[ix * (k.bx // 2) + (first + j + 2), pl.ds(pl.multiple_of(iy * (by // 2), 8), k.rows // 2), :]
        half_ref[j, pl.ds(0, k.rows // 2, stride=2), :] = e
        half_ref[j, pl.ds(1, k.rows // 2, stride=2), :] = e
    spread = spread_matrix(k.l1, k.lanes)
    for j in range(n):
        put(j, dot(half_ref[j], spread))


def overlap_add(k, g_ref, b1, n, rows, y_skip, first_of):
    zero(b1)
    for i in range(k.gx):
        for j in range(k.gy):
            at_y = j * (k.by // 2) + y_skip
            for q in range(n):
                x = i * (k.bx // 2) + first_of(i) + q
                if 0 <= x < k.nx1:
                    part = g_ref[i * k.gy + j, q * rows:(q + 1) * rows, :]
                    b1[x + 2, at_y:at_y + rows, :] += part


def own_lanes(k, v):
    half = k.bz // 2
    first, second = v[:, :k.bz], v[:, k.bz:]
    lane = iota(first.shape, 1)
    return jnp.where(lane < half, pltpu.roll(first, half, 1), pltpu.roll(second, half, 1))


def assemble_edges(k, refs, b1, b, pad):
    g_ref, win_ref, got_a, got_b, w_ref, low_ref, high_ref = refs
    ix, iy, iz = place()
    bx, by = k.bx, k.by
    overlap_add(k, g_ref, b1, k.c1_n, k.c1_rows, 2, k.c1_first)
    even = lax.rem(iy, 2) == 0
    for x in range(bx):
        b[x + pad, :SIDE, :] = jnp.where(even, got_b[x], got_a[x])
        b[x + pad, SIDE:SIDE + by, :] = win_ref[x]
        b[x + pad, SIDE + by:, :] = jnp.where(even, got_a[x], got_b[x])
    base = k.c1_n * k.c1_rows
    span = k.edge * 2 * by
    y_low, y_high = jnp.maximum(iy - 1, 0), jnp.minimum(iy + 1, k.gy - 1)
    for side in range(2):
        if k.one:
            who, shift = 1 - ix, 0
        else:
            who = jnp.maximum(ix - 1, 0) if side == 0 else jnp.minimum(ix + 1, k.gx - 1)
            shift = span if side == 0 else 0
        for j in range(k.edge):
            at = pad - k.edge + j if side == 0 else pad + bx + j
            for t in range(2):
                row = base + shift + (2 * j + t) * by
                lanes = slice(t * k.bz, (t + 1) * k.bz)
                b[at, :SIDE, lanes] = g_ref[who * k.gy + y_low, row + by - 8:row + by, :]
                b[at, SIDE:SIDE + by, lanes] = g_ref[who * k.gy + iy, row:row + by, :]
                b[at, SIDE + by:, lanes] = g_ref[who * k.gy + y_high, row:row + 8, :]
    half, part = k.bz // 2, k.bz // 4

    def winds(x):
        low, high = low_ref[x], high_ref[x]
        q, r = x // 4, x % 4
        return (wind_window(k, w_ref[0, x], low, half, high, 0),
                wind_window(k, w_ref[1, x], low, half + part, high, part),
                wind_window(k, w_ref[2, x], low_ref[bx + q], part * r, high_ref[bx + q], part * r))

    return winds


def middle_kernel(k, assemble, ins, pack_ref, xa_ref, xb_ref, own_ref,
                  b1, m1, e1, half1, b2, u2, v2, b, m, v, vel, flux, half_ref, c2):
    ix, iy, iz = place()
    bx, by = k.bx, k.by
    pad = 5
    winds = assemble(k, ins, b1, b, pad)
    coarse(k, iz, b1, m1, e1, half1, b2, u2, v2)
    mask = fine_mask(k, iy, iz)

    def clean(i):
        b[i] = b[i] * (mask * x_inside(k, ix, i - pad))

    each(bx + 2 * pad, clean)

    def put(j, e):
        for t in range(2):
            v[pad - 4 + 2 * j + t] = e

    prolonged(k, e1, ix, iy, -2, bx // 2 + 4, half_ref, put)

    def pre(i):
        at = i + pad - 4
        here = mask * x_inside(k, ix, i - 4)
        v[at] = (v[at] + C0 * (b[at] + mix(b, at))) * here

    each(bx + 8, pre)

    def post1(i):
        at = i + pad - 3
        m[at] = (mix(v, at) + C0 * b[at]) * (mask * x_inside(k, ix, i - 3))

    each(bx + 6, post1)

    def post2(i):
        at = i + pad - 2
        v[at] = (mix(m, at) + C0 * b[at]) * (mask * x_inside(k, ix, i - 2))

    each(bx + 4, post2)

    def speed(i):
        at = i + pad - 1
        here = 0.5 * (mask * x_inside(k, ix, i - 1))
        c = v[at]
        vel[0, i] = (v[at + 1] - v[at - 1]) * here
        vel[1, i] = (up(c, 0) - down(c, 0)) * here
        vel[2, i] = (up(c, 1) - down(c, 1)) * here

    each(bx + 2, speed)
    own_mask = mask[SIDE:SIDE + by, :]
    zero(flux)
    for x in range(bx):
        w0, w1, w2 = (0.5 * w for w in winds(x))
        for d in range(3):
            c = vel[d, x + 1, SIDE:SIDE + by, :]
            xp, xm = vel[d, x + 2, SIDE:SIDE + by, :], vel[d, x, SIDE:SIDE + by, :]
            yp, ym = vel[d, x + 1, SIDE + 1:SIDE + by + 1, :], vel[d, x + 1, SIDE - 1:SIDE + by - 1, :]
            zp, zm = up(c, 1), down(c, 1)
            near = (xp + xm) + (yp + ym) + (zp + zm)
            total = 7.0 * c - near + w0 * (xp - xm) + w1 * (yp - ym) + w2 * (zp - zm)
            flux[d, x + 2, SIDE:SIDE + by, :] = total * own_mask
    zero(b)
    zero(m)

    def spread_flux(i):
        at = i + pad - 1
        f1, f2 = flux[1, i + 1], flux[2, i + 1]
        total = (flux[0, i + 2] - flux[0, i]) + (up(f1, 0) - down(f1, 0)) + (up(f2, 1) - down(f2, 1))
        b[at] = total * (-0.5 * (mask * x_inside(k, ix, i - 1)))

    each(bx + 2, spread_flux)
    zero(v)

    def power1_pure(i):
        at = i + pad - 2
        m[at] = mix(b, at) * (mask * x_inside(k, ix, i - 2))

    each(bx + 4, power1_pure)

    def power2(i):
        at = i + pad - 3
        v[at] = mix(m, at) * (mask * x_inside(k, ix, i - 3))

    each(bx + 6, power2)

    def power3(i):
        at = i + pad - 4
        b[at] = C0 * ((b[at] + m[at]) + (v[at] + mix(v, at))) * (mask * x_inside(k, ix, i - 4))

    each(bx + 8, power3)
    restrict_planes(v, pad - 4, bx // 2 + 4, half_ref, c2, 0.125)
    start = (k.c2_first(ix) + 2) if k.one else 0
    for j in range(k.c2_n):
        pack_ref[j * k.c2_rows:(j + 1) * k.c2_rows, :] = c2[start + j]
    row8 = iota((8, k.bz), 0)
    at = k.c2_n * k.c2_rows
    start = (k.yf_first(ix) if k.one else -3) + pad
    for j in range(k.yf_n):
        c = own_lanes(k, jnp.where(iota((8, k.lanes), 0) < 4, b[start + j, SIDE + by:, :], b[start + j, :SIDE, :]))
        pack_ref[at:at + 8, :] = c
        at += 8
    upper = lax.rem(ix, 2) == 0
    first_a = pad + jnp.where(upper, bx, -4)
    first_b = pad + jnp.where(upper, -4, bx)
    for j in range(4):
        xa_ref[j] = own_lanes(k, b[first_a + j, SIDE:SIDE + by, :])
        if xb_ref is not None:
            xb_ref[j] = own_lanes(k, b[first_b + j, SIDE:SIDE + by, :])
    for x in range(bx):
        own_ref[x] = own_lanes(k, b[x + pad, SIDE:SIDE + by, :])


def last_kernel(k, g_ref, own_ref, xa_ref, xb_ref, out_ref, b1, m1, e1, half1, b2, u2, v2, v, m, half_ref):
    ix, iy, iz = place()
    bx, by = k.bx, k.by
    overlap_add(k, g_ref, b1, k.c2_n, k.c2_rows, 0, k.c2_first)
    coarse(k, iz, b1, m1, e1, half1, b2, u2, v2)
    pad = 2
    mask = fine_mask(k, iy, iz)

    def put(j, e):
        for t in range(2):
            plane = -2 + 2 * j + t
            v[pad + plane] = e * (mask * x_inside(k, ix, plane))

    prolonged(k, e1, ix, iy, -1, bx // 2 + 2, half_ref, put)

    def post1(i):
        at = i + pad - 1
        m[at] = mix(v, at) * (mask * x_inside(k, ix, i - 1))

    each(bx + 2, post1)
    base = k.c2_n * k.c2_rows
    low_ok = jnp.where(iy > 0, 1.0, 0.0).astype(jnp.float32)
    high_ok = jnp.where(iy < k.gy - 1, 1.0, 0.0).astype(jnp.float32)
    y_low, y_high = jnp.maximum(iy - 1, 0), jnp.minimum(iy + 1, k.gy - 1)
    row8 = iota((8, k.bz), 0)
    low_keep = jnp.where(row8 < 4, low_ok, 0.0)
    high_keep = jnp.where(row8 >= 4, high_ok, 0.0)
    for x in range(bx):
        out_ref[x] = own_lanes(k, mix(m, x + pad)[SIDE:SIDE + by, :]) + own_ref[x]

    def frame(who, first, x_from, x_to, ok):
        for x in range(x_from, x_to):
            row = base + (x - first) * 8
            if not isinstance(row, int):
                row = pl.multiple_of(row, 8)
            lo = g_ref[who * k.gy + y_low, pl.ds(row, 8), :] * ok
            hi = g_ref[who * k.gy + y_high, pl.ds(row, 8), :] * ok
            out_ref[x, :8, :] += lo * low_keep
            out_ref[x, by - 8:, :] += hi * high_keep

    one = jnp.float32(1.0)
    frame(ix, k.yf_first(ix), 0, bx, one)
    upper = lax.rem(ix, 2) == 0
    if k.one:
        for j in range(3):
            x = jnp.where(ix == 0, bx - 3 + j, j)
            row = pl.multiple_of(base + jnp.where(ix == 0, j, bx + j) * 8, 8)
            lo = g_ref[(1 - ix) * k.gy + y_low, pl.ds(row, 8), :]
            hi = g_ref[(1 - ix) * k.gy + y_high, pl.ds(row, 8), :]
            out_ref[x, :8, :] += lo * low_keep
            out_ref[x, by - 8:, :] += hi * high_keep
    else:
        frame(jnp.maximum(ix - 1, 0), -3 - bx, 0, 3, jnp.where(ix > 0, 1.0, 0.0).astype(jnp.float32))
        frame(jnp.minimum(ix + 1, k.gx - 1), bx - 3, bx - 3, bx, jnp.where(ix < k.gx - 1, 1.0, 0.0).astype(jnp.float32))
    for j in range(4):
        out_ref[jnp.where(upper, bx - 4, 0) + j] += xa_ref[j]
        if xb_ref is not None:
            out_ref[jnp.where(upper, 0, bx - 4) + j] += xb_ref[j]


def call(kernel, outs, scratch, args, flops):
    f32 = lambda s: jax.ShapeDtypeStruct(s, jnp.float32)
    return pl.pallas_call(
        kernel,
        out_shape=[f32(s) for s in outs],
        scratch_shapes=[pltpu.VMEM(s, jnp.float32) for s in scratch],
        compiler_params=pltpu.CompilerParams(vmem_limit_bytes=40 * 1024 * 1024),
        cost_estimate=pl.CostEstimate(flops=flops, bytes_accessed=1 << 20, transcendentals=0),
    )(*args)


def pairs(n):
    first = [(i, i ^ 1) for i in range(n) if (i ^ 1) < n]
    second = [(i + s, i + 1 - s) for i in range(1, n - 1, 2) for s in (0, 1)]
    return first, second


def chain(n, step):
    return [(i, i + step) for i in range(n) if 0 <= i + step < n]


def coarse_scratch(k):
    n1, n2, rows2 = k.nx1, k.nx1 // 2, k.rows1p // 2
    big = (n1 + 4, k.rows1, k.l1)
    return [big, big, big, (n2, k.rows1p, k.l1), (n2, rows2, k.l1), (n2 + 2, rows2, k.l1), (n2 + 2, rows2, k.l1)]


def edge_form(k, pressure, wind):
    bx, by, bz = k.bx, k.by, k.bz
    slab = (bx + -(-bx // 4), by, bz)
    right, left = call(functools.partial(slab_kernel, k), [slab, slab], [], (pressure, wind), 1 << 20)
    low = lax.ppermute(right, "gz", chain(k.gz, 1))
    high = lax.ppermute(left, "gz", chain(k.gz, -1))
    fine = lambda n: (n, k.rows, k.lanes)
    window, send_a, send_b, pack = call(
        functools.partial(first_kernel, k),
        [(bx, by, k.lanes), (bx, 8, k.lanes), (bx, 8, k.lanes), (k.pack1, bz)],
        [fine(bx + 6), fine(bx + 6), (bx // 2 + 2, k.rows, k.l1), (bx // 2 + 2, k.rows // 2, k.l1)],
        (pressure, low, high), 1 << 22)
    ya, yb = pairs(k.gy)
    got_a = lax.ppermute(send_a, "gy", ya)
    got_b = lax.ppermute(send_b, "gy", yb)
    gathered = lax.all_gather(pack, PLANE)
    return assemble_edges, (gathered, window, got_a, got_b, wind, low, high)


def general(k, pressure, wind):
    bx, by, bz = k.bx, k.by, k.bz
    fine = lambda n: (n, k.rows, k.lanes)
    assemble, args = edge_form(k, pressure, wind)
    xa, xb = pairs(k.gx)
    x_outs = [(4, by, bz)] * (2 if xb else 1)

    def middle(*refs):
        ins, rest = refs[:len(args)], refs[len(args):]
        pack_ref, rest = rest[0], rest[1:]
        xa_ref, rest = rest[0], rest[1:]
        xb_ref = None
        if xb:
            xb_ref, rest = rest[0], rest[1:]
        middle_kernel(k, assemble, ins, pack_ref, xa_ref, xb_ref, *rest)

    big = fine(bx + 10)
    outs = call(
        middle, [(k.pack2, bz)] + x_outs + [(bx, by, bz)],
        coarse_scratch(k) + [big, big, big, (3,) + fine(bx + 2), (3,) + fine(bx + 4),
                             (bx // 2 + 4, k.rows, k.l1), (bx // 2 + 4, k.rows // 2, k.l1)],
        args, 1 << 24)
    pack, frames, own = outs[0], outs[1:-1], outs[-1]
    got = [lax.ppermute(f, "gx", perm) for f, perm in zip(frames, (xa, xb))]
    gathered = lax.all_gather(pack, PLANE)

    def last(*refs):
        g_ref, own_ref, xa_ref, rest = refs[0], refs[1], refs[2], refs[3:]
        xb_ref = None
        if xb:
            xb_ref, rest = rest[0], rest[1:]
        last_kernel(k, g_ref, own_ref, xa_ref, xb_ref, *rest)

    (result,) = call(
        last, [(bx, by, bz)],
        coarse_scratch(k) + [fine(bx + 4), fine(bx + 4), (bx // 2 + 2, k.rows, k.l1)],
        (gathered, own, *got), 1 << 23)
    return result

FR = 5
CR = 2


class Mirror:
    def __init__(self, gx, gy, gz, bx, by, bz):
        self.gx, self.gy, self.gz, self.bx, self.by, self.bz = gx, gy, gz, bx, by, bz
        self.rows = by + 2 * FR
        self.core = by + 8
        self.nx, self.ny = gx * bx, gy * by
        self.nx1, self.ny1 = self.nx // 2, self.ny // 2
        self.rows1 = self.ny1 + 8
        self.part = bz // 4
        groups = lambda n: -(-n // 4)
        self.fine_n = bx + 5
        self.at_fine = groups(self.nx1) * self.ny1
        self.at_wind = self.at_fine + groups(self.fine_n) * self.rows
        self.slab_rows = self.at_wind + groups(3 * bx) * by
        self.c2_n, self.c2_rows = bx // 2 + 2, by // 2 + 4
        self.c2 = self.c2_n * self.c2_rows
        self.yf_n = bx + 3
        self.to3 = self.c2 + 8 * self.yf_n
        self.to4 = self.c2 + 8 * 3 + 4 * by
        self.to7 = self.c2 + 8 * 3
        self.to1 = 4 * self.c2 + 8 * self.yf_n + 8 * 3


def exact_dot(x, a):
    high = x.astype(jnp.bfloat16)
    low = (x - high.astype(jnp.float32)).astype(jnp.bfloat16)
    return (jnp.dot(high, a, preferred_element_type=jnp.float32)
            + jnp.dot(low, a, preferred_element_type=jnp.float32))


def matrix(hit, value):
    return jnp.where(hit, value, 0.0).astype(jnp.float32).astype(jnp.bfloat16)


def flag(good):
    return jnp.where(good, 1.0, 0.0).astype(jnp.float32)


def beside(c0, c1):
    n = c0.shape[1]
    lane = iota(c0.shape, 1)
    last, first = lane == n - 1, lane == 0
    u0, u1, d0, d1 = up(c0, 1), up(c1, 1), down(c0, 1), down(c1, 1)
    return ((jnp.where(last, u1, u0), jnp.where(last, u0, u1)),
            (jnp.where(first, d1, d0), jnp.where(first, d0, d1)))


def mix_halves(s, i, halves=2):
    n = s.shape[2] - 2
    c = [s[i + 1, h, 1:1 + n, :] for h in range(2)]
    plus, minus = beside(*c)
    out = []
    for h in range(halves):
        near = (s[i, h, 1:1 + n, :] + s[i + 2, h, 1:1 + n, :]) + (s[i + 1, h, 2:2 + n, :] + s[i + 1, h, :n, :])
        out.append((1.0 - OMEGA) * c[h] + W * (near + (plus[h] + minus[h])))
    return out


def halves_mask(k, iy, iz):
    y = iota((k.core, k.bz), 0) + (iy * k.by - 4)
    lane = iota((k.core, k.bz), 1)
    y_good = (y >= 0) & (y < k.ny)
    edge = flag(y_good)
    side = jnp.where(lane < k.bz // 2, jnp.where(iz < k.gz - 1, 1.0, 0.0), jnp.where(iz > 0, 1.0, 0.0))
    return edge, edge * side.astype(jnp.float32)


def zero_rim(s):
    s[0] = jnp.zeros(s.shape[1:], jnp.float32)
    n = s.shape[2]
    for i in range(1, s.shape[0]):
        for h in range(2):
            s[i, h, 0:1, :] = jnp.zeros((1, s.shape[3]), jnp.float32)
            s[i, h, n - 1:n, :] = jnp.zeros((1, s.shape[3]), jnp.float32)


def mix1(k, s, i, n, at):
    c = s[i + 1, at:at + n, :]
    near = (s[i, at:at + n, :] + s[i + 2, at:at + n, :]) + (s[i + 1, at + 1:at + n + 1, :] + s[i + 1, at - 1:at + n - 1, :])
    return (1.0 - OMEGA) * c + W * (near + (up(c, 1) + down(c, 1)))


def coarse_plane(k, iz, b1, m1, e1, half_ref, b2, u2, v2):
    n1, n2, ny, l1 = k.nx1, k.nx1 // 2, k.ny1, k.bz
    ny2 = ny // 2
    lane = iota((ny, l1), 1)
    low_ok, high_ok = flag(iz > 0), flag(iz < k.gz - 1)
    mask1 = jnp.where(lane < l1 // 2, 1.0, jnp.where(lane < 3 * l1 // 4, high_ok, low_ok))
    lane2 = iota((ny2, l1), 1)
    own2 = l1 // 8
    mask2 = jnp.where(lane2 < own2, low_ok, jnp.where(lane2 < 3 * own2, 1.0, jnp.where(lane2 < 4 * own2, high_ok, 0.0)))
    for s in (m1, e1):
        for i in (0, n1 + 1):
            s[i] = jnp.zeros(s.shape[1:], jnp.float32)
    for s in (b1, m1, e1):
        for i in range(n1):
            s[i + 1, :CR, :] = jnp.zeros((CR, l1), jnp.float32)
            s[i + 1, CR + ny:, :] = jnp.zeros((k.rows1 - CR - ny, l1), jnp.float32)
    zero(u2)
    zero(v2)
    for i in range(n1):
        b1[i + 1, CR:CR + ny, :] = b1[i + 1, CR:CR + ny, :] * mask1
    for i in range(n1):
        c = mix1(k, b1, i, ny, CR) * mask1
        m1[i + 1, CR:CR + ny, :] = c
        e1[i + 1, CR:CR + ny, :] = C1 * (b1[i + 1, CR:CR + ny, :] + c)
    row, column = iota((l1, l1), 0), iota((l1, l1), 1)
    linear = lambda x: (jnp.where(x < 3 * l1 // 4, x, x - l1) >> 1) + own2
    for j in range(n2):
        half_ref[j] = mix1(k, m1, 2 * j, ny, CR) + mix1(k, m1, 2 * j + 1, ny, CR)
    pairs_sum = [half_ref[j, pl.ds(0, ny2, stride=2), :] + half_ref[j, pl.ds(1, ny2, stride=2), :] for j in range(n2)]
    r2 = exact_dot(jnp.concatenate(pairs_sum, axis=0), matrix(linear(row) == column, 0.125))
    for j in range(n2):
        c = r2[j * ny2:(j + 1) * ny2] * (mask2 * C2)
        b2[j] = c
        u2[j + 1, 1:1 + ny2, :] = c
    src, dst = u2, v2
    for _ in range(3):
        for j in range(n2):
            dst[j + 1, 1:1 + ny2, :] = (mix1(k, src, j, ny2, 1) + b2[j]) * mask2
        src, dst = dst, src
    stack = jnp.concatenate([src[j + 1, 1:1 + ny2, :] for j in range(n2)], axis=0)
    spread = exact_dot(stack, matrix(row == linear(column), 1.0))
    for j in range(n2):
        e = spread[j * ny2:(j + 1) * ny2]
        half_ref[j, pl.ds(0, ny2, stride=2), :] = e
        half_ref[j, pl.ds(1, ny2, stride=2), :] = e
    for j in range(n2):
        e = half_ref[j]
        for t in range(2):
            e1[2 * j + t + 1, CR:CR + ny, :] = e1[2 * j + t + 1, CR:CR + ny, :] + e
    for src, dst in ((e1, m1), (m1, e1)):
        for i in range(n1):
            dst[i + 1, CR:CR + ny, :] = (mix1(k, src, i, ny, CR) + C1 * b1[i + 1, CR:CR + ny, :]) * mask1


def from_end(ix, i, count):
    return jnp.where(ix == 0, i, count - 1 - i)


def prolong_halves(k, iy, e1, n, v):
    half, rows = k.bz // 2, k.core // 2
    first = pl.multiple_of(iy * (k.by // 2), 8)
    stack = jnp.concatenate([e1[j + 1, pl.ds(first, 16), :] for j in range(n)], axis=0)
    row, column = iota((k.bz, 2 * k.bz), 0), iota((k.bz, 2 * k.bz), 1)
    spread = exact_dot(stack, matrix(row == (column >> 1), 1.0))
    for j in range(n):
        for h in range(2):
            e = spread[16 * j:16 * j + rows, h * k.bz:(h + 1) * k.bz]
            for t in range(2):
                v[2 * j + t + 1, h, pl.ds(1, rows, stride=2), :] = e
                v[2 * j + t + 1, h, pl.ds(2, rows, stride=2), :] = e


def take_slab(k, ref, base, rows, i, to):
    at = base + (i // 4) * rows
    return lane_roll(ref[at:at + rows, :], to - k.part * (i % 4))


def plane_kernel(k, g_ref, w_ref, c1_ref, win_ref, right_ref, left_ref, p, m, q, half_ref):
    ix, iy, iz = place()
    bx, by, bz, nx, ny, part = k.bx, k.by, k.bz, k.nx, k.ny, k.part
    p[0] = jnp.zeros(p.shape[1:], jnp.float32)
    p[nx + 1] = jnp.zeros(p.shape[1:], jnp.float32)
    m[0] = jnp.zeros(m.shape[1:], jnp.float32)
    m[nx + 1] = jnp.zeros(m.shape[1:], jnp.float32)
    for x in range(nx):
        p[x + 1, :FR, :] = jnp.zeros((FR, bz), jnp.float32)
        p[x + 1, FR + ny:, :] = jnp.zeros((p.shape[1] - FR - ny, bz), jnp.float32)
        m[x + 1, 0:1, :] = jnp.zeros((1, bz), jnp.float32)
        m[x + 1, ny + 1:, :] = jnp.zeros((m.shape[1] - ny - 1, bz), jnp.float32)
        who = ix if x < bx else 1 - ix
        for j in range(k.gy):
            p[x + 1, FR + j * by:FR + (j + 1) * by, :] = g_ref[who * k.gy + j, from_end(ix, x % bx, bx)]
    lane = iota((ny, bz), 1)
    first, last = lane == 0, lane == bz - 1
    ends = jnp.where(first, flag(iz > 0), jnp.where(last, flag(iz < k.gz - 1), 0.0)) * (W * W)

    def parts(s, x, at):
        c = s[x + 1, at:at + ny, :]
        four = (s[x, at:at + ny, :] + s[x + 2, at:at + ny, :]) + (s[x + 1, at + 1:at + ny + 1, :] + s[x + 1, at - 1:at + ny - 1, :])
        along = jnp.where(last, 0.0, up(c, 1)) + jnp.where(first, 0.0, down(c, 1))
        return c, four, (1.0 - OMEGA) * c + W * (four + along)

    for x in range(nx):
        c, four, mixed = parts(p, x, FR)
        m[x + 1, 1:1 + ny, :] = mixed
        q[x] = (1.0 - OMEGA + W) * c + (mixed + W * four)
    row, column = iota((bz, bz), 0), iota((bz, bz), 1)
    own = matrix((row >> 1) == column, 0.125)
    rim = ((row == 0) & (column == bz - 1)) | ((row == bz - 1) & (column == bz // 2))
    rim = matrix(rim, 0.125)
    half_rows = ny // 2
    for j in range(k.nx1):
        s = None
        for x in (2 * j, 2 * j + 1):
            r = parts(m, x, 1)[2] + ends * p[x + 1, FR:FR + ny, :]
            s = r if s is None else s + r
        half_ref[j] = s
        t = (q[2 * j, pl.ds(0, half_rows, stride=2), :] + q[2 * j, pl.ds(1, half_rows, stride=2), :]
             + q[2 * j + 1, pl.ds(0, half_rows, stride=2), :] + q[2 * j + 1, pl.ds(1, half_rows, stride=2), :])
        s = half_ref[j, pl.ds(0, half_rows, stride=2), :] + half_ref[j, pl.ds(1, half_rows, stride=2), :]
        c1_ref[j] = exact_dot(s, own) + exact_dot(W * t, rim)

    def pack(ref, base, rows, n, load, from_lane):
        lane = iota((rows, bz), 1)
        for group in range(-(-n // 4)):
            total = jnp.zeros((rows, bz), jnp.float32)
            for r in range(min(4, n - 4 * group)):
                moved = lane_roll(load(4 * group + r), part * r - from_lane)
                total = jnp.where((lane >= part * r) & (lane < part * (r + 1)), moved, total)
            ref[base + group * rows:base + (group + 1) * rows, :] = total

    for i in range(k.fine_n):
        win_ref[i] = p[i + 1, pl.ds(pl.multiple_of(iy * by, 8), k.rows), :]
    for ref, lane1, lane0 in ((right_ref, part + 1, 3 * part), (left_ref, bz - 1, 0)):
        pack(ref, 0, k.ny1, k.nx1, lambda i: c1_ref[i], lane1)
        pack(ref, k.at_fine, k.rows, k.fine_n, lambda i: win_ref[i], lane0)
        pack(ref, k.at_wind, by, 3 * bx, lambda i: w_ref[i // bx, from_end(ix, i % bx, bx)], lane0)


def solve_kernel(k, c1_ref, win_ref, w_ref, low_ref, high_ref, to3_ref, to4_ref, to7_ref, own_ref,
                 b1, m1, e1, half1, b2, u2, v2, b, m, v, vel, flux, half_ref):
    ix, iy, iz = place()
    bx, by, bz, part, n = k.bx, k.by, k.bz, k.part, k.core
    lane = iota((k.ny1, bz), 1)
    for s in (b1,):
        for i in (0, k.nx1 + 1):
            s[i] = jnp.zeros(s.shape[1:], jnp.float32)
    for x in range(k.nx1):
        low = take_slab(k, low_ref, 0, k.ny1, x, 3 * part + 1)
        high = take_slab(k, high_ref, 0, k.ny1, x, 2 * part - 1)
        low = jnp.where((lane >= 3 * part + 1) | (lane == 0), low, 0.0)
        high = jnp.where((lane >= 2 * part - 1) & (lane < 3 * part - 1), high, 0.0)
        b1[x + 1, CR:CR + k.ny1, :] = c1_ref[x] + (low + high)
    coarse_plane(k, iz, b1, m1, e1, half1, b2, u2, v2)
    mask = halves_mask(k, iy, iz)
    for s in (b, m, v):
        zero_rim(s)

    def outer(low, high, lane):
        return jnp.where(lane >= 3 * part, low, jnp.where(lane < part, high, 0.0))

    lane = iota((k.rows, bz), 1)
    for i in range(k.fine_n):
        b[i + 1, 0] = win_ref[i]
        b[i + 1, 1] = outer(take_slab(k, low_ref, k.at_fine, k.rows, i, 3 * part),
                            take_slab(k, high_ref, k.at_fine, k.rows, i, 0), lane)
    prolong_halves(k, iy, e1, bx // 2 + 2, v)
    for i in range(bx + 4):
        mb = mix_halves(b, i)
        for h in range(2):
            v[i + 1, h, 1:1 + n, :] = (v[i + 1, h, 1:1 + n, :] + C0 * (b[i + 1, h, 1:1 + n, :] + mb[h])) * mask[h]
    for src, dst, count in ((v, m, bx + 3), (m, v, bx + 2)):
        for i in range(count):
            c = mix_halves(src, i)
            for h in range(2):
                dst[i + 1, h, 1:1 + n, :] = (c[h] + C0 * b[i + 1, h, 1:1 + n, :]) * mask[h]
    half_mask = [0.5 * c for c in mask]
    for d in range(3):
        vel[d, 0] = jnp.zeros(vel.shape[2:], jnp.float32)
    for i in range(bx + 1):
        plus, minus = beside(v[i + 1, 0, 1:1 + n, :], v[i + 1, 1, 1:1 + n, :])
        for h in range(2):
            vel[0, i + 1, h] = (v[i + 2, h, 1:1 + n, :] - v[i, h, 1:1 + n, :]) * half_mask[h]
            vel[1, i + 1, h] = (v[i + 1, h, 2:2 + n, :] - v[i + 1, h, :n, :]) * half_mask[h]
            vel[2, i + 1, h] = (plus[h] - minus[h]) * half_mask[h]
    own_at = 4
    zero(flux)
    sign = jnp.where(ix == 0, 0.5, -0.5).astype(jnp.float32)
    lane = iota((by, bz), 1)
    for x in range(bx):
        winds = []
        for d in range(3):
            low = take_slab(k, low_ref, k.at_wind, by, d * bx + x, 3 * part)
            high = take_slab(k, high_ref, k.at_wind, by, d * bx + x, 0)
            scale = sign if d == 0 else 0.5
            winds.append((scale * w_ref[d, from_end(ix, x, bx)], scale * outer(low, high, lane)))
        for d in range(3):
            at = lambda i, h, r: vel[d, i + 1, h, own_at + r:own_at + r + by, :]
            c = [at(x, h, 0) for h in range(2)]
            plus, minus = beside(*c)
            for h in range(2):
                xp, xm, yp, ym, zp, zm = at(x + 1, h, 0), at(x - 1, h, 0), at(x, h, 1), at(x, h, -1), plus[h], minus[h]
                near = (xp + xm) + (yp + ym) + (zp + zm)
                total = 7.0 * c[h] - near + winds[0][h] * (xp - xm) + winds[1][h] * (yp - ym) + winds[2][h] * (zp - zm)
                if h == 1:
                    total = total * mask[1][own_at:own_at + by]
                flux[d, x + 1, h, own_at + 1:own_at + 1 + by, :] = total
    minus_mask = [-0.5 * c for c in mask]
    for s, first in ((b, bx + 2), (m, bx + 3), (v, bx + 4)):
        for i in range(first, bx + 6):
            s[i] = jnp.zeros(s.shape[1:], jnp.float32)
    for i in range(bx + 1):
        plus, minus = beside(flux[2, i + 1, 0, 1:1 + n, :], flux[2, i + 1, 1, 1:1 + n, :])
        for h in range(2):
            total = (flux[0, i + 2, h, 1:1 + n, :] - flux[0, i, h, 1:1 + n, :]
                     + (flux[1, i + 1, h, 2:2 + n, :] - flux[1, i + 1, h, :n, :]) + (plus[h] - minus[h]))
            b[i + 1, h, 1:1 + n, :] = total * minus_mask[h]
    zero_rows = jnp.zeros((1, bz), jnp.float32)
    for i in range(bx + 1):
        for h in range(2):
            b[i + 1, h, 0:1, :] = zero_rows
            b[i + 1, h, n + 1:n + 2, :] = zero_rows
    for src, dst, count in ((b, m, bx + 2), (m, v, bx + 3)):
        for i in range(count):
            c = mix_halves(src, i)
            for h in range(2):
                dst[i + 1, h, 1:1 + n, :] = c[h] * mask[h]
    half_rows = n // 2
    for j in range(k.c2_n):
        for h in range(2):
            take = lambda i, r: v[i + 1, h, pl.ds(r, half_rows, stride=2), :]
            half_ref[h, j, :half_rows, :] = (take(2 * j, 1) + take(2 * j, 2)) + (take(2 * j + 1, 1) + take(2 * j + 1, 2))
            half_ref[h, j, half_rows:, :] = jnp.zeros((16 - half_rows, bz), jnp.float32)
    row, column = iota((bz, bz), 0), iota((bz, bz), 1)
    c2 = (exact_dot(half_ref[0].reshape(k.c2_n * 16, bz), matrix((row >> 1) == column, 0.125))
          + exact_dot(half_ref[1].reshape(k.c2_n * 16, bz), matrix((row >> 1) + bz // 2 == column, 0.125)))
    for j in range(k.c2_n):
        for ref in (to3_ref, to4_ref, to7_ref):
            ref[j * k.c2_rows:(j + 1) * k.c2_rows, :] = c2[16 * j:16 * j + k.c2_rows]
    for i in range(bx + 4):
        c = mix_halves(v, i, 1)[0]
        at = lambda s: s[i + 1, 0, 1:1 + n, :]
        c = C0 * ((at(b) + at(m)) + (at(v) + c)) * mask[0]
        if i < bx:
            own_ref[i] = c[4:4 + by]
        else:
            row = k.to7 + by * (i - bx)
            to4_ref[row:row + by, :] = c[4:4 + by]
        places = [(to3_ref, k.c2 + 8 * i)] if i < k.yf_n else []
        if bx <= i < k.yf_n:
            places += [(ref, k.c2 + 8 * (i - bx)) for ref in (to4_ref, to7_ref)]
        for ref, row in places:
            ref[row:row + 4, :] = c[4 + by:8 + by]
            ref[row + 4:row + 8, :] = c[:4]


def share_kernel(k, own_ref, got3_ref, got4_ref, got7_ref, out_ref):
    c2 = k.c2
    for n, ref in enumerate((own_ref, got3_ref, got4_ref, got7_ref)):
        out_ref[n * c2:(n + 1) * c2, :] = ref[:c2, :]
    out_ref[4 * c2:4 * c2 + 8 * k.yf_n, :] = own_ref[c2:, :]
    out_ref[4 * c2 + 8 * k.yf_n:, :] = got4_ref[c2:c2 + 24, :]


def close_kernel(k, mine_ref, got_ref, got3_ref, got4_ref, got7_ref, own_ref, out_ref,
                 parts, b1, m1, e1, half1, b2, u2, v2, v, m):
    ix, iy, iz = place()
    bx, by, bz, n, c2 = k.bx, k.by, k.bz, k.core, k.c2
    for slot, near, far in ((0, mine_ref, 0), (3, mine_ref, 1), (1, got_ref, 0), (2, got_ref, 1)):
        parts[slot] = near[far * c2:(far + 1) * c2, :]
        parts[4 + slot] = near[(2 + far) * c2:(3 + far) * c2, :]
    zero(b1)
    for side in range(2):
        for j in range(k.gy):
            at = j * (by // 2)
            slot = 4 * side + (iy ^ j)
            for q in range(k.c2_n):
                x = q if side == 0 else k.nx1 - 1 - q
                b1[x + 1, at:at + k.c2_rows, :] += parts[slot, q * k.c2_rows:(q + 1) * k.c2_rows, :]
    coarse_plane(k, iz, b1, m1, e1, half1, b2, u2, v2)
    mask = halves_mask(k, iy, iz)
    for s in (v, m):
        zero_rim(s)
    prolong_halves(k, iy, e1, bx // 2 + 1, v)
    for i in range(bx + 2):
        for h in range(2):
            v[i + 1, h, 1:1 + n, :] = v[i + 1, h, 1:1 + n, :] * mask[h]
    for i in range(bx + 1):
        c = mix_halves(v, i)
        for h in range(2):
            m[i + 1, h, 1:1 + n, :] = c[h] * mask[h]
    odd = lax.rem(iy, 2) == 1
    chip_ok = flag((iy > 0) & (iy < k.gy - 1))

    def frames(core, core_at, chip, chip_at):
        row = lambda ref, at, r: ref[at + r:at + r + 4, :]
        low = jnp.where(odd, row(core, core_at, 0), row(chip, chip_at, 0) * chip_ok)
        high = jnp.where(odd, row(chip, chip_at, 4) * chip_ok, row(core, core_at, 4))
        return low, high

    for i in range(bx):
        c = mix_halves(m, i, 1)[0][4:4 + by] + own_ref[i]
        if i >= bx - 4:
            row = k.to7 + by * (bx - 1 - i)
            c = c + got4_ref[row:row + by, :]
        at = from_end(ix, i, bx)
        out_ref[at] = c
        low, high = frames(got_ref, 4 * c2 + 8 * i, got3_ref, c2 + 8 * i)
        if i >= bx - 3:
            row = 8 * (bx - 1 - i)
            low2, high2 = frames(got_ref, 4 * c2 + 8 * k.yf_n + row, got7_ref, c2 + row)
            low, high = low + low2, high + high2
        out_ref[at, :4, :] += low
        out_ref[at, by - 4:, :] += high


def mirrored(k, pressure, wind):
    bx, by, bz = k.bx, k.by, k.bz
    n1, n2 = k.nx1, k.nx1 // 2
    fine = lambda n: (n + 2, 2, k.rows, bz)
    level1 = [(n1 + 2, k.rows1, bz)] * 3
    level2 = [(n2, k.ny1, bz), (n2, k.ny1 // 2, bz)] + [(n2 + 2, k.ny1 // 2 + 2, bz)] * 2
    gathered = lax.all_gather(pressure, PLANE)
    c1, window, right, left = call(
        functools.partial(plane_kernel, k),
        [(n1, k.ny1, bz), (k.fine_n, k.rows, bz), (k.slab_rows, bz), (k.slab_rows, bz)],
        [(k.nx + 2, -(-(k.ny + 2 * FR) // 8) * 8, bz), (k.nx + 2, k.ny + 2, bz), (k.nx, k.ny, bz), (n1, k.ny, bz)],
        (gathered, wind), 1 << 22)
    low = lax.ppermute(right, "gz", chain(k.gz, 1))
    high = lax.ppermute(left, "gz", chain(k.gz, -1))
    to3, to4, to7, own = call(
        functools.partial(solve_kernel, k),
        [(k.to3, bz), (k.to4, bz), (k.to7, bz), (bx, by, bz)],
        level1 + level2 + [fine(bx + 5)] * 3 + [(3, bx + 3, 2, k.core, bz), (3,) + fine(bx + 1), (2, k.c2_n, 16, bz)],
        (c1, window, wind, low, high), 1 << 24)
    crossed = lambda v, d: lax.ppermute(v, PLANE, [(i, i ^ d) for i in range(k.gx * k.gy)])
    got3, got4, got7 = crossed(to3, 3), crossed(to4, 4), crossed(to7, 7)
    (mine,) = call(functools.partial(share_kernel, k), [(k.to1, bz)], [], (to3, got3, got4, got7), 1 << 12)
    (result,) = call(
        functools.partial(close_kernel, k), [(bx, by, bz)],
        [(8, k.c2, bz)] + level1 + level2 + [fine(bx + 2)] * 2,
        (mine, crossed(mine, 1), got3, got4, got7, own), 1 << 23)
    return result


def solution(mesh):
    gx, gy, gz = (mesh.shape[a] for a in ("gx", "gy", "gz"))

    def run(pressure, wind):
        form, sizes = (mirrored, Mirror) if (gx, gy) == (2, 4) else (general, Sizes)
        return form(sizes(gx, gy, gz, *pressure.shape), pressure, wind)

    in_specs = (P("gx", "gy", "gz"), P(None, "gx", "gy", "gz"))
    return jax.shard_map(run, mesh=mesh, in_specs=in_specs, out_specs=P("gx", "gy", "gz"), check_vma=False)
```

```python
import functools

import jax
import jax.numpy as jnp
from jax import lax
from jax.experimental import pallas as pl
from jax.experimental.pallas import tpu as pltpu
from jax.sharding import PartitionSpec as P

OMEGA = 0.8
W = OMEGA / 6.0
C0, C1, C2 = W, 4.0 * W, 16.0 * W
SIDE = 8
PLANE = ("gx", "gy")


def up(v, axis):
    return pltpu.roll(v, v.shape[axis] - 1, axis)


def down(v, axis):
    return pltpu.roll(v, 1, axis)


def mix(s, i):
    c = s[i]
    near = (s[i - 1] + s[i + 1]) + (up(c, 0) + down(c, 0)) + (up(c, 1) + down(c, 1))
    return (1.0 - OMEGA) * c + W * near


def each(n, step):
    lax.fori_loop(0, n, lambda i, _: step(i), None, unroll=True)


def iota(shape, axis):
    return lax.broadcasted_iota(jnp.int32, shape, axis)


def pair_matrix(rows, columns, value):
    hit = (iota((rows, columns), 0) >> 1) == iota((rows, columns), 1)
    return jnp.where(hit, value, 0.0).astype(jnp.float32)


def spread_matrix(rows, columns):
    hit = (iota((rows, columns), 1) >> 1) == iota((rows, columns), 0)
    return jnp.where(hit, 1.0, 0.0).astype(jnp.float32)


def dot(a, b):
    return jnp.dot(a, b, precision=lax.Precision.HIGHEST, preferred_element_type=jnp.float32)


def window_mask(shape, y_first, y_count, z_first, z_count):
    y = iota(shape, 0) + y_first
    z = iota(shape, 1) + z_first
    good = (y >= 0) & (y < y_count) & (z >= 0) & (z < z_count)
    return jnp.where(good, 1.0, 0.0).astype(jnp.float32)


class Sizes:
    def __init__(self, gx, gy, gz, bx, by, bz):
        self.gx, self.gy, self.gz = gx, gy, gz
        self.bx, self.by, self.bz = bx, by, bz
        self.rows, self.lanes = by + 2 * SIDE, 2 * bz
        self.one = gx == 2
        self.c1_n = bx // 2 + (1 if self.one else 2)
        self.c2_n = bx // 2 + (2 if self.one else 4)
        self.yf_n = bx + (3 if self.one else 6)
        self.nx1, self.ny1 = gx * bx // 2, gy * by // 2
        self.rows1 = self.ny1 + SIDE
        self.rows1p = -(-self.rows1 // 16) * 16
        self.l1 = bz
        self.c1_rows = by // 2 + 4
        self.c2_rows = by // 2 + 8
        self.edge = 5
        self.edge_sets = 1 if self.one else 2
        self.pack1 = self.c1_n * self.c1_rows + self.edge_sets * self.edge * 2 * by
        self.pack2 = self.c2_n * self.c2_rows + self.yf_n * 8

    def c1_first(self, i):
        return -i if self.one else -1

    def c2_first(self, i):
        return -2 * i if self.one else -2

    def yf_first(self, i):
        return -3 * i if self.one else -3


def slab_kernel(k, p_ref, w_ref, right_ref, left_ref):
    bx, bz = k.bx, k.bz
    half, part = bz // 2, bz // 4
    lane = iota((k.by, bz), 1)
    for x in range(bx):
        p = pltpu.roll(p_ref[x], half, 1)
        a, b = w_ref[0, x], w_ref[1, x]
        right_ref[x] = jnp.where(lane < half, p, jnp.where(lane < half + part, pltpu.roll(a, bz - part, 1), b))
        left_ref[x] = jnp.where(lane >= half, p, jnp.where(lane < part, a, pltpu.roll(b, part, 1)))
    for q in range(-(-bx // 4)):
        r_all, l_all = jnp.zeros((k.by, bz), jnp.float32), jnp.zeros((k.by, bz), jnp.float32)
        for r in range(min(4, bx - 4 * q)):
            c = w_ref[2, 4 * q + r]
            here = (lane >= part * r) & (lane < part * (r + 1))
            r_all = jnp.where(here, pltpu.roll(c, (part * r + part) % bz, 1), r_all)
            l_all = jnp.where(here, pltpu.roll(c, part * r, 1) if r else c, l_all)
        right_ref[bx + q] = r_all
        left_ref[bx + q] = l_all


def lane_roll(v, shift):
    shift = shift % v.shape[1]
    return pltpu.roll(v, shift, 1) if shift else v


def pressure_window(k, p, low, high):
    half = k.bz // 2
    lane = iota(p.shape, 1)
    p = pltpu.roll(p, half, 1)
    return jnp.concatenate([jnp.where(lane < half, low, p), jnp.where(lane < half, p, high)], axis=1)


def wind_window(k, w, low, low_at, high, high_at):
    half, part = k.bz // 2, k.bz // 4
    lane = iota(w.shape, 1)
    w = pltpu.roll(w, half, 1)
    first = jnp.where(lane >= half, w, jnp.where(lane >= part, lane_roll(low, part - low_at), 0.0))
    second = jnp.where(lane < half, w, jnp.where(lane < half + part, lane_roll(high, half - high_at), 0.0))
    return jnp.concatenate([first, second], axis=1)


def place():
    return lax.axis_index("gx"), lax.axis_index("gy"), lax.axis_index("gz")


def fine_mask(k, iy, iz):
    return window_mask((k.rows, k.lanes), iy * k.by - SIDE, k.gy * k.by, iz * k.bz - k.bz // 2, k.gz * k.bz)


def x_inside(k, ix, plane):
    place_x = ix * k.bx + plane
    return jnp.where((place_x >= 0) & (place_x < k.gx * k.bx), 1.0, 0.0).astype(jnp.float32)


def restrict_planes(src, first, n, half_ref, out, value):
    rows, lanes = src.shape[1], src.shape[2]
    a = pair_matrix(lanes, half_ref.shape[2], value)

    def step(j):
        s = src[first + 2 * j] + src[first + 2 * j + 1]
        half_ref[j] = dot(s + up(s, 0), a)

    for j in range(n):
        step(j)
    for j in range(n):
        out[j] = half_ref[j, pl.ds(0, rows // 2, stride=2), :]


def zero(ref):
    ref[...] = jnp.zeros(ref.shape, ref.dtype)


def first_kernel(k, p_ref, low_ref, high_ref, win_ref, send_a, send_b, pack_ref, b, m, half_ref, c1):
    ix, iy, iz = place()
    bx, by = k.bx, k.by
    pad = 3
    zero(b)
    zero(m)
    for x in range(bx):
        w = pressure_window(k, p_ref[x], low_ref[x], high_ref[x])
        win_ref[x] = w
        b[x + pad, SIDE:SIDE + by, :] = w
    tail = lax.rem(iy, 2) == 0
    for x in range(bx):
        head_rows, tail_rows = win_ref[x, :8, :], win_ref[x, by - 8:, :]
        send_a[x] = jnp.where(tail, tail_rows, head_rows)
        send_b[x] = jnp.where(tail, head_rows, tail_rows)
    mask = fine_mask(k, iy, iz)

    def step1(i):
        m[i + pad - 1] = mix(b, i + pad - 1) * (mask * x_inside(k, ix, i - 1))

    each(bx + 2, step1)

    def step2(i):
        b[i + pad - 2] = mix(m, i + pad - 2)

    each(bx + 4, step2)
    restrict_planes(b, pad - 2, bx // 2 + 2, half_ref, c1, 0.125)
    start = (k.c1_first(ix) + 1) if k.one else 0
    for j in range(k.c1_n):
        pack_ref[j * k.c1_rows:(j + 1) * k.c1_rows, :] = c1[start + j, 2:2 + k.c1_rows, :]
    at = k.c1_n * k.c1_rows
    starts = [(1 - ix) * (bx - k.edge)] if k.one else [0, bx - k.edge]
    for first in starts:
        for j in range(k.edge):
            for t in range(2):
                pack_ref[at:at + by, :] = win_ref[first + j, :, t * k.bz:(t + 1) * k.bz]
                at += by


def coarse(k, iz, b1, m1, e1, half_ref, b2, u2, v2):
    n1, n2 = k.nx1, k.nx1 // 2
    rows1, rows2, l1 = k.rows1, k.rows1p // 2, k.l1
    y0 = -(SIDE // 2)
    mask1 = window_mask((rows1, l1), y0, k.ny1, iz * (k.bz // 2) - k.bz // 4, k.gz * (k.bz // 2))
    lane2 = iota((rows2, l1), 1)
    mask2 = window_mask((rows2, l1), y0 // 2, k.ny1 // 2, iz * (k.bz // 4) - k.bz // 8, k.gz * (k.bz // 4))
    mask2 = jnp.where(lane2 < l1 // 2, mask2, 0.0)
    zero(m1)
    zero(e1)
    zero(u2)
    zero(v2)
    for i in range(n1):
        b1[i + 2] = b1[i + 2] * mask1

    def pre(i):
        c = mix(b1, i + 2) * mask1
        m1[i + 2] = c
        e1[i + 2] = C1 * (b1[i + 2] + c)

    each(n1, pre)
    a = pair_matrix(l1, l1, 0.125)
    for j in range(n2):
        s = mix(m1, 2 * j + 2) + mix(m1, 2 * j + 3)
        half_ref[j, :rows1, :] = dot(s + up(s, 0), a)
        if k.rows1p > rows1:
            half_ref[j, rows1:, :] = jnp.zeros((k.rows1p - rows1, l1), jnp.float32)
    for j in range(n2):
        s = half_ref[j, pl.ds(0, rows2, stride=2), :] * (mask2 * C2)
        b2[j] = s
        u2[j + 1] = s
    src, dst = u2, v2
    for _ in range(3):
        for j in range(n2):
            dst[j + 1] = (mix(src, j + 1) + b2[j]) * mask2
        src, dst = dst, src
    spread = spread_matrix(l1, l1)
    for j in range(n2):
        e = dot(src[j + 1], spread)
        half_ref[j, pl.ds(0, rows2, stride=2), :] = e
        half_ref[j, pl.ds(1, rows2, stride=2), :] = e
    for j in range(n2):
        e = half_ref[j, :rows1, :]
        e1[2 * j + 2] += e
        e1[2 * j + 3] += e
    for src, dst in ((e1, m1), (m1, e1)):

        def post(i):
            dst[i + 2] = (mix(src, i + 2) + C1 * b1[i + 2]) * mask1

        each(n1, post)


def prolonged(k, e1, ix, iy, first, n, half_ref, put):
    by = k.by
    for j in range(n):
        e = e1[ix * (k.bx // 2) + (first + j + 2), pl.ds(pl.multiple_of(iy * (by // 2), 8), k.rows // 2), :]
        half_ref[j, pl.ds(0, k.rows // 2, stride=2), :] = e
        half_ref[j, pl.ds(1, k.rows // 2, stride=2), :] = e
    spread = spread_matrix(k.l1, k.lanes)
    for j in range(n):
        put(j, dot(half_ref[j], spread))


def overlap_add(k, g_ref, b1, n, rows, y_skip, first_of):
    zero(b1)
    for i in range(k.gx):
        for j in range(k.gy):
            at_y = j * (k.by // 2) + y_skip
            for q in range(n):
                x = i * (k.bx // 2) + first_of(i) + q
                if 0 <= x < k.nx1:
                    part = g_ref[i * k.gy + j, q * rows:(q + 1) * rows, :]
                    b1[x + 2, at_y:at_y + rows, :] += part


def own_lanes(k, v):
    half = k.bz // 2
    first, second = v[:, :k.bz], v[:, k.bz:]
    lane = iota(first.shape, 1)
    return jnp.where(lane < half, pltpu.roll(first, half, 1), pltpu.roll(second, half, 1))


def assemble_edges(k, refs, b1, b, pad):
    g_ref, win_ref, got_a, got_b, w_ref, low_ref, high_ref = refs
    ix, iy, iz = place()
    bx, by = k.bx, k.by
    overlap_add(k, g_ref, b1, k.c1_n, k.c1_rows, 2, k.c1_first)
    even = lax.rem(iy, 2) == 0
    for x in range(bx):
        b[x + pad, :SIDE, :] = jnp.where(even, got_b[x], got_a[x])
        b[x + pad, SIDE:SIDE + by, :] = win_ref[x]
        b[x + pad, SIDE + by:, :] = jnp.where(even, got_a[x], got_b[x])
    base = k.c1_n * k.c1_rows
    span = k.edge * 2 * by
    y_low, y_high = jnp.maximum(iy - 1, 0), jnp.minimum(iy + 1, k.gy - 1)
    for side in range(2):
        if k.one:
            who, shift = 1 - ix, 0
        else:
            who = jnp.maximum(ix - 1, 0) if side == 0 else jnp.minimum(ix + 1, k.gx - 1)
            shift = span if side == 0 else 0
        for j in range(k.edge):
            at = pad - k.edge + j if side == 0 else pad + bx + j
            for t in range(2):
                row = base + shift + (2 * j + t) * by
                lanes = slice(t * k.bz, (t + 1) * k.bz)
                b[at, :SIDE, lanes] = g_ref[who * k.gy + y_low, row + by - 8:row + by, :]
                b[at, SIDE:SIDE + by, lanes] = g_ref[who * k.gy + iy, row:row + by, :]
                b[at, SIDE + by:, lanes] = g_ref[who * k.gy + y_high, row:row + 8, :]
    half, part = k.bz // 2, k.bz // 4

    def winds(x):
        low, high = low_ref[x], high_ref[x]
        q, r = x // 4, x % 4
        return (wind_window(k, w_ref[0, x], low, half, high, 0),
                wind_window(k, w_ref[1, x], low, half + part, high, part),
                wind_window(k, w_ref[2, x], low_ref[bx + q], part * r, high_ref[bx + q], part * r))

    return winds


def middle_kernel(k, assemble, ins, pack_ref, xa_ref, xb_ref, own_ref,
                  b1, m1, e1, half1, b2, u2, v2, b, m, v, vel, flux, half_ref, c2):
    ix, iy, iz = place()
    bx, by = k.bx, k.by
    pad = 5
    winds = assemble(k, ins, b1, b, pad)
    coarse(k, iz, b1, m1, e1, half1, b2, u2, v2)
    mask = fine_mask(k, iy, iz)

    def clean(i):
        b[i] = b[i] * (mask * x_inside(k, ix, i - pad))

    each(bx + 2 * pad, clean)

    def put(j, e):
        for t in range(2):
            v[pad - 4 + 2 * j + t] = e

    prolonged(k, e1, ix, iy, -2, bx // 2 + 4, half_ref, put)

    def pre(i):
        at = i + pad - 4
        here = mask * x_inside(k, ix, i - 4)
        v[at] = (v[at] + C0 * (b[at] + mix(b, at))) * here

    each(bx + 8, pre)

    def post1(i):
        at = i + pad - 3
        m[at] = (mix(v, at) + C0 * b[at]) * (mask * x_inside(k, ix, i - 3))

    each(bx + 6, post1)

    def post2(i):
        at = i + pad - 2
        v[at] = (mix(m, at) + C0 * b[at]) * (mask * x_inside(k, ix, i - 2))

    each(bx + 4, post2)

    def speed(i):
        at = i + pad - 1
        here = 0.5 * (mask * x_inside(k, ix, i - 1))
        c = v[at]
        vel[0, i] = (v[at + 1] - v[at - 1]) * here
        vel[1, i] = (up(c, 0) - down(c, 0)) * here
        vel[2, i] = (up(c, 1) - down(c, 1)) * here

    each(bx + 2, speed)
    own_mask = mask[SIDE:SIDE + by, :]
    zero(flux)
    for x in range(bx):
        w0, w1, w2 = (0.5 * w for w in winds(x))
        for d in range(3):
            c = vel[d, x + 1, SIDE:SIDE + by, :]
            xp, xm = vel[d, x + 2, SIDE:SIDE + by, :], vel[d, x, SIDE:SIDE + by, :]
            yp, ym = vel[d, x + 1, SIDE + 1:SIDE + by + 1, :], vel[d, x + 1, SIDE - 1:SIDE + by - 1, :]
            zp, zm = up(c, 1), down(c, 1)
            near = (xp + xm) + (yp + ym) + (zp + zm)
            total = 7.0 * c - near + w0 * (xp - xm) + w1 * (yp - ym) + w2 * (zp - zm)
            flux[d, x + 2, SIDE:SIDE + by, :] = total * own_mask
    zero(b)
    zero(m)

    def spread_flux(i):
        at = i + pad - 1
        f1, f2 = flux[1, i + 1], flux[2, i + 1]
        total = (flux[0, i + 2] - flux[0, i]) + (up(f1, 0) - down(f1, 0)) + (up(f2, 1) - down(f2, 1))
        b[at] = total * (-0.5 * (mask * x_inside(k, ix, i - 1)))

    each(bx + 2, spread_flux)
    zero(v)

    def power1_pure(i):
        at = i + pad - 2
        m[at] = mix(b, at) * (mask * x_inside(k, ix, i - 2))

    each(bx + 4, power1_pure)

    def power2(i):
        at = i + pad - 3
        v[at] = mix(m, at) * (mask * x_inside(k, ix, i - 3))

    each(bx + 6, power2)

    def power3(i):
        at = i + pad - 4
        b[at] = C0 * ((b[at] + m[at]) + (v[at] + mix(v, at))) * (mask * x_inside(k, ix, i - 4))

    each(bx + 8, power3)
    restrict_planes(v, pad - 4, bx // 2 + 4, half_ref, c2, 0.125)
    start = (k.c2_first(ix) + 2) if k.one else 0
    for j in range(k.c2_n):
        pack_ref[j * k.c2_rows:(j + 1) * k.c2_rows, :] = c2[start + j]
    row8 = iota((8, k.bz), 0)
    at = k.c2_n * k.c2_rows
    start = (k.yf_first(ix) if k.one else -3) + pad
    for j in range(k.yf_n):
        c = own_lanes(k, jnp.where(iota((8, k.lanes), 0) < 4, b[start + j, SIDE + by:, :], b[start + j, :SIDE, :]))
        pack_ref[at:at + 8, :] = c
        at += 8
    upper = lax.rem(ix, 2) == 0
    first_a = pad + jnp.where(upper, bx, -4)
    first_b = pad + jnp.where(upper, -4, bx)
    for j in range(4):
        xa_ref[j] = own_lanes(k, b[first_a + j, SIDE:SIDE + by, :])
        if xb_ref is not None:
            xb_ref[j] = own_lanes(k, b[first_b + j, SIDE:SIDE + by, :])
    for x in range(bx):
        own_ref[x] = own_lanes(k, b[x + pad, SIDE:SIDE + by, :])


def last_kernel(k, g_ref, own_ref, xa_ref, xb_ref, out_ref, b1, m1, e1, half1, b2, u2, v2, v, m, half_ref):
    ix, iy, iz = place()
    bx, by = k.bx, k.by
    overlap_add(k, g_ref, b1, k.c2_n, k.c2_rows, 0, k.c2_first)
    coarse(k, iz, b1, m1, e1, half1, b2, u2, v2)
    pad = 2
    mask = fine_mask(k, iy, iz)

    def put(j, e):
        for t in range(2):
            plane = -2 + 2 * j + t
            v[pad + plane] = e * (mask * x_inside(k, ix, plane))

    prolonged(k, e1, ix, iy, -1, bx // 2 + 2, half_ref, put)

    def post1(i):
        at = i + pad - 1
        m[at] = mix(v, at) * (mask * x_inside(k, ix, i - 1))

    each(bx + 2, post1)
    base = k.c2_n * k.c2_rows
    low_ok = jnp.where(iy > 0, 1.0, 0.0).astype(jnp.float32)
    high_ok = jnp.where(iy < k.gy - 1, 1.0, 0.0).astype(jnp.float32)
    y_low, y_high = jnp.maximum(iy - 1, 0), jnp.minimum(iy + 1, k.gy - 1)
    row8 = iota((8, k.bz), 0)
    low_keep = jnp.where(row8 < 4, low_ok, 0.0)
    high_keep = jnp.where(row8 >= 4, high_ok, 0.0)
    for x in range(bx):
        out_ref[x] = own_lanes(k, mix(m, x + pad)[SIDE:SIDE + by, :]) + own_ref[x]

    def frame(who, first, x_from, x_to, ok):
        for x in range(x_from, x_to):
            row = base + (x - first) * 8
            if not isinstance(row, int):
                row = pl.multiple_of(row, 8)
            lo = g_ref[who * k.gy + y_low, pl.ds(row, 8), :] * ok
            hi = g_ref[who * k.gy + y_high, pl.ds(row, 8), :] * ok
            out_ref[x, :8, :] += lo * low_keep
            out_ref[x, by - 8:, :] += hi * high_keep

    one = jnp.float32(1.0)
    frame(ix, k.yf_first(ix), 0, bx, one)
    upper = lax.rem(ix, 2) == 0
    if k.one:
        for j in range(3):
            x = jnp.where(ix == 0, bx - 3 + j, j)
            row = pl.multiple_of(base + jnp.where(ix == 0, j, bx + j) * 8, 8)
            lo = g_ref[(1 - ix) * k.gy + y_low, pl.ds(row, 8), :]
            hi = g_ref[(1 - ix) * k.gy + y_high, pl.ds(row, 8), :]
            out_ref[x, :8, :] += lo * low_keep
            out_ref[x, by - 8:, :] += hi * high_keep
    else:
        frame(jnp.maximum(ix - 1, 0), -3 - bx, 0, 3, jnp.where(ix > 0, 1.0, 0.0).astype(jnp.float32))
        frame(jnp.minimum(ix + 1, k.gx - 1), bx - 3, bx - 3, bx, jnp.where(ix < k.gx - 1, 1.0, 0.0).astype(jnp.float32))
    for j in range(4):
        out_ref[jnp.where(upper, bx - 4, 0) + j] += xa_ref[j]
        if xb_ref is not None:
            out_ref[jnp.where(upper, 0, bx - 4) + j] += xb_ref[j]


def call(kernel, outs, scratch, args, flops):
    f32 = lambda s: jax.ShapeDtypeStruct(s, jnp.float32)
    return pl.pallas_call(
        kernel,
        out_shape=[f32(s) for s in outs],
        scratch_shapes=[pltpu.VMEM(s, jnp.float32) for s in scratch],
        compiler_params=pltpu.CompilerParams(vmem_limit_bytes=40 * 1024 * 1024),
        cost_estimate=pl.CostEstimate(flops=flops, bytes_accessed=1 << 20, transcendentals=0),
    )(*args)


def pairs(n):
    first = [(i, i ^ 1) for i in range(n) if (i ^ 1) < n]
    second = [(i + s, i + 1 - s) for i in range(1, n - 1, 2) for s in (0, 1)]
    return first, second


def chain(n, step):
    return [(i, i + step) for i in range(n) if 0 <= i + step < n]


def coarse_scratch(k):
    n1, n2, rows2 = k.nx1, k.nx1 // 2, k.rows1p // 2
    big = (n1 + 4, k.rows1, k.l1)
    return [big, big, big, (n2, k.rows1p, k.l1), (n2, rows2, k.l1), (n2 + 2, rows2, k.l1), (n2 + 2, rows2, k.l1)]


def edge_form(k, pressure, wind):
    bx, by, bz = k.bx, k.by, k.bz
    slab = (bx + -(-bx // 4), by, bz)
    right, left = call(functools.partial(slab_kernel, k), [slab, slab], [], (pressure, wind), 1 << 20)
    low = lax.ppermute(right, "gz", chain(k.gz, 1))
    high = lax.ppermute(left, "gz", chain(k.gz, -1))
    fine = lambda n: (n, k.rows, k.lanes)
    window, send_a, send_b, pack = call(
        functools.partial(first_kernel, k),
        [(bx, by, k.lanes), (bx, 8, k.lanes), (bx, 8, k.lanes), (k.pack1, bz)],
        [fine(bx + 6), fine(bx + 6), (bx // 2 + 2, k.rows, k.l1), (bx // 2 + 2, k.rows // 2, k.l1)],
        (pressure, low, high), 1 << 22)
    ya, yb = pairs(k.gy)
    got_a = lax.ppermute(send_a, "gy", ya)
    got_b = lax.ppermute(send_b, "gy", yb)
    gathered = lax.all_gather(pack, PLANE)
    return assemble_edges, (gathered, window, got_a, got_b, wind, low, high)


def general(k, pressure, wind):
    bx, by, bz = k.bx, k.by, k.bz
    fine = lambda n: (n, k.rows, k.lanes)
    assemble, args = edge_form(k, pressure, wind)
    xa, xb = pairs(k.gx)
    x_outs = [(4, by, bz)] * (2 if xb else 1)

    def middle(*refs):
        ins, rest = refs[:len(args)], refs[len(args):]
        pack_ref, rest = rest[0], rest[1:]
        xa_ref, rest = rest[0], rest[1:]
        xb_ref = None
        if xb:
            xb_ref, rest = rest[0], rest[1:]
        middle_kernel(k, assemble, ins, pack_ref, xa_ref, xb_ref, *rest)

    big = fine(bx + 10)
    outs = call(
        middle, [(k.pack2, bz)] + x_outs + [(bx, by, bz)],
        coarse_scratch(k) + [big, big, big, (3,) + fine(bx + 2), (3,) + fine(bx + 4),
                             (bx // 2 + 4, k.rows, k.l1), (bx // 2 + 4, k.rows // 2, k.l1)],
        args, 1 << 24)
    pack, frames, own = outs[0], outs[1:-1], outs[-1]
    got = [lax.ppermute(f, "gx", perm) for f, perm in zip(frames, (xa, xb))]
    gathered = lax.all_gather(pack, PLANE)

    def last(*refs):
        g_ref, own_ref, xa_ref, rest = refs[0], refs[1], refs[2], refs[3:]
        xb_ref = None
        if xb:
            xb_ref, rest = rest[0], rest[1:]
        last_kernel(k, g_ref, own_ref, xa_ref, xb_ref, *rest)

    (result,) = call(
        last, [(bx, by, bz)],
        coarse_scratch(k) + [fine(bx + 4), fine(bx + 4), (bx // 2 + 2, k.rows, k.l1)],
        (gathered, own, *got), 1 << 23)
    return result

FR = 5
CR = 2


class Mirror:
    def __init__(self, gx, gy, gz, bx, by, bz):
        self.gx, self.gy, self.gz, self.bx, self.by, self.bz = gx, gy, gz, bx, by, bz
        self.rows = by + 2 * FR
        self.core = by + 8
        self.nx, self.ny = gx * bx, gy * by
        self.nx1, self.ny1 = self.nx // 2, self.ny // 2
        self.rows1 = self.ny1 + 8
        self.part = bz // 4
        groups = lambda n: -(-n // 4)
        self.fine_n = bx + 5
        self.at_fine = groups(self.nx1) * self.ny1
        self.at_wind = self.at_fine + groups(self.fine_n) * self.rows
        self.slab_rows = self.at_wind + groups(3 * bx) * by
        self.c2_n, self.c2_rows = bx // 2 + 2, by // 2 + 4
        self.c2 = self.c2_n * self.c2_rows
        self.yf_n = bx + 3
        self.to3 = self.c2 + 8 * self.yf_n
        self.to4 = self.c2 + 8 * 3 + 4 * by
        self.to7 = self.c2 + 8 * 3
        self.to1 = 4 * self.c2 + 8 * self.yf_n + 8 * 3


def exact_dot(x, a):
    high = x.astype(jnp.bfloat16)
    low = (x - high.astype(jnp.float32)).astype(jnp.bfloat16)
    return (jnp.dot(high, a, preferred_element_type=jnp.float32)
            + jnp.dot(low, a, preferred_element_type=jnp.float32))


def matrix(hit, value):
    return jnp.where(hit, value, 0.0).astype(jnp.float32).astype(jnp.bfloat16)


def flag(good):
    return jnp.where(good, 1.0, 0.0).astype(jnp.float32)


def beside(c0, c1):
    n = c0.shape[1]
    lane = iota(c0.shape, 1)
    last, first = lane == n - 1, lane == 0
    u0, u1, d0, d1 = up(c0, 1), up(c1, 1), down(c0, 1), down(c1, 1)
    return ((jnp.where(last, u1, u0), jnp.where(last, u0, u1)),
            (jnp.where(first, d1, d0), jnp.where(first, d0, d1)))


def mix_halves(s, i, halves=2):
    n = s.shape[2] - 2
    c = [s[i + 1, h, 1:1 + n, :] for h in range(2)]
    plus, minus = beside(*c)
    out = []
    for h in range(halves):
        near = (s[i, h, 1:1 + n, :] + s[i + 2, h, 1:1 + n, :]) + (s[i + 1, h, 2:2 + n, :] + s[i + 1, h, :n, :])
        out.append((1.0 - OMEGA) * c[h] + W * (near + (plus[h] + minus[h])))
    return out


def halves_mask(k, iy, iz):
    y = iota((k.core, k.bz), 0) + (iy * k.by - 4)
    lane = iota((k.core, k.bz), 1)
    y_good = (y >= 0) & (y < k.ny)
    edge = flag(y_good)
    side = jnp.where(lane < k.bz // 2, jnp.where(iz < k.gz - 1, 1.0, 0.0), jnp.where(iz > 0, 1.0, 0.0))
    return edge, edge * side.astype(jnp.float32)


def zero_rim(s):
    s[0] = jnp.zeros(s.shape[1:], jnp.float32)
    n = s.shape[2]
    for i in range(1, s.shape[0]):
        for h in range(2):
            s[i, h, 0:1, :] = jnp.zeros((1, s.shape[3]), jnp.float32)
            s[i, h, n - 1:n, :] = jnp.zeros((1, s.shape[3]), jnp.float32)


def mix1(k, s, i, n, at):
    c = s[i + 1, at:at + n, :]
    near = (s[i, at:at + n, :] + s[i + 2, at:at + n, :]) + (s[i + 1, at + 1:at + n + 1, :] + s[i + 1, at - 1:at + n - 1, :])
    return (1.0 - OMEGA) * c + W * (near + (up(c, 1) + down(c, 1)))


def coarse_plane(k, iz, b1, m1, e1, half_ref, b2, u2, v2):
    n1, n2, ny, l1 = k.nx1, k.nx1 // 2, k.ny1, k.bz
    ny2 = ny // 2
    lane = iota((ny, l1), 1)
    low_ok, high_ok = flag(iz > 0), flag(iz < k.gz - 1)
    mask1 = jnp.where(lane < l1 // 2, 1.0, jnp.where(lane < 3 * l1 // 4, high_ok, low_ok))
    lane2 = iota((ny2, l1), 1)
    own2 = l1 // 8
    mask2 = jnp.where(lane2 < own2, low_ok, jnp.where(lane2 < 3 * own2, 1.0, jnp.where(lane2 < 4 * own2, high_ok, 0.0)))
    for s in (m1, e1):
        for i in (0, n1 + 1):
            s[i] = jnp.zeros(s.shape[1:], jnp.float32)
    for s in (b1, m1, e1):
        for i in range(n1):
            s[i + 1, :CR, :] = jnp.zeros((CR, l1), jnp.float32)
            s[i + 1, CR + ny:, :] = jnp.zeros((k.rows1 - CR - ny, l1), jnp.float32)
    zero(u2)
    zero(v2)
    for i in range(n1):
        b1[i + 1, CR:CR + ny, :] = b1[i + 1, CR:CR + ny, :] * mask1
    for i in range(n1):
        c = mix1(k, b1, i, ny, CR) * mask1
        m1[i + 1, CR:CR + ny, :] = c
        e1[i + 1, CR:CR + ny, :] = C1 * (b1[i + 1, CR:CR + ny, :] + c)
    row, column = iota((l1, l1), 0), iota((l1, l1), 1)
    linear = lambda x: (jnp.where(x < 3 * l1 // 4, x, x - l1) >> 1) + own2
    for j in range(n2):
        half_ref[j] = mix1(k, m1, 2 * j, ny, CR) + mix1(k, m1, 2 * j + 1, ny, CR)
    pairs_sum = [half_ref[j, pl.ds(0, ny2, stride=2), :] + half_ref[j, pl.ds(1, ny2, stride=2), :] for j in range(n2)]
    r2 = exact_dot(jnp.concatenate(pairs_sum, axis=0), matrix(linear(row) == column, 0.125))
    for j in range(n2):
        c = r2[j * ny2:(j + 1) * ny2] * (mask2 * C2)
        b2[j] = c
        u2[j + 1, 1:1 + ny2, :] = c
    src, dst = u2, v2
    for _ in range(3):
        for j in range(n2):
            dst[j + 1, 1:1 + ny2, :] = (mix1(k, src, j, ny2, 1) + b2[j]) * mask2
        src, dst = dst, src
    stack = jnp.concatenate([src[j + 1, 1:1 + ny2, :] for j in range(n2)], axis=0)
    spread = exact_dot(stack, matrix(row == linear(column), 1.0))
    for j in range(n2):
        e = spread[j * ny2:(j + 1) * ny2]
        half_ref[j, pl.ds(0, ny2, stride=2), :] = e
        half_ref[j, pl.ds(1, ny2, stride=2), :] = e
    for j in range(n2):
        e = half_ref[j]
        for t in range(2):
            e1[2 * j + t + 1, CR:CR + ny, :] = e1[2 * j + t + 1, CR:CR + ny, :] + e
    for src, dst in ((e1, m1), (m1, e1)):
        for i in range(n1):
            dst[i + 1, CR:CR + ny, :] = (mix1(k, src, i, ny, CR) + C1 * b1[i + 1, CR:CR + ny, :]) * mask1


def from_end(ix, i, count):
    return jnp.where(ix == 0, i, count - 1 - i)


def prolong_halves(k, iy, e1, n, v):
    half, rows = k.bz // 2, k.core // 2
    first = pl.multiple_of(iy * (k.by // 2), 8)
    stack = jnp.concatenate([e1[j + 1, pl.ds(first, 16), :] for j in range(n)], axis=0)
    row, column = iota((k.bz, 2 * k.bz), 0), iota((k.bz, 2 * k.bz), 1)
    spread = exact_dot(stack, matrix(row == (column >> 1), 1.0))
    for j in range(n):
        for h in range(2):
            e = spread[16 * j:16 * j + rows, h * k.bz:(h + 1) * k.bz]
            for t in range(2):
                v[2 * j + t + 1, h, pl.ds(1, rows, stride=2), :] = e
                v[2 * j + t + 1, h, pl.ds(2, rows, stride=2), :] = e


def take_slab(k, ref, base, rows, i, to):
    at = base + (i // 4) * rows
    return lane_roll(ref[at:at + rows, :], to - k.part * (i % 4))


def plane_kernel(k, g_ref, w_ref, c1_ref, win_ref, first_ref, second_ref, p, m, q, half_ref):
    ix, iy, iz = place()
    bx, by, bz, nx, ny, part = k.bx, k.by, k.bz, k.nx, k.ny, k.part
    p[0] = jnp.zeros(p.shape[1:], jnp.float32)
    p[nx + 1] = jnp.zeros(p.shape[1:], jnp.float32)
    m[0] = jnp.zeros(m.shape[1:], jnp.float32)
    m[nx + 1] = jnp.zeros(m.shape[1:], jnp.float32)
    for x in range(nx):
        p[x + 1, :FR, :] = jnp.zeros((FR, bz), jnp.float32)
        p[x + 1, FR + ny:, :] = jnp.zeros((p.shape[1] - FR - ny, bz), jnp.float32)
        m[x + 1, 0:1, :] = jnp.zeros((1, bz), jnp.float32)
        m[x + 1, ny + 1:, :] = jnp.zeros((m.shape[1] - ny - 1, bz), jnp.float32)
        who = ix if x < bx else 1 - ix
        for j in range(k.gy):
            p[x + 1, FR + j * by:FR + (j + 1) * by, :] = g_ref[who * k.gy + j, from_end(ix, x % bx, bx)]
    lane = iota((ny, bz), 1)
    first, last = lane == 0, lane == bz - 1
    ends = jnp.where(first, flag(iz > 0), jnp.where(last, flag(iz < k.gz - 1), 0.0)) * (W * W)

    def parts(s, x, at):
        c = s[x + 1, at:at + ny, :]
        four = (s[x, at:at + ny, :] + s[x + 2, at:at + ny, :]) + (s[x + 1, at + 1:at + ny + 1, :] + s[x + 1, at - 1:at + ny - 1, :])
        along = jnp.where(last, 0.0, up(c, 1)) + jnp.where(first, 0.0, down(c, 1))
        return c, four, (1.0 - OMEGA) * c + W * (four + along)

    for x in range(nx):
        c, four, mixed = parts(p, x, FR)
        m[x + 1, 1:1 + ny, :] = mixed
        q[x] = (1.0 - OMEGA + W) * c + (mixed + W * four)
    row, column = iota((bz, bz), 0), iota((bz, bz), 1)
    own = matrix((row >> 1) == column, 0.125)
    rim = ((row == 0) & (column == bz - 1)) | ((row == bz - 1) & (column == bz // 2))
    rim = matrix(rim, 0.125)
    half_rows = ny // 2
    for j in range(k.nx1):
        s = None
        for x in (2 * j, 2 * j + 1):
            r = parts(m, x, 1)[2] + ends * p[x + 1, FR:FR + ny, :]
            s = r if s is None else s + r
        half_ref[j] = s
        t = (q[2 * j, pl.ds(0, half_rows, stride=2), :] + q[2 * j, pl.ds(1, half_rows, stride=2), :]
             + q[2 * j + 1, pl.ds(0, half_rows, stride=2), :] + q[2 * j + 1, pl.ds(1, half_rows, stride=2), :])
        s = half_ref[j, pl.ds(0, half_rows, stride=2), :] + half_ref[j, pl.ds(1, half_rows, stride=2), :]
        c1_ref[j] = exact_dot(s, own) + exact_dot(W * t, rim)

    even = lax.rem(iz, 2) == 0

    def pack(base, rows, n, load, right_lane, left_lane):
        lane = iota((rows, bz), 1)
        for group in range(-(-n // 4)):
            right, left = jnp.zeros((rows, bz), jnp.float32), jnp.zeros((rows, bz), jnp.float32)
            for r in range(min(4, n - 4 * group)):
                here = (lane >= part * r) & (lane < part * (r + 1))
                c = load(4 * group + r)
                right = jnp.where(here, lane_roll(c, part * r - right_lane), right)
                left = jnp.where(here, lane_roll(c, part * r - left_lane), left)
            at = slice(base + group * rows, base + (group + 1) * rows)
            first_ref[at, :] = jnp.where(even, right, left)
            second_ref[at, :] = jnp.where(even, left, right)

    for i in range(k.fine_n):
        win_ref[i] = p[i + 1, pl.ds(pl.multiple_of(iy * by, 8), k.rows), :]
    pack(0, k.ny1, k.nx1, lambda i: c1_ref[i], part + 1, bz - 1)
    pack(k.at_fine, k.rows, k.fine_n, lambda i: win_ref[i], 3 * part, 0)
    pack(k.at_wind, by, 3 * bx, lambda i: w_ref[i // bx, from_end(ix, i % bx, bx)], 3 * part, 0)


def solve_kernel(k, c1_ref, win_ref, w_ref, first_ref, second_ref, to3_ref, to4_ref, to7_ref, own_ref,
                 low_ref, high_ref, b1, m1, e1, half1, b2, u2, v2, b, m, v, vel, flux, half_ref):
    ix, iy, iz = place()
    bx, by, bz, part, n = k.bx, k.by, k.bz, k.part, k.core
    even = lax.rem(iz, 2) == 0
    low_ref[...] = jnp.where(even, second_ref[...], first_ref[...])
    high_ref[...] = jnp.where(even, first_ref[...], second_ref[...])
    lane = iota((k.ny1, bz), 1)
    for s in (b1,):
        for i in (0, k.nx1 + 1):
            s[i] = jnp.zeros(s.shape[1:], jnp.float32)
    for x in range(k.nx1):
        low = take_slab(k, low_ref, 0, k.ny1, x, 3 * part + 1)
        high = take_slab(k, high_ref, 0, k.ny1, x, 2 * part - 1)
        low = jnp.where((lane >= 3 * part + 1) | (lane == 0), low, 0.0)
        high = jnp.where((lane >= 2 * part - 1) & (lane < 3 * part - 1), high, 0.0)
        b1[x + 1, CR:CR + k.ny1, :] = c1_ref[x] + (low + high)
    coarse_plane(k, iz, b1, m1, e1, half1, b2, u2, v2)
    mask = halves_mask(k, iy, iz)
    for s in (b, m, v):
        zero_rim(s)

    def outer(low, high, lane):
        return jnp.where(lane >= 3 * part, low, jnp.where(lane < part, high, 0.0))

    lane = iota((k.rows, bz), 1)
    for i in range(k.fine_n):
        b[i + 1, 0] = win_ref[i]
        b[i + 1, 1] = outer(take_slab(k, low_ref, k.at_fine, k.rows, i, 3 * part),
                            take_slab(k, high_ref, k.at_fine, k.rows, i, 0), lane)
    prolong_halves(k, iy, e1, bx // 2 + 2, v)
    for i in range(bx + 4):
        mb = mix_halves(b, i)
        for h in range(2):
            v[i + 1, h, 1:1 + n, :] = (v[i + 1, h, 1:1 + n, :] + C0 * (b[i + 1, h, 1:1 + n, :] + mb[h])) * mask[h]
    for src, dst, count in ((v, m, bx + 3), (m, v, bx + 2)):
        for i in range(count):
            c = mix_halves(src, i)
            for h in range(2):
                dst[i + 1, h, 1:1 + n, :] = (c[h] + C0 * b[i + 1, h, 1:1 + n, :]) * mask[h]
    half_mask = [0.5 * c for c in mask]
    for d in range(3):
        vel[d, 0] = jnp.zeros(vel.shape[2:], jnp.float32)
    for i in range(bx + 1):
        plus, minus = beside(v[i + 1, 0, 1:1 + n, :], v[i + 1, 1, 1:1 + n, :])
        for h in range(2):
            vel[0, i + 1, h] = (v[i + 2, h, 1:1 + n, :] - v[i, h, 1:1 + n, :]) * half_mask[h]
            vel[1, i + 1, h] = (v[i + 1, h, 2:2 + n, :] - v[i + 1, h, :n, :]) * half_mask[h]
            vel[2, i + 1, h] = (plus[h] - minus[h]) * half_mask[h]
    own_at = 4
    zero(flux)
    sign = jnp.where(ix == 0, 0.5, -0.5).astype(jnp.float32)
    lane = iota((by, bz), 1)
    for x in range(bx):
        winds = []
        for d in range(3):
            low = take_slab(k, low_ref, k.at_wind, by, d * bx + x, 3 * part)
            high = take_slab(k, high_ref, k.at_wind, by, d * bx + x, 0)
            scale = sign if d == 0 else 0.5
            winds.append((scale * w_ref[d, from_end(ix, x, bx)], scale * outer(low, high, lane)))
        for d in range(3):
            at = lambda i, h, r: vel[d, i + 1, h, own_at + r:own_at + r + by, :]
            c = [at(x, h, 0) for h in range(2)]
            plus, minus = beside(*c)
            for h in range(2):
                xp, xm, yp, ym, zp, zm = at(x + 1, h, 0), at(x - 1, h, 0), at(x, h, 1), at(x, h, -1), plus[h], minus[h]
                near = (xp + xm) + (yp + ym) + (zp + zm)
                total = 7.0 * c[h] - near + winds[0][h] * (xp - xm) + winds[1][h] * (yp - ym) + winds[2][h] * (zp - zm)
                if h == 1:
                    total = total * mask[1][own_at:own_at + by]
                flux[d, x + 1, h, own_at + 1:own_at + 1 + by, :] = total
    minus_mask = [-0.5 * c for c in mask]
    for s, first in ((b, bx + 2), (m, bx + 3), (v, bx + 4)):
        for i in range(first, bx + 6):
            s[i] = jnp.zeros(s.shape[1:], jnp.float32)
    for i in range(bx + 1):
        plus, minus = beside(flux[2, i + 1, 0, 1:1 + n, :], flux[2, i + 1, 1, 1:1 + n, :])
        for h in range(2):
            total = (flux[0, i + 2, h, 1:1 + n, :] - flux[0, i, h, 1:1 + n, :]
                     + (flux[1, i + 1, h, 2:2 + n, :] - flux[1, i + 1, h, :n, :]) + (plus[h] - minus[h]))
            b[i + 1, h, 1:1 + n, :] = total * minus_mask[h]
    zero_rows = jnp.zeros((1, bz), jnp.float32)
    for i in range(bx + 1):
        for h in range(2):
            b[i + 1, h, 0:1, :] = zero_rows
            b[i + 1, h, n + 1:n + 2, :] = zero_rows
    for src, dst, count in ((b, m, bx + 2), (m, v, bx + 3)):
        for i in range(count):
            c = mix_halves(src, i)
            for h in range(2):
                dst[i + 1, h, 1:1 + n, :] = c[h] * mask[h]
    half_rows = n // 2
    for j in range(k.c2_n):
        for h in range(2):
            take = lambda i, r: v[i + 1, h, pl.ds(r, half_rows, stride=2), :]
            half_ref[h, j, :half_rows, :] = (take(2 * j, 1) + take(2 * j, 2)) + (take(2 * j + 1, 1) + take(2 * j + 1, 2))
            half_ref[h, j, half_rows:, :] = jnp.zeros((16 - half_rows, bz), jnp.float32)
    row, column = iota((bz, bz), 0), iota((bz, bz), 1)
    c2 = (exact_dot(half_ref[0].reshape(k.c2_n * 16, bz), matrix((row >> 1) == column, 0.125))
          + exact_dot(half_ref[1].reshape(k.c2_n * 16, bz), matrix((row >> 1) + bz // 2 == column, 0.125)))
    for j in range(k.c2_n):
        for ref in (to3_ref, to4_ref, to7_ref):
            ref[j * k.c2_rows:(j + 1) * k.c2_rows, :] = c2[16 * j:16 * j + k.c2_rows]
    for i in range(bx + 4):
        c = mix_halves(v, i, 1)[0]
        at = lambda s: s[i + 1, 0, 1:1 + n, :]
        c = C0 * ((at(b) + at(m)) + (at(v) + c)) * mask[0]
        if i < bx:
            own_ref[i] = c[4:4 + by]
        else:
            row = k.to7 + by * (i - bx)
            to4_ref[row:row + by, :] = c[4:4 + by]
        places = [(to3_ref, k.c2 + 8 * i)] if i < k.yf_n else []
        if bx <= i < k.yf_n:
            places += [(ref, k.c2 + 8 * (i - bx)) for ref in (to4_ref, to7_ref)]
        for ref, row in places:
            ref[row:row + 4, :] = c[4 + by:8 + by]
            ref[row + 4:row + 8, :] = c[:4]


def share_kernel(k, own_ref, got3_ref, got4_ref, got7_ref, out_ref):
    c2 = k.c2
    for n, ref in enumerate((own_ref, got3_ref, got4_ref, got7_ref)):
        out_ref[n * c2:(n + 1) * c2, :] = ref[:c2, :]
    out_ref[4 * c2:4 * c2 + 8 * k.yf_n, :] = own_ref[c2:, :]
    out_ref[4 * c2 + 8 * k.yf_n:, :] = got4_ref[c2:c2 + 24, :]


def close_kernel(k, mine_ref, got_ref, got3_ref, got4_ref, got7_ref, own_ref, out_ref,
                 parts, b1, m1, e1, half1, b2, u2, v2, v, m):
    ix, iy, iz = place()
    bx, by, bz, n, c2 = k.bx, k.by, k.bz, k.core, k.c2
    for slot, near, far in ((0, mine_ref, 0), (3, mine_ref, 1), (1, got_ref, 0), (2, got_ref, 1)):
        parts[slot] = near[far * c2:(far + 1) * c2, :]
        parts[4 + slot] = near[(2 + far) * c2:(3 + far) * c2, :]
    zero(b1)
    for side in range(2):
        for j in range(k.gy):
            at = j * (by // 2)
            slot = 4 * side + (iy ^ j)
            for q in range(k.c2_n):
                x = q if side == 0 else k.nx1 - 1 - q
                b1[x + 1, at:at + k.c2_rows, :] += parts[slot, q * k.c2_rows:(q + 1) * k.c2_rows, :]
    coarse_plane(k, iz, b1, m1, e1, half1, b2, u2, v2)
    mask = halves_mask(k, iy, iz)
    for s in (v, m):
        zero_rim(s)
    prolong_halves(k, iy, e1, bx // 2 + 1, v)
    for i in range(bx + 2):
        for h in range(2):
            v[i + 1, h, 1:1 + n, :] = v[i + 1, h, 1:1 + n, :] * mask[h]
    for i in range(bx + 1):
        c = mix_halves(v, i)
        for h in range(2):
            m[i + 1, h, 1:1 + n, :] = c[h] * mask[h]
    odd = lax.rem(iy, 2) == 1
    chip_ok = flag((iy > 0) & (iy < k.gy - 1))

    def frames(core, core_at, chip, chip_at):
        row = lambda ref, at, r: ref[at + r:at + r + 4, :]
        low = jnp.where(odd, row(core, core_at, 0), row(chip, chip_at, 0) * chip_ok)
        high = jnp.where(odd, row(chip, chip_at, 4) * chip_ok, row(core, core_at, 4))
        return low, high

    for i in range(bx):
        c = mix_halves(m, i, 1)[0][4:4 + by] + own_ref[i]
        if i >= bx - 4:
            row = k.to7 + by * (bx - 1 - i)
            c = c + got4_ref[row:row + by, :]
        at = from_end(ix, i, bx)
        out_ref[at] = c
        low, high = frames(got_ref, 4 * c2 + 8 * i, got3_ref, c2 + 8 * i)
        if i >= bx - 3:
            row = 8 * (bx - 1 - i)
            low2, high2 = frames(got_ref, 4 * c2 + 8 * k.yf_n + row, got7_ref, c2 + row)
            low, high = low + low2, high + high2
        out_ref[at, :4, :] += low
        out_ref[at, by - 4:, :] += high


def mirrored(k, pressure, wind):
    bx, by, bz = k.bx, k.by, k.bz
    n1, n2 = k.nx1, k.nx1 // 2
    fine = lambda n: (n + 2, 2, k.rows, bz)
    level1 = [(n1 + 2, k.rows1, bz)] * 3
    level2 = [(n2, k.ny1, bz), (n2, k.ny1 // 2, bz)] + [(n2 + 2, k.ny1 // 2 + 2, bz)] * 2
    gathered = lax.all_gather(pressure, PLANE)
    c1, window, first, second = call(
        functools.partial(plane_kernel, k),
        [(n1, k.ny1, bz), (k.fine_n, k.rows, bz), (k.slab_rows, bz), (k.slab_rows, bz)],
        [(k.nx + 2, -(-(k.ny + 2 * FR) // 8) * 8, bz), (k.nx + 2, k.ny + 2, bz), (k.nx, k.ny, bz), (n1, k.ny, bz)],
        (gathered, wind), 1 << 22)
    first, second = (lax.ppermute(v, "gz", p) for v, p in zip((first, second), pairs(k.gz)))
    to3, to4, to7, own = call(
        functools.partial(solve_kernel, k),
        [(k.to3, bz), (k.to4, bz), (k.to7, bz), (bx, by, bz)],
        [(k.slab_rows, bz)] * 2 + level1 + level2 + [fine(bx + 5)] * 3 + [(3, bx + 3, 2, k.core, bz), (3,) + fine(bx + 1), (2, k.c2_n, 16, bz)],
        (c1, window, wind, first, second), 1 << 24)
    crossed = lambda v, d: lax.ppermute(v, PLANE, [(i, i ^ d) for i in range(k.gx * k.gy)])
    got3, got4, got7 = crossed(to3, 3), crossed(to4, 4), crossed(to7, 7)
    (mine,) = call(functools.partial(share_kernel, k), [(k.to1, bz)], [], (to3, got3, got4, got7), 1 << 12)
    (result,) = call(
        functools.partial(close_kernel, k), [(bx, by, bz)],
        [(8, k.c2, bz)] + level1 + level2 + [fine(bx + 2)] * 2,
        (mine, crossed(mine, 1), got3, got4, got7, own), 1 << 23)
    return result


def solution(mesh):
    gx, gy, gz = (mesh.shape[a] for a in ("gx", "gy", "gz"))

    def run(pressure, wind):
        form, sizes = (mirrored, Mirror) if (gx, gy) == (2, 4) else (general, Sizes)
        return form(sizes(gx, gy, gz, *pressure.shape), pressure, wind)

    in_specs = (P("gx", "gy", "gz"), P(None, "gx", "gy", "gz"))
    return jax.shard_map(run, mesh=mesh, in_specs=in_specs, out_specs=P("gx", "gy", "gz"), check_vma=False)
```

```python
import functools

import jax
import jax.numpy as jnp
from jax import lax
from jax.experimental import pallas as pl
from jax.experimental.pallas import tpu as pltpu
from jax.sharding import PartitionSpec as P


OMEGA = 0.8
W = OMEGA / 6.0
C0, C1, C2 = W, 4.0 * W, 16.0 * W
SIDE = 8
PLANE = ("gx", "gy")


def up(v, axis):
    return pltpu.roll(v, v.shape[axis] - 1, axis)


def down(v, axis):
    return pltpu.roll(v, 1, axis)


def mix(s, i):
    c = s[i]
    near = (s[i - 1] + s[i + 1]) + (up(c, 0) + down(c, 0)) + (up(c, 1) + down(c, 1))
    return (1.0 - OMEGA) * c + W * near


def each(n, step):
    lax.fori_loop(0, n, lambda i, _: step(i), None, unroll=True)


def iota(shape, axis):
    return lax.broadcasted_iota(jnp.int32, shape, axis)


def pair_matrix(rows, columns, value):
    hit = (iota((rows, columns), 0) >> 1) == iota((rows, columns), 1)
    return jnp.where(hit, value, 0.0).astype(jnp.float32)


def spread_matrix(rows, columns):
    hit = (iota((rows, columns), 1) >> 1) == iota((rows, columns), 0)
    return jnp.where(hit, 1.0, 0.0).astype(jnp.float32)


def dot(a, b):
    return jnp.dot(a, b, precision=lax.Precision.HIGHEST, preferred_element_type=jnp.float32)


def window_mask(shape, y_first, y_count, z_first, z_count):
    y = iota(shape, 0) + y_first
    z = iota(shape, 1) + z_first
    good = (y >= 0) & (y < y_count) & (z >= 0) & (z < z_count)
    return jnp.where(good, 1.0, 0.0).astype(jnp.float32)


class Sizes:
    def __init__(self, gx, gy, gz, bx, by, bz):
        self.gx, self.gy, self.gz = gx, gy, gz
        self.bx, self.by, self.bz = bx, by, bz
        self.rows, self.lanes = by + 2 * SIDE, 2 * bz
        self.one = gx == 2
        self.c1_n = bx // 2 + (1 if self.one else 2)
        self.c2_n = bx // 2 + (2 if self.one else 4)
        self.yf_n = bx + (3 if self.one else 6)
        self.nx1, self.ny1 = gx * bx // 2, gy * by // 2
        self.rows1 = self.ny1 + SIDE
        self.rows1p = -(-self.rows1 // 16) * 16
        self.l1 = bz
        self.c1_rows = by // 2 + 4
        self.c2_rows = by // 2 + 8
        self.edge = 5
        self.edge_sets = 1 if self.one else 2
        self.pack1 = self.c1_n * self.c1_rows + self.edge_sets * self.edge * 2 * by
        self.pack2 = self.c2_n * self.c2_rows + self.yf_n * 8

    def c1_first(self, i):
        return -i if self.one else -1

    def c2_first(self, i):
        return -2 * i if self.one else -2

    def yf_first(self, i):
        return -3 * i if self.one else -3


def slab_kernel(k, p_ref, w_ref, right_ref, left_ref):
    bx, bz = k.bx, k.bz
    half, part = bz // 2, bz // 4
    lane = iota((k.by, bz), 1)
    for x in range(bx):
        p = pltpu.roll(p_ref[x], half, 1)
        a, b = w_ref[0, x], w_ref[1, x]
        right_ref[x] = jnp.where(lane < half, p, jnp.where(lane < half + part, pltpu.roll(a, bz - part, 1), b))
        left_ref[x] = jnp.where(lane >= half, p, jnp.where(lane < part, a, pltpu.roll(b, part, 1)))
    for q in range(-(-bx // 4)):
        r_all, l_all = jnp.zeros((k.by, bz), jnp.float32), jnp.zeros((k.by, bz), jnp.float32)
        for r in range(min(4, bx - 4 * q)):
            c = w_ref[2, 4 * q + r]
            here = (lane >= part * r) & (lane < part * (r + 1))
            r_all = jnp.where(here, pltpu.roll(c, (part * r + part) % bz, 1), r_all)
            l_all = jnp.where(here, pltpu.roll(c, part * r, 1) if r else c, l_all)
        right_ref[bx + q] = r_all
        left_ref[bx + q] = l_all


def lane_roll(v, shift):
    shift = shift % v.shape[1]
    return pltpu.roll(v, shift, 1) if shift else v


def pressure_window(k, p, low, high):
    half = k.bz // 2
    lane = iota(p.shape, 1)
    p = pltpu.roll(p, half, 1)
    return jnp.concatenate([jnp.where(lane < half, low, p), jnp.where(lane < half, p, high)], axis=1)


def wind_window(k, w, low, low_at, high, high_at):
    half, part = k.bz // 2, k.bz // 4
    lane = iota(w.shape, 1)
    w = pltpu.roll(w, half, 1)
    first = jnp.where(lane >= half, w, jnp.where(lane >= part, lane_roll(low, part - low_at), 0.0))
    second = jnp.where(lane < half, w, jnp.where(lane < half + part, lane_roll(high, half - high_at), 0.0))
    return jnp.concatenate([first, second], axis=1)


def place():
    return lax.axis_index("gx"), lax.axis_index("gy"), lax.axis_index("gz")


def fine_mask(k, iy, iz):
    return window_mask((k.rows, k.lanes), iy * k.by - SIDE, k.gy * k.by, iz * k.bz - k.bz // 2, k.gz * k.bz)


def x_inside(k, ix, plane):
    place_x = ix * k.bx + plane
    return jnp.where((place_x >= 0) & (place_x < k.gx * k.bx), 1.0, 0.0).astype(jnp.float32)


def restrict_planes(src, first, n, half_ref, out, value):
    rows, lanes = src.shape[1], src.shape[2]
    a = pair_matrix(lanes, half_ref.shape[2], value)

    def step(j):
        s = src[first + 2 * j] + src[first + 2 * j + 1]
        half_ref[j] = dot(s + up(s, 0), a)

    for j in range(n):
        step(j)
    for j in range(n):
        out[j] = half_ref[j, pl.ds(0, rows // 2, stride=2), :]


def zero(ref):
    ref[...] = jnp.zeros(ref.shape, ref.dtype)


def first_kernel(k, p_ref, low_ref, high_ref, win_ref, send_a, send_b, pack_ref, b, m, half_ref, c1):
    ix, iy, iz = place()
    bx, by = k.bx, k.by
    pad = 3
    zero(b)
    zero(m)
    for x in range(bx):
        w = pressure_window(k, p_ref[x], low_ref[x], high_ref[x])
        win_ref[x] = w
        b[x + pad, SIDE:SIDE + by, :] = w
    tail = lax.rem(iy, 2) == 0
    for x in range(bx):
        head_rows, tail_rows = win_ref[x, :8, :], win_ref[x, by - 8:, :]
        send_a[x] = jnp.where(tail, tail_rows, head_rows)
        send_b[x] = jnp.where(tail, head_rows, tail_rows)
    mask = fine_mask(k, iy, iz)

    def step1(i):
        m[i + pad - 1] = mix(b, i + pad - 1) * (mask * x_inside(k, ix, i - 1))

    each(bx + 2, step1)

    def step2(i):
        b[i + pad - 2] = mix(m, i + pad - 2)

    each(bx + 4, step2)
    restrict_planes(b, pad - 2, bx // 2 + 2, half_ref, c1, 0.125)
    start = (k.c1_first(ix) + 1) if k.one else 0
    for j in range(k.c1_n):
        pack_ref[j * k.c1_rows:(j + 1) * k.c1_rows, :] = c1[start + j, 2:2 + k.c1_rows, :]
    at = k.c1_n * k.c1_rows
    starts = [(1 - ix) * (bx - k.edge)] if k.one else [0, bx - k.edge]
    for first in starts:
        for j in range(k.edge):
            for t in range(2):
                pack_ref[at:at + by, :] = win_ref[first + j, :, t * k.bz:(t + 1) * k.bz]
                at += by


def coarse(k, iz, b1, m1, e1, half_ref, b2, u2, v2):
    n1, n2 = k.nx1, k.nx1 // 2
    rows1, rows2, l1 = k.rows1, k.rows1p // 2, k.l1
    y0 = -(SIDE // 2)
    mask1 = window_mask((rows1, l1), y0, k.ny1, iz * (k.bz // 2) - k.bz // 4, k.gz * (k.bz // 2))
    lane2 = iota((rows2, l1), 1)
    mask2 = window_mask((rows2, l1), y0 // 2, k.ny1 // 2, iz * (k.bz // 4) - k.bz // 8, k.gz * (k.bz // 4))
    mask2 = jnp.where(lane2 < l1 // 2, mask2, 0.0)
    zero(m1)
    zero(e1)
    zero(u2)
    zero(v2)
    for i in range(n1):
        b1[i + 2] = b1[i + 2] * mask1

    def pre(i):
        c = mix(b1, i + 2) * mask1
        m1[i + 2] = c
        e1[i + 2] = C1 * (b1[i + 2] + c)

    each(n1, pre)
    a = pair_matrix(l1, l1, 0.125)
    for j in range(n2):
        s = mix(m1, 2 * j + 2) + mix(m1, 2 * j + 3)
        half_ref[j, :rows1, :] = dot(s + up(s, 0), a)
        if k.rows1p > rows1:
            half_ref[j, rows1:, :] = jnp.zeros((k.rows1p - rows1, l1), jnp.float32)
    for j in range(n2):
        s = half_ref[j, pl.ds(0, rows2, stride=2), :] * (mask2 * C2)
        b2[j] = s
        u2[j + 1] = s
    src, dst = u2, v2
    for _ in range(3):
        for j in range(n2):
            dst[j + 1] = (mix(src, j + 1) + b2[j]) * mask2
        src, dst = dst, src
    spread = spread_matrix(l1, l1)
    for j in range(n2):
        e = dot(src[j + 1], spread)
        half_ref[j, pl.ds(0, rows2, stride=2), :] = e
        half_ref[j, pl.ds(1, rows2, stride=2), :] = e
    for j in range(n2):
        e = half_ref[j, :rows1, :]
        e1[2 * j + 2] += e
        e1[2 * j + 3] += e
    for src, dst in ((e1, m1), (m1, e1)):

        def post(i):
            dst[i + 2] = (mix(src, i + 2) + C1 * b1[i + 2]) * mask1

        each(n1, post)


def prolonged(k, e1, ix, iy, first, n, half_ref, put):
    by = k.by
    for j in range(n):
        e = e1[ix * (k.bx // 2) + (first + j + 2), pl.ds(pl.multiple_of(iy * (by // 2), 8), k.rows // 2), :]
        half_ref[j, pl.ds(0, k.rows // 2, stride=2), :] = e
        half_ref[j, pl.ds(1, k.rows // 2, stride=2), :] = e
    spread = spread_matrix(k.l1, k.lanes)
    for j in range(n):
        put(j, dot(half_ref[j], spread))


def overlap_add(k, g_ref, b1, n, rows, y_skip, first_of):
    zero(b1)
    for i in range(k.gx):
        for j in range(k.gy):
            at_y = j * (k.by // 2) + y_skip
            for q in range(n):
                x = i * (k.bx // 2) + first_of(i) + q
                if 0 <= x < k.nx1:
                    part = g_ref[i * k.gy + j, q * rows:(q + 1) * rows, :]
                    b1[x + 2, at_y:at_y + rows, :] += part


def own_lanes(k, v):
    half = k.bz // 2
    first, second = v[:, :k.bz], v[:, k.bz:]
    lane = iota(first.shape, 1)
    return jnp.where(lane < half, pltpu.roll(first, half, 1), pltpu.roll(second, half, 1))


def assemble_edges(k, refs, b1, b, pad):
    g_ref, win_ref, got_a, got_b, w_ref, low_ref, high_ref = refs
    ix, iy, _ = place()
    bx, by = k.bx, k.by
    overlap_add(k, g_ref, b1, k.c1_n, k.c1_rows, 2, k.c1_first)
    even = lax.rem(iy, 2) == 0
    for x in range(bx):
        b[x + pad, :SIDE, :] = jnp.where(even, got_b[x], got_a[x])
        b[x + pad, SIDE:SIDE + by, :] = win_ref[x]
        b[x + pad, SIDE + by:, :] = jnp.where(even, got_a[x], got_b[x])
    base = k.c1_n * k.c1_rows
    span = k.edge * 2 * by
    y_low, y_high = jnp.maximum(iy - 1, 0), jnp.minimum(iy + 1, k.gy - 1)
    for side in range(2):
        if k.one:
            who, shift = 1 - ix, 0
        else:
            who = jnp.maximum(ix - 1, 0) if side == 0 else jnp.minimum(ix + 1, k.gx - 1)
            shift = span if side == 0 else 0
        for j in range(k.edge):
            at = pad - k.edge + j if side == 0 else pad + bx + j
            for t in range(2):
                row = base + shift + (2 * j + t) * by
                lanes = slice(t * k.bz, (t + 1) * k.bz)
                b[at, :SIDE, lanes] = g_ref[who * k.gy + y_low, row + by - 8:row + by, :]
                b[at, SIDE:SIDE + by, lanes] = g_ref[who * k.gy + iy, row:row + by, :]
                b[at, SIDE + by:, lanes] = g_ref[who * k.gy + y_high, row:row + 8, :]
    half, part = k.bz // 2, k.bz // 4

    def winds(x):
        low, high = low_ref[x], high_ref[x]
        q, r = x // 4, x % 4
        return (wind_window(k, w_ref[0, x], low, half, high, 0),
                wind_window(k, w_ref[1, x], low, half + part, high, part),
                wind_window(k, w_ref[2, x], low_ref[bx + q], part * r, high_ref[bx + q], part * r))

    return winds


def middle_kernel(k, assemble, ins, pack_ref, xa_ref, xb_ref, own_ref,
                  b1, m1, e1, half1, b2, u2, v2, b, m, v, vel, flux, half_ref, c2):
    ix, iy, iz = place()
    bx, by = k.bx, k.by
    pad = 5
    winds = assemble(k, ins, b1, b, pad)
    coarse(k, iz, b1, m1, e1, half1, b2, u2, v2)
    mask = fine_mask(k, iy, iz)

    def clean(i):
        b[i] = b[i] * (mask * x_inside(k, ix, i - pad))

    each(bx + 2 * pad, clean)

    def put(j, e):
        for t in range(2):
            v[pad - 4 + 2 * j + t] = e

    prolonged(k, e1, ix, iy, -2, bx // 2 + 4, half_ref, put)

    def pre(i):
        at = i + pad - 4
        here = mask * x_inside(k, ix, i - 4)
        v[at] = (v[at] + C0 * (b[at] + mix(b, at))) * here

    each(bx + 8, pre)

    def post1(i):
        at = i + pad - 3
        m[at] = (mix(v, at) + C0 * b[at]) * (mask * x_inside(k, ix, i - 3))

    each(bx + 6, post1)

    def post2(i):
        at = i + pad - 2
        v[at] = (mix(m, at) + C0 * b[at]) * (mask * x_inside(k, ix, i - 2))

    each(bx + 4, post2)

    def speed(i):
        at = i + pad - 1
        here = 0.5 * (mask * x_inside(k, ix, i - 1))
        c = v[at]
        vel[0, i] = (v[at + 1] - v[at - 1]) * here
        vel[1, i] = (up(c, 0) - down(c, 0)) * here
        vel[2, i] = (up(c, 1) - down(c, 1)) * here

    each(bx + 2, speed)
    own_mask = mask[SIDE:SIDE + by, :]
    zero(flux)
    for x in range(bx):
        w0, w1, w2 = (0.5 * w for w in winds(x))
        for d in range(3):
            c = vel[d, x + 1, SIDE:SIDE + by, :]
            xp, xm = vel[d, x + 2, SIDE:SIDE + by, :], vel[d, x, SIDE:SIDE + by, :]
            yp, ym = vel[d, x + 1, SIDE + 1:SIDE + by + 1, :], vel[d, x + 1, SIDE - 1:SIDE + by - 1, :]
            zp, zm = up(c, 1), down(c, 1)
            near = (xp + xm) + (yp + ym) + (zp + zm)
            total = 7.0 * c - near + w0 * (xp - xm) + w1 * (yp - ym) + w2 * (zp - zm)
            flux[d, x + 2, SIDE:SIDE + by, :] = total * own_mask
    zero(b)
    zero(m)

    def spread_flux(i):
        at = i + pad - 1
        f1, f2 = flux[1, i + 1], flux[2, i + 1]
        total = (flux[0, i + 2] - flux[0, i]) + (up(f1, 0) - down(f1, 0)) + (up(f2, 1) - down(f2, 1))
        b[at] = total * (-0.5 * (mask * x_inside(k, ix, i - 1)))

    each(bx + 2, spread_flux)
    zero(v)

    def power1_pure(i):
        at = i + pad - 2
        m[at] = mix(b, at) * (mask * x_inside(k, ix, i - 2))

    each(bx + 4, power1_pure)

    def power2(i):
        at = i + pad - 3
        v[at] = mix(m, at) * (mask * x_inside(k, ix, i - 3))

    each(bx + 6, power2)

    def power3(i):
        at = i + pad - 4
        b[at] = C0 * ((b[at] + m[at]) + (v[at] + mix(v, at))) * (mask * x_inside(k, ix, i - 4))

    each(bx + 8, power3)
    restrict_planes(v, pad - 4, bx // 2 + 4, half_ref, c2, 0.125)
    start = (k.c2_first(ix) + 2) if k.one else 0
    for j in range(k.c2_n):
        pack_ref[j * k.c2_rows:(j + 1) * k.c2_rows, :] = c2[start + j]
    row8 = iota((8, k.bz), 0)
    at = k.c2_n * k.c2_rows
    start = (k.yf_first(ix) if k.one else -3) + pad
    for j in range(k.yf_n):
        c = own_lanes(k, jnp.where(iota((8, k.lanes), 0) < 4, b[start + j, SIDE + by:, :], b[start + j, :SIDE, :]))
        pack_ref[at:at + 8, :] = c
        at += 8
    upper = lax.rem(ix, 2) == 0
    first_a = pad + jnp.where(upper, bx, -4)
    first_b = pad + jnp.where(upper, -4, bx)
    for j in range(4):
        xa_ref[j] = own_lanes(k, b[first_a + j, SIDE:SIDE + by, :])
        if xb_ref is not None:
            xb_ref[j] = own_lanes(k, b[first_b + j, SIDE:SIDE + by, :])
    for x in range(bx):
        own_ref[x] = own_lanes(k, b[x + pad, SIDE:SIDE + by, :])


def last_kernel(k, g_ref, own_ref, xa_ref, xb_ref, out_ref, b1, m1, e1, half1, b2, u2, v2, v, m, half_ref):
    ix, iy, iz = place()
    bx, by = k.bx, k.by
    overlap_add(k, g_ref, b1, k.c2_n, k.c2_rows, 0, k.c2_first)
    coarse(k, iz, b1, m1, e1, half1, b2, u2, v2)
    pad = 2
    mask = fine_mask(k, iy, iz)

    def put(j, e):
        for t in range(2):
            plane = -2 + 2 * j + t
            v[pad + plane] = e * (mask * x_inside(k, ix, plane))

    prolonged(k, e1, ix, iy, -1, bx // 2 + 2, half_ref, put)

    def post1(i):
        at = i + pad - 1
        m[at] = mix(v, at) * (mask * x_inside(k, ix, i - 1))

    each(bx + 2, post1)
    base = k.c2_n * k.c2_rows
    low_ok = jnp.where(iy > 0, 1.0, 0.0).astype(jnp.float32)
    high_ok = jnp.where(iy < k.gy - 1, 1.0, 0.0).astype(jnp.float32)
    y_low, y_high = jnp.maximum(iy - 1, 0), jnp.minimum(iy + 1, k.gy - 1)
    row8 = iota((8, k.bz), 0)
    low_keep = jnp.where(row8 < 4, low_ok, 0.0)
    high_keep = jnp.where(row8 >= 4, high_ok, 0.0)
    for x in range(bx):
        out_ref[x] = own_lanes(k, mix(m, x + pad)[SIDE:SIDE + by, :]) + own_ref[x]

    def frame(who, first, x_from, x_to, ok):
        for x in range(x_from, x_to):
            row = base + (x - first) * 8
            if not isinstance(row, int):
                row = pl.multiple_of(row, 8)
            lo = g_ref[who * k.gy + y_low, pl.ds(row, 8), :] * ok
            hi = g_ref[who * k.gy + y_high, pl.ds(row, 8), :] * ok
            out_ref[x, :8, :] += lo * low_keep
            out_ref[x, by - 8:, :] += hi * high_keep

    one = jnp.float32(1.0)
    frame(ix, k.yf_first(ix), 0, bx, one)
    upper = lax.rem(ix, 2) == 0
    if k.one:
        for j in range(3):
            x = jnp.where(ix == 0, bx - 3 + j, j)
            row = pl.multiple_of(base + jnp.where(ix == 0, j, bx + j) * 8, 8)
            lo = g_ref[(1 - ix) * k.gy + y_low, pl.ds(row, 8), :]
            hi = g_ref[(1 - ix) * k.gy + y_high, pl.ds(row, 8), :]
            out_ref[x, :8, :] += lo * low_keep
            out_ref[x, by - 8:, :] += hi * high_keep
    else:
        frame(jnp.maximum(ix - 1, 0), -3 - bx, 0, 3, jnp.where(ix > 0, 1.0, 0.0).astype(jnp.float32))
        frame(jnp.minimum(ix + 1, k.gx - 1), bx - 3, bx - 3, bx, jnp.where(ix < k.gx - 1, 1.0, 0.0).astype(jnp.float32))
    for j in range(4):
        out_ref[jnp.where(upper, bx - 4, 0) + j] += xa_ref[j]
        if xb_ref is not None:
            out_ref[jnp.where(upper, 0, bx - 4) + j] += xb_ref[j]


def call(kernel, outs, scratch, args, flops):
    f32 = lambda s: jax.ShapeDtypeStruct(s, jnp.float32)
    return pl.pallas_call(
        kernel,
        out_shape=[f32(s) for s in outs],
        scratch_shapes=[pltpu.VMEM(s, jnp.float32) for s in scratch],
        compiler_params=pltpu.CompilerParams(vmem_limit_bytes=40 * 1024 * 1024),
        cost_estimate=pl.CostEstimate(flops=flops, bytes_accessed=1 << 20, transcendentals=0),
    )(*args)


def pairs(n):
    first = [(i, i ^ 1) for i in range(n) if (i ^ 1) < n]
    second = [(i + s, i + 1 - s) for i in range(1, n - 1, 2) for s in (0, 1)]
    return first, second


def chain(n, step):
    return [(i, i + step) for i in range(n) if 0 <= i + step < n]


def coarse_scratch(k):
    n1, n2, rows2 = k.nx1, k.nx1 // 2, k.rows1p // 2
    big = (n1 + 4, k.rows1, k.l1)
    return [big, big, big, (n2, k.rows1p, k.l1), (n2, rows2, k.l1), (n2 + 2, rows2, k.l1), (n2 + 2, rows2, k.l1)]


def edge_form(k, pressure, wind):
    bx, by, bz = k.bx, k.by, k.bz
    slab = (bx + -(-bx // 4), by, bz)
    right, left = call(functools.partial(slab_kernel, k), [slab, slab], [], (pressure, wind), 1 << 20)
    low = lax.ppermute(right, "gz", chain(k.gz, 1))
    high = lax.ppermute(left, "gz", chain(k.gz, -1))
    fine = lambda n: (n, k.rows, k.lanes)
    window, send_a, send_b, pack = call(
        functools.partial(first_kernel, k),
        [(bx, by, k.lanes), (bx, 8, k.lanes), (bx, 8, k.lanes), (k.pack1, bz)],
        [fine(bx + 6), fine(bx + 6), (bx // 2 + 2, k.rows, k.l1), (bx // 2 + 2, k.rows // 2, k.l1)],
        (pressure, low, high), 1 << 22)
    ya, yb = pairs(k.gy)
    got_a = lax.ppermute(send_a, "gy", ya)
    got_b = lax.ppermute(send_b, "gy", yb)
    gathered = lax.all_gather(pack, PLANE)
    return assemble_edges, (gathered, window, got_a, got_b, wind, low, high)


def general(k, pressure, wind):
    bx, by, bz = k.bx, k.by, k.bz
    fine = lambda n: (n, k.rows, k.lanes)
    assemble, args = edge_form(k, pressure, wind)
    xa, xb = pairs(k.gx)
    x_outs = [(4, by, bz)] * (2 if xb else 1)

    def middle(*refs):
        ins, rest = refs[:len(args)], refs[len(args):]
        pack_ref, rest = rest[0], rest[1:]
        xa_ref, rest = rest[0], rest[1:]
        xb_ref = None
        if xb:
            xb_ref, rest = rest[0], rest[1:]
        middle_kernel(k, assemble, ins, pack_ref, xa_ref, xb_ref, *rest)

    big = fine(bx + 10)
    outs = call(
        middle, [(k.pack2, bz)] + x_outs + [(bx, by, bz)],
        coarse_scratch(k) + [big, big, big, (3,) + fine(bx + 2), (3,) + fine(bx + 4),
                             (bx // 2 + 4, k.rows, k.l1), (bx // 2 + 4, k.rows // 2, k.l1)],
        args, 1 << 24)
    pack, frames, own = outs[0], outs[1:-1], outs[-1]
    got = [lax.ppermute(f, "gx", perm) for f, perm in zip(frames, (xa, xb))]
    gathered = lax.all_gather(pack, PLANE)

    def last(*refs):
        g_ref, own_ref, xa_ref, rest = refs[0], refs[1], refs[2], refs[3:]
        xb_ref = None
        if xb:
            xb_ref, rest = rest[0], rest[1:]
        last_kernel(k, g_ref, own_ref, xa_ref, xb_ref, *rest)

    (result,) = call(
        last, [(bx, by, bz)],
        coarse_scratch(k) + [fine(bx + 4), fine(bx + 4), (bx // 2 + 2, k.rows, k.l1)],
        (gathered, own, *got), 1 << 23)
    return result


FR = 5
TOP = 8
CR = 2


class Mirror:
    def __init__(self, gx, gy, gz, bx, by, bz):
        self.gx, self.gy, self.gz, self.bx, self.by, self.bz = gx, gy, gz, bx, by, bz
        self.rows = by + 2 * FR
        self.core = by + 8
        self.nx, self.ny = gx * bx, gy * by
        self.nx1, self.ny1 = self.nx // 2, self.ny // 2
        self.rows1 = self.ny1 + 8
        self.part = bz // 4
        groups = lambda n: -(-n // 4)
        self.fine_n = bx + 5
        self.at_fine = groups(self.nx1) * self.ny1
        self.slab_rows = self.at_fine + groups(self.fine_n) * self.rows
        self.wind_rows = groups(3 * bx) * by
        self.c2_n, self.c2_rows = bx // 2 + 2, by // 2 + 4
        self.c2 = self.c2_n * self.c2_rows
        self.yf_n = bx + 3
        self.to3 = self.c2 + 8 * self.yf_n
        self.to4 = self.c2 + 8 * 3 + 4 * by
        self.to7 = self.c2 + 8 * 3
        self.to1 = 4 * self.c2 + 8 * self.yf_n + 8 * 3


def exact_dot(x, a):
    high = x.astype(jnp.bfloat16)
    low = (x - high.astype(jnp.float32)).astype(jnp.bfloat16)
    return (jnp.dot(high, a, preferred_element_type=jnp.float32)
            + jnp.dot(low, a, preferred_element_type=jnp.float32))


def matrix(hit, value):
    return jnp.where(hit, value, 0.0).astype(jnp.float32).astype(jnp.bfloat16)


def flag(good):
    return jnp.where(good, 1.0, 0.0).astype(jnp.float32)


def beside(c0, c1):
    n = c0.shape[1]
    lane = iota(c0.shape, 1)
    last, first = lane == n - 1, lane == 0
    u0, u1, d0, d1 = up(c0, 1), up(c1, 1), down(c0, 1), down(c1, 1)
    return ((jnp.where(last, u1, u0), jnp.where(last, u0, u1)),
            (jnp.where(first, d1, d0), jnp.where(first, d0, d1)))


def mix_halves(s, i, halves=2):
    n = s.shape[2] - 2
    c = [s[i + 1, h, 1:1 + n, :] for h in range(2)]
    plus, minus = beside(*c)
    out = []
    for h in range(halves):
        near = (s[i, h, 1:1 + n, :] + s[i + 2, h, 1:1 + n, :]) + (s[i + 1, h, 2:2 + n, :] + s[i + 1, h, :n, :])
        out.append((1.0 - OMEGA) * c[h] + W * (near + (plus[h] + minus[h])))
    return out


def halves_mask(k, iy, iz):
    y = iota((k.core, k.bz), 0) + (iy * k.by - 4)
    lane = iota((k.core, k.bz), 1)
    y_good = (y >= 0) & (y < k.ny)
    edge = flag(y_good)
    side = jnp.where(lane < k.bz // 2, jnp.where(iz < k.gz - 1, 1.0, 0.0), jnp.where(iz > 0, 1.0, 0.0))
    return edge, edge * side.astype(jnp.float32)


def zero_rim(s):
    s[0] = jnp.zeros(s.shape[1:], jnp.float32)
    n = s.shape[2]
    for i in range(1, s.shape[0]):
        for h in range(2):
            s[i, h, 0:1, :] = jnp.zeros((1, s.shape[3]), jnp.float32)
            s[i, h, n - 1:n, :] = jnp.zeros((1, s.shape[3]), jnp.float32)


def mix1(s, i, n, at):
    c = s[i + 1, at:at + n, :]
    near = (s[i, at:at + n, :] + s[i + 2, at:at + n, :]) + (s[i + 1, at + 1:at + n + 1, :] + s[i + 1, at - 1:at + n - 1, :])
    return (1.0 - OMEGA) * c + W * (near + (up(c, 1) + down(c, 1)))


def coarse_plane(k, iz, b1, m1, e1, half_ref, b2, u2, v2):
    n1, n2, ny, l1 = k.nx1, k.nx1 // 2, k.ny1, k.bz
    ny2 = ny // 2
    lane = iota((ny, l1), 1)
    low_ok, high_ok = flag(iz > 0), flag(iz < k.gz - 1)
    mask1 = jnp.where(lane < l1 // 2, 1.0, jnp.where(lane < 3 * l1 // 4, high_ok, low_ok))
    lane2 = iota((ny2, l1), 1)
    own2 = l1 // 8
    mask2 = jnp.where(lane2 < own2, low_ok, jnp.where(lane2 < 3 * own2, 1.0, jnp.where(lane2 < 4 * own2, high_ok, 0.0)))
    for s in (m1, e1):
        for i in (0, n1 + 1):
            s[i] = jnp.zeros(s.shape[1:], jnp.float32)
    for s in (b1, m1, e1):
        for i in range(n1):
            s[i + 1, :CR, :] = jnp.zeros((CR, l1), jnp.float32)
            s[i + 1, CR + ny:, :] = jnp.zeros((k.rows1 - CR - ny, l1), jnp.float32)
    zero(u2)
    zero(v2)
    for i in range(n1):
        b1[i + 1, CR:CR + ny, :] = b1[i + 1, CR:CR + ny, :] * mask1
    for i in range(n1):
        c = mix1(b1, i, ny, CR) * mask1
        m1[i + 1, CR:CR + ny, :] = c
        e1[i + 1, CR:CR + ny, :] = C1 * (b1[i + 1, CR:CR + ny, :] + c)
    row, column = iota((l1, l1), 0), iota((l1, l1), 1)
    linear = lambda x: (jnp.where(x < 3 * l1 // 4, x, x - l1) >> 1) + own2
    for j in range(n2):
        half_ref[j] = mix1(m1, 2 * j, ny, CR) + mix1(m1, 2 * j + 1, ny, CR)
    pairs_sum = [half_ref[j, pl.ds(0, ny2, stride=2), :] + half_ref[j, pl.ds(1, ny2, stride=2), :] for j in range(n2)]
    r2 = exact_dot(jnp.concatenate(pairs_sum, axis=0), matrix(linear(row) == column, 0.125))
    for j in range(n2):
        c = r2[j * ny2:(j + 1) * ny2] * (mask2 * C2)
        b2[j] = c
        u2[j + 1, 1:1 + ny2, :] = c
    src, dst = u2, v2
    for _ in range(3):
        for j in range(n2):
            dst[j + 1, 1:1 + ny2, :] = (mix1(src, j, ny2, 1) + b2[j]) * mask2
        src, dst = dst, src
    stack = jnp.concatenate([src[j + 1, 1:1 + ny2, :] for j in range(n2)], axis=0)
    spread = exact_dot(stack, matrix(row == linear(column), 1.0))
    for j in range(n2):
        e = spread[j * ny2:(j + 1) * ny2]
        half_ref[j, pl.ds(0, ny2, stride=2), :] = e
        half_ref[j, pl.ds(1, ny2, stride=2), :] = e
    for j in range(n2):
        e = half_ref[j]
        for t in range(2):
            e1[2 * j + t + 1, CR:CR + ny, :] = e1[2 * j + t + 1, CR:CR + ny, :] + e
    for src, dst in ((e1, m1), (m1, e1)):
        for i in range(n1):
            dst[i + 1, CR:CR + ny, :] = (mix1(src, i, ny, CR) + C1 * b1[i + 1, CR:CR + ny, :]) * mask1


def from_end(ix, i, count):
    return jnp.where(ix == 0, i, count - 1 - i)


def prolong_halves(k, iy, e1, n, v):
    rows = k.core // 2
    first = pl.multiple_of(iy * (k.by // 2), 8)
    stack = jnp.concatenate([e1[j + 1, pl.ds(first, 16), :] for j in range(n)], axis=0)
    row, column = iota((k.bz, 2 * k.bz), 0), iota((k.bz, 2 * k.bz), 1)
    spread = exact_dot(stack, matrix(row == (column >> 1), 1.0))
    for j in range(n):
        for h in range(2):
            e = spread[16 * j:16 * j + rows, h * k.bz:(h + 1) * k.bz]
            for t in range(2):
                v[2 * j + t + 1, h, pl.ds(1, rows, stride=2), :] = e
                v[2 * j + t + 1, h, pl.ds(2, rows, stride=2), :] = e


def take_slab(k, ref, base, rows, i, to):
    at = base + (i // 4) * rows
    return lane_roll(ref[at:at + rows, :], to - k.part * (i % 4))


def pack_slabs(k, iz, first_ref, second_ref, base, rows, n, load, right_lane, left_lane):
    part, bz = k.part, k.bz
    even = lax.rem(iz, 2) == 0
    lane = iota((rows, bz), 1)
    for group in range(-(-n // 4)):
        right, left = jnp.zeros((rows, bz), jnp.float32), jnp.zeros((rows, bz), jnp.float32)
        for r in range(min(4, n - 4 * group)):
            here = (lane >= part * r) & (lane < part * (r + 1))
            c = load(4 * group + r)
            right = jnp.where(here, lane_roll(c, part * r - right_lane), right)
            left = jnp.where(here, lane_roll(c, part * r - left_lane), left)
        at = slice(base + group * rows, base + (group + 1) * rows)
        first_ref[at, :] = jnp.where(even, right, left)
        second_ref[at, :] = jnp.where(even, left, right)


def wind_kernel(k, p_ref, w_ref, own_ref, first_ref, second_ref):
    ix, _, iz = place()
    own_ref[...] = p_ref[...]
    pack_slabs(k, iz, first_ref, second_ref, 0, k.by, 3 * k.bx,
               lambda i: w_ref[i // k.bx, from_end(ix, i % k.bx, k.bx)], 3 * k.part, 0)


def join_kernel(a_ref, b_ref, c_ref, d_ref, out_ref):
    for i, ref in enumerate((a_ref, b_ref, c_ref, d_ref)):
        out_ref[i] = ref[...]


def plane_kernel(k, mine_ref, theirs_ref, c1_ref, win_ref, first_ref, second_ref, p, m, q, half_ref, wide):
    ix, iy, iz = place()
    bx, by, bz, nx, ny, part = k.bx, k.by, k.bz, k.nx, k.ny, k.part
    p[0] = jnp.zeros(p.shape[1:], jnp.float32)
    p[nx + 1] = jnp.zeros(p.shape[1:], jnp.float32)
    m[0] = jnp.zeros(m.shape[1:], jnp.float32)
    m[nx + 1] = jnp.zeros(m.shape[1:], jnp.float32)
    for x in range(nx):
        p[x + 1, :TOP, :] = jnp.zeros((TOP, bz), jnp.float32)
        p[x + 1, TOP + ny:, :] = jnp.zeros((p.shape[1] - TOP - ny, bz), jnp.float32)
        m[x + 1, 0:1, :] = jnp.zeros((1, bz), jnp.float32)
        m[x + 1, ny + 1:, :] = jnp.zeros((m.shape[1] - ny - 1, bz), jnp.float32)
    for side in range(2):
        for other, ref, block in ((0, mine_ref, 0), (3, mine_ref, 1), (1, theirs_ref, 0), (2, theirs_ref, 1)):
            at = pl.multiple_of(TOP + by * (iy ^ other), 8)
            for x in range(bx):
                p[side * bx + x + 1, pl.ds(at, by), :] = ref[2 * side + block, from_end(ix, x, bx)]
    lane = iota((ny, bz), 1)
    first, last = lane == 0, lane == bz - 1
    ends = jnp.where(first, flag(iz > 0), jnp.where(last, flag(iz < k.gz - 1), 0.0)) * (W * W)

    def parts(s, x, at):
        c = s[x + 1, at:at + ny, :]
        four = (s[x, at:at + ny, :] + s[x + 2, at:at + ny, :]) + (s[x + 1, at + 1:at + ny + 1, :] + s[x + 1, at - 1:at + ny - 1, :])
        along = jnp.where(last, 0.0, up(c, 1)) + jnp.where(first, 0.0, down(c, 1))
        return c, four, (1.0 - OMEGA) * c + W * (four + along)

    for x in range(nx):
        c, four, mixed = parts(p, x, TOP)
        m[x + 1, 1:1 + ny, :] = mixed
        q[x] = (1.0 - OMEGA + W) * c + (mixed + W * four)
    row, column = iota((bz, bz), 0), iota((bz, bz), 1)
    own = matrix((row >> 1) == column, 0.125)
    rim = ((row == 0) & (column == bz - 1)) | ((row == bz - 1) & (column == bz // 2))
    rim = matrix(rim, 0.125)
    half_rows = ny // 2
    for j in range(k.nx1):
        s = None
        for x in (2 * j, 2 * j + 1):
            r = parts(m, x, 1)[2] + ends * p[x + 1, TOP:TOP + ny, :]
            s = r if s is None else s + r
        half_ref[j] = s
        t = (q[2 * j, pl.ds(0, half_rows, stride=2), :] + q[2 * j, pl.ds(1, half_rows, stride=2), :]
             + q[2 * j + 1, pl.ds(0, half_rows, stride=2), :] + q[2 * j + 1, pl.ds(1, half_rows, stride=2), :])
        s = half_ref[j, pl.ds(0, half_rows, stride=2), :] + half_ref[j, pl.ds(1, half_rows, stride=2), :]
        c1_ref[j] = exact_dot(s, own) + exact_dot(W * t, rim)

    for i in range(k.fine_n):
        wide[i] = p[i + 1, pl.ds(pl.multiple_of(iy * by, 8), by + 16), :]
    for i in range(k.fine_n):
        win_ref[i] = wide[i, TOP - FR:TOP + by + FR, :]
    pack = functools.partial(pack_slabs, k, iz, first_ref, second_ref)
    pack(0, k.ny1, k.nx1, lambda i: c1_ref[i], part + 1, bz - 1)
    pack(k.at_fine, k.rows, k.fine_n, lambda i: win_ref[i], 3 * part, 0)


def solve_kernel(k, c1_ref, win_ref, w_ref, first_ref, second_ref, wind1_ref, wind2_ref, to3_ref, to4_ref, to7_ref, own_ref,
                 low_ref, high_ref, low_wind, high_wind, b1, m1, e1, half1, b2, u2, v2, b, m, v, vel, flux, half_ref):
    ix, iy, iz = place()
    bx, by, bz, part, n = k.bx, k.by, k.bz, k.part, k.core
    even = lax.rem(iz, 2) == 0
    for low, high, first, second in ((low_ref, high_ref, first_ref, second_ref), (low_wind, high_wind, wind1_ref, wind2_ref)):
        low[...] = jnp.where(even, second[...], first[...])
        high[...] = jnp.where(even, first[...], second[...])
    lane = iota((k.ny1, bz), 1)
    for s in (b1,):
        for i in (0, k.nx1 + 1):
            s[i] = jnp.zeros(s.shape[1:], jnp.float32)
    for x in range(k.nx1):
        low = take_slab(k, low_ref, 0, k.ny1, x, 3 * part + 1)
        high = take_slab(k, high_ref, 0, k.ny1, x, 2 * part - 1)
        low = jnp.where((lane >= 3 * part + 1) | (lane == 0), low, 0.0)
        high = jnp.where((lane >= 2 * part - 1) & (lane < 3 * part - 1), high, 0.0)
        b1[x + 1, CR:CR + k.ny1, :] = c1_ref[x] + (low + high)
    coarse_plane(k, iz, b1, m1, e1, half1, b2, u2, v2)
    mask = halves_mask(k, iy, iz)
    for s in (b, m, v):
        zero_rim(s)

    def outer(low, high, lane):
        return jnp.where(lane >= 3 * part, low, jnp.where(lane < part, high, 0.0))

    lane = iota((k.rows, bz), 1)
    for i in range(k.fine_n):
        b[i + 1, 0] = win_ref[i]
        b[i + 1, 1] = outer(take_slab(k, low_ref, k.at_fine, k.rows, i, 3 * part),
                            take_slab(k, high_ref, k.at_fine, k.rows, i, 0), lane)
    prolong_halves(k, iy, e1, bx // 2 + 2, v)
    for i in range(bx + 4):
        mb = mix_halves(b, i)
        for h in range(2):
            v[i + 1, h, 1:1 + n, :] = (v[i + 1, h, 1:1 + n, :] + C0 * (b[i + 1, h, 1:1 + n, :] + mb[h])) * mask[h]
    for src, dst, count in ((v, m, bx + 3), (m, v, bx + 2)):
        for i in range(count):
            c = mix_halves(src, i)
            for h in range(2):
                dst[i + 1, h, 1:1 + n, :] = (c[h] + C0 * b[i + 1, h, 1:1 + n, :]) * mask[h]
    half_mask = [0.5 * c for c in mask]
    for d in range(3):
        vel[d, 0] = jnp.zeros(vel.shape[2:], jnp.float32)
    for i in range(bx + 1):
        plus, minus = beside(v[i + 1, 0, 1:1 + n, :], v[i + 1, 1, 1:1 + n, :])
        for h in range(2):
            vel[0, i + 1, h] = (v[i + 2, h, 1:1 + n, :] - v[i, h, 1:1 + n, :]) * half_mask[h]
            vel[1, i + 1, h] = (v[i + 1, h, 2:2 + n, :] - v[i + 1, h, :n, :]) * half_mask[h]
            vel[2, i + 1, h] = (plus[h] - minus[h]) * half_mask[h]
    own_at = 4
    zero(flux)
    sign = jnp.where(ix == 0, 0.5, -0.5).astype(jnp.float32)
    lane = iota((by, bz), 1)
    for x in range(bx):
        winds = []
        for d in range(3):
            low = take_slab(k, low_wind, 0, by, d * bx + x, 3 * part)
            high = take_slab(k, high_wind, 0, by, d * bx + x, 0)
            scale = sign if d == 0 else 0.5
            winds.append((scale * w_ref[d, from_end(ix, x, bx)], scale * outer(low, high, lane)))
        for d in range(3):
            at = lambda i, h, r: vel[d, i + 1, h, own_at + r:own_at + r + by, :]
            c = [at(x, h, 0) for h in range(2)]
            plus, minus = beside(*c)
            for h in range(2):
                xp, xm, yp, ym, zp, zm = at(x + 1, h, 0), at(x - 1, h, 0), at(x, h, 1), at(x, h, -1), plus[h], minus[h]
                near = (xp + xm) + (yp + ym) + (zp + zm)
                total = 7.0 * c[h] - near + winds[0][h] * (xp - xm) + winds[1][h] * (yp - ym) + winds[2][h] * (zp - zm)
                if h == 1:
                    total = total * mask[1][own_at:own_at + by]
                flux[d, x + 1, h, own_at + 1:own_at + 1 + by, :] = total
    minus_mask = [-0.5 * c for c in mask]
    for s, first in ((b, bx + 2), (m, bx + 3), (v, bx + 4)):
        for i in range(first, bx + 6):
            s[i] = jnp.zeros(s.shape[1:], jnp.float32)
    for i in range(bx + 1):
        plus, minus = beside(flux[2, i + 1, 0, 1:1 + n, :], flux[2, i + 1, 1, 1:1 + n, :])
        for h in range(2):
            total = (flux[0, i + 2, h, 1:1 + n, :] - flux[0, i, h, 1:1 + n, :]
                     + (flux[1, i + 1, h, 2:2 + n, :] - flux[1, i + 1, h, :n, :]) + (plus[h] - minus[h]))
            b[i + 1, h, 1:1 + n, :] = total * minus_mask[h]
    zero_rows = jnp.zeros((1, bz), jnp.float32)
    for i in range(bx + 1):
        for h in range(2):
            b[i + 1, h, 0:1, :] = zero_rows
            b[i + 1, h, n + 1:n + 2, :] = zero_rows
    for src, dst, count in ((b, m, bx + 2), (m, v, bx + 3)):
        for i in range(count):
            c = mix_halves(src, i)
            for h in range(2):
                dst[i + 1, h, 1:1 + n, :] = c[h] * mask[h]
    half_rows = n // 2
    for j in range(k.c2_n):
        for h in range(2):
            take = lambda i, r: v[i + 1, h, pl.ds(r, half_rows, stride=2), :]
            half_ref[h, j, :half_rows, :] = (take(2 * j, 1) + take(2 * j, 2)) + (take(2 * j + 1, 1) + take(2 * j + 1, 2))
            half_ref[h, j, half_rows:, :] = jnp.zeros((16 - half_rows, bz), jnp.float32)
    row, column = iota((bz, bz), 0), iota((bz, bz), 1)
    c2 = (exact_dot(half_ref[0].reshape(k.c2_n * 16, bz), matrix((row >> 1) == column, 0.125))
          + exact_dot(half_ref[1].reshape(k.c2_n * 16, bz), matrix((row >> 1) + bz // 2 == column, 0.125)))
    for j in range(k.c2_n):
        for ref in (to3_ref, to4_ref, to7_ref):
            ref[j * k.c2_rows:(j + 1) * k.c2_rows, :] = c2[16 * j:16 * j + k.c2_rows]
    for i in range(bx + 4):
        c = mix_halves(v, i, 1)[0]
        at = lambda s: s[i + 1, 0, 1:1 + n, :]
        c = C0 * ((at(b) + at(m)) + (at(v) + c)) * mask[0]
        if i < bx:
            own_ref[i] = c[4:4 + by]
        else:
            row = k.to7 + by * (i - bx)
            to4_ref[row:row + by, :] = c[4:4 + by]
        places = [(to3_ref, k.c2 + 8 * i)] if i < k.yf_n else []
        if bx <= i < k.yf_n:
            places += [(ref, k.c2 + 8 * (i - bx)) for ref in (to4_ref, to7_ref)]
        for ref, row in places:
            ref[row:row + 4, :] = c[4 + by:8 + by]
            ref[row + 4:row + 8, :] = c[:4]


def share_kernel(k, own_ref, got3_ref, got4_ref, got7_ref, out_ref):
    c2 = k.c2
    for n, ref in enumerate((own_ref, got3_ref, got4_ref, got7_ref)):
        out_ref[n * c2:(n + 1) * c2, :] = ref[:c2, :]
    out_ref[4 * c2:4 * c2 + 8 * k.yf_n, :] = own_ref[c2:, :]
    out_ref[4 * c2 + 8 * k.yf_n:, :] = got4_ref[c2:c2 + 24, :]


def close_kernel(k, mine_ref, got_ref, got3_ref, got4_ref, got7_ref, own_ref, out_ref,
                 parts, b1, m1, e1, half1, b2, u2, v2, v, m):
    ix, iy, iz = place()
    bx, by, n, c2 = k.bx, k.by, k.core, k.c2
    for slot, near, far in ((0, mine_ref, 0), (3, mine_ref, 1), (1, got_ref, 0), (2, got_ref, 1)):
        parts[slot] = near[far * c2:(far + 1) * c2, :]
        parts[4 + slot] = near[(2 + far) * c2:(3 + far) * c2, :]
    zero(b1)
    for side in range(2):
        for j in range(k.gy):
            at = j * (by // 2)
            slot = 4 * side + (iy ^ j)
            for q in range(k.c2_n):
                x = q if side == 0 else k.nx1 - 1 - q
                b1[x + 1, at:at + k.c2_rows, :] += parts[slot, q * k.c2_rows:(q + 1) * k.c2_rows, :]
    coarse_plane(k, iz, b1, m1, e1, half1, b2, u2, v2)
    mask = halves_mask(k, iy, iz)
    for s in (v, m):
        zero_rim(s)
    prolong_halves(k, iy, e1, bx // 2 + 1, v)
    for i in range(bx + 2):
        for h in range(2):
            v[i + 1, h, 1:1 + n, :] = v[i + 1, h, 1:1 + n, :] * mask[h]
    for i in range(bx + 1):
        c = mix_halves(v, i)
        for h in range(2):
            m[i + 1, h, 1:1 + n, :] = c[h] * mask[h]
    odd = lax.rem(iy, 2) == 1
    chip_ok = flag((iy > 0) & (iy < k.gy - 1))

    def frames(core, core_at, chip, chip_at):
        row = lambda ref, at, r: ref[at + r:at + r + 4, :]
        low = jnp.where(odd, row(core, core_at, 0), row(chip, chip_at, 0) * chip_ok)
        high = jnp.where(odd, row(chip, chip_at, 4) * chip_ok, row(core, core_at, 4))
        return low, high

    for i in range(bx):
        c = mix_halves(m, i, 1)[0][4:4 + by] + own_ref[i]
        if i >= bx - 4:
            row = k.to7 + by * (bx - 1 - i)
            c = c + got4_ref[row:row + by, :]
        at = from_end(ix, i, bx)
        out_ref[at] = c
        low, high = frames(got_ref, 4 * c2 + 8 * i, got3_ref, c2 + 8 * i)
        if i >= bx - 3:
            row = 8 * (bx - 1 - i)
            low2, high2 = frames(got_ref, 4 * c2 + 8 * k.yf_n + row, got7_ref, c2 + row)
            low, high = low + low2, high + high2
        out_ref[at, :4, :] += low
        out_ref[at, by - 4:, :] += high


def mirrored(k, pressure, wind):
    bx, by, bz = k.bx, k.by, k.bz
    n1, n2 = k.nx1, k.nx1 // 2
    fine = lambda n: (n + 2, 2, k.rows, bz)
    level1 = [(n1 + 2, k.rows1, bz)] * 3
    level2 = [(n2, k.ny1, bz), (n2, k.ny1 // 2, bz)] + [(n2 + 2, k.ny1 // 2 + 2, bz)] * 2
    crossed = lambda v, d: lax.ppermute(v, PLANE, [(i, i ^ d) for i in range(k.gx * k.gy)])
    swapped = lambda pair: [lax.ppermute(v, "gz", p) for v, p in zip(pair, pairs(k.gz))]
    got = [crossed(pressure, d) for d in (3, 4, 7)]
    mine, *wind_slabs = call(
        functools.partial(wind_kernel, k), [(bx, by, bz)] + [(k.wind_rows, bz)] * 2, [], (pressure, wind), 1 << 18)
    wind_slabs = swapped(wind_slabs)
    (mine,) = call(join_kernel, [(4, bx, by, bz)], [], (mine, *got), 1 << 12)
    c1, window, first, second = call(
        functools.partial(plane_kernel, k),
        [(n1, k.ny1, bz), (k.fine_n, k.rows, bz), (k.slab_rows, bz), (k.slab_rows, bz)],
        [(k.nx + 2, k.ny + 2 * TOP, bz), (k.nx + 2, k.ny + 2, bz), (k.nx, k.ny, bz), (n1, k.ny, bz), (k.fine_n, by + 16, bz)],
        (mine, crossed(mine, 1)), 1 << 22)
    first, second = swapped((first, second))
    to3, to4, to7, own = call(
        functools.partial(solve_kernel, k),
        [(k.to3, bz), (k.to4, bz), (k.to7, bz), (bx, by, bz)],
        [(k.slab_rows, bz)] * 2 + [(k.wind_rows, bz)] * 2 + level1 + level2 + [fine(bx + 5)] * 3 + [(3, bx + 3, 2, k.core, bz), (3,) + fine(bx + 1), (2, k.c2_n, 16, bz)],
        (c1, window, wind, first, second, *wind_slabs), 1 << 24)
    got3, got4, got7 = crossed(to3, 3), crossed(to4, 4), crossed(to7, 7)
    (mine,) = call(functools.partial(share_kernel, k), [(k.to1, bz)], [], (to3, got3, got4, got7), 1 << 12)
    (result,) = call(
        functools.partial(close_kernel, k), [(bx, by, bz)],
        [(8, k.c2, bz)] + level1 + level2 + [fine(bx + 2)] * 2,
        (mine, crossed(mine, 1), got3, got4, got7, own), 1 << 23)
    return result


def solution(mesh):
    gx, gy, gz = (mesh.shape[a] for a in ("gx", "gy", "gz"))
    mirror = (gx, gy) == (2, 4)

    def run(pressure, wind):
        form, sizes = (mirrored, Mirror) if mirror else (general, Sizes)
        return form(sizes(gx, gy, gz, *pressure.shape), pressure, wind)

    in_specs = (P("gx", "gy", "gz"), P(None, "gx", "gy", "gz"))
    return jax.shard_map(run, mesh=mesh, in_specs=in_specs, out_specs=P("gx", "gy", "gz"), check_vma=False)
```
